32 devices in a mesh: outer: 4 (over y, core), inner: 8 (over z, x).
Axes of the slice: x: 2, y: 2, z: 4, core: 2. Of those that a mesh axis runs over, the one named last changes fastest.
Arguments:
- amplitudes: float32 [2, 8388608], P(None, ('outer', 'inner')), may hold values from -200 to 200
Outputs:
- transformed: float32 [2, 8388608], P(None, ('outer', 'inner'))
- checks: float32 [3], replicated
The draws below stay inside these ranges and needn't reach their ends.
All inputs are finite; a program needn't handle non-finite values.
Results may differ from the reference program's by a relative error of at most 0.00007.
Values sent between devices are 32-bit elements; how exact they have to be, the bound alone decides.
A program may use at most 64 MiB of HBM per device.

```python
import math
import jax
import jax.numpy as jnp
from jax import lax

AMP_DEV = 262144
WINDOW = 9
DEVICES = 32


def draw_amplitudes(key, part):
    total_len = AMP_DEV * DEVICES
    first, second = jax.random.split(key, 2)
    position = jnp.arange(total_len, dtype=jnp.int32)
    device_pos = (position // AMP_DEV).astype(jnp.float32) / max(DEVICES - 1, 1)
    cell_scale = jnp.exp(jax.random.uniform(second, (total_len,), jnp.float32) * math.log(10.0))
    values = jnp.clip(jax.random.normal(first, (2, total_len), jnp.float32), -5.0, 5.0)
    ramp = 3.0 ** device_pos
    return values * ramp * cell_scale / 3.0


def setup_inputs(seed: int = 0) -> dict:
    streams_of = jax.random.split(jax.random.key(seed), 2)
    return {
        "amplitudes": draw_amplitudes(jax.random.fold_in(streams_of[1], 71), 0),
    }


def bit_reverse_table(count):
    result = []
    for value in range(2 ** count):
        flipped = 0
        for bit_pos in range(count):
            flipped = flipped | (value >> bit_pos & 1) << count - 1 - bit_pos
        result.append(flipped)
    return jnp.array(result, dtype=jnp.int32)

def reference(amplitudes):
    columns = 2 ** WINDOW
    total_len = AMP_DEV * DEVICES
    qubits = total_len.bit_length() - 1
    complex_amp = lax.complex(amplitudes[0], amplitudes[1]).reshape(-1, columns)
    spectrum = jnp.fft.ifft(complex_amp, axis=-1) * math.sqrt(columns)
    windowed = spectrum[:, bit_reverse_table(WINDOW)].reshape(-1)
    stacked = jnp.stack([jnp.real(windowed), jnp.imag(windowed)])
    expanded = stacked.reshape((2,) + (2,) * qubits)
    reversed_field = jnp.transpose(expanded, [0] + list(range(qubits, 0, -1))).reshape(2, total_len)
    mean_square = jnp.sum(reversed_field * reversed_field) / total_len
    factor = lax.rsqrt(mean_square + 1e-06)
    transformed = reversed_field * factor
    angles = jnp.arange(total_len, dtype=jnp.int32).astype(jnp.float32) * (2.0 * math.pi / total_len)
    cosine = jnp.cos(angles)
    sine = jnp.sin(angles)
    scaled = 1.0 / math.sqrt(total_len)
    phase_real = jnp.sum(transformed[0] * cosine + transformed[1] * sine) * scaled
    phase_imag = jnp.sum(transformed[1] * cosine - transformed[0] * sine) * scaled
    return (transformed, jnp.stack([mean_square, phase_real, phase_imag]))
```

```python
import functools
import math

import jax
import jax.numpy as jnp
import numpy as np
from jax import lax
from jax.experimental import pallas as pl
from jax.experimental.pallas import tpu as pltpu
from jax.sharding import PartitionSpec as P

WINDOW = 9
COLUMNS = 2**WINDOW
LANES = 128
SUB = 8
RADIX = COLUMNS // LANES
PIECES = ((0,), (1, 2), (3,))
MESH = pl.DeviceIdType.MESH


def rev(value, count):
    out = 0
    for bit in range(count):
        out |= (value >> bit & 1) << (count - 1 - bit)
    return out


def split_bf16(values):
    high = values.astype(jnp.bfloat16)
    return high, (values - high.astype(np.float32)).astype(jnp.bfloat16)


def tables(n_devices, total_len):
    f = np.arange(COLUMNS).reshape(LANES, RADIX).T
    lane = np.arange(LANES)
    ang = (f[:, :, None] * lane) % COLUMNS * (2.0 * np.pi / COLUMNS)
    c, s = np.cos(ang) / math.sqrt(COLUMNS), np.sin(ang) / math.sqrt(COLUMNS)
    table = np.stack([np.concatenate([c, -s], -1), np.concatenate([s, c], -1)], 2)
    table = table.reshape(RADIX, 2 * LANES, 2 * LANES).astype(np.float32)
    slots = 2.0 * np.pi / total_len * np.arange(n_devices)
    subs = 2.0 * np.pi / total_len * n_devices * RADIX * np.arange(SUB)
    turn = np.zeros((2 * (n_devices + SUB), LANES), np.float32)
    turn[:n_devices], turn[n_devices : 2 * n_devices] = np.cos(slots)[:, None], np.sin(slots)[:, None]
    turn[2 * n_devices : 2 * n_devices + SUB, 1] = np.cos(subs) * math.sqrt(COLUMNS)
    turn[2 * n_devices + SUB :, 1] = np.sin(subs) * math.sqrt(COLUMNS)
    return table, turn


def pieces_of(n_devices):
    rows = [len(chunks) * RADIX * SUB + (k == 0) for k, chunks in enumerate(PIECES)]
    return rows, [r if r % 2 else r + 4 for r in rows]


def turn_tiles(recv, pitch, place, h, n_devices, factor):
    tile = jnp.concatenate(
        [recv[pl.ds((place * RADIX + rev(j, 2)) * SUB + h, n_devices, stride=pitch), :] for j in range(RADIX)], 0)
    turned = tile.T.reshape(LANES // SUB, SUB, LANES)
    return [turned[m] * factor for m in range(LANES // SUB)]


def kernel(n_outer, n_inner, total_len, x_hbm, th_hbm, tl_hbm, turn_hbm, *refs):
    n_pieces = len(PIECES)
    field, last, tot_ref, fac_ref, x_ref, th_ref, tl_ref, turn_ref, bh_ref, bl_ref = refs[:10]
    sends, recvs = refs[10 : 10 + n_pieces], [*refs[10 + n_pieces : 9 + 2 * n_pieces], last]
    send_sem, recv_sem, own_sem, load_sem = refs[9 + 2 * n_pieces :]
    n_devices = n_outer * n_inner
    obits, ibits = n_outer.bit_length() - 1, n_inner.bit_length() - 1
    span = LANES
    q_rows = span + 4

    loads = []
    for g in range(RADIX):
        for q in range(SUB):
            loads.append(pltpu.make_async_copy(
                x_hbm.at[pl.ds((g * SUB + q) * span, span)],
                x_ref.at[pl.ds((g * SUB + rev(q, 3)) * q_rows, span)], load_sem.at[g]))
    rest = [pltpu.make_async_copy(src, dst, load_sem.at[RADIX + k]) for k, (src, dst) in enumerate(
        [(th_hbm, th_ref), (tl_hbm, tl_ref), (turn_hbm, turn_ref)])]
    for load in loads + rest:
        load.start()

    o, i = lax.axis_index("outer"), lax.axis_index("inner")
    me = o * n_inner + i
    slot = 0
    odelta, idelta = [], []
    for k in range(obits):
        bit = o // 2**k % 2
        slot = slot + bit * 2 ** (obits - 1 - k)
        odelta.append((1 - 2 * bit) * 2**k)
    for k in range(ibits):
        bit = i // 2**k % 2
        slot = slot + bit * 2 ** (ibits - 1 - k) * n_outer
        idelta.append((1 - 2 * bit) * 2**k)

    def peer(mo, mi):
        po, pi = o, i
        for k in range(obits):
            if mo >> k & 1:
                po = po + odelta[k]
        for k in range(ibits):
            if mi >> k & 1:
                pi = pi + idelta[k]
        return po, pi

    peers = [peer(mo, mi) for mi in range(n_inner - 1, -1, -1) for mo in range(n_outer) if mo or mi]
    barrier = pltpu.get_barrier_semaphore()
    for p in peers:
        pl.semaphore_signal(barrier, inc=1, device_id=p, device_id_type=MESH)

    rows, pitches = pieces_of(n_devices)

    def send(k):
        dst = recvs[k].at[pl.ds(slot * pitches[k], rows[k])]
        for po, pi in peers:
            pltpu.make_async_remote_copy(
                src_ref=sends[k].at[pl.ds((po * n_inner + pi) * rows[k], rows[k])], dst_ref=dst,
                send_sem=send_sem, recv_sem=recv_sem.at[k],
                device_id=(po, pi), device_id_type=MESH).start()
        own_copy(k).start()

    def own_copy(k):
        return pltpu.make_async_copy(
            sends[k].at[pl.ds(me * rows[k], rows[k])],
            recvs[k].at[pl.ds(slot * pitches[k], rows[k])], own_sem.at[k])

    def wait_rows(ref, count, sem):
        part = ref.at[pl.ds(0, count)]
        pltpu.make_async_copy(part, part, sem).wait()

    zero = jnp.zeros((SUB, LANES), jnp.float32)
    squares, zr, zi = [zero] * 4, zero, zero
    for g in range(RADIX):
        wait_rows(x_ref, SUB * span, load_sem.at[g])
        for pair in range(SUB):
            part = [[[x_ref[pl.ds(g * SUB * q_rows + (2 * pair + w) * SUB + 2 * ct + s, SUB, stride=q_rows), :]
                      for w in range(2)] for s in range(2)] for ct in range(RADIX)]
            for ct in range(RADIX):
                for s in range(2):
                    for w in range(2):
                        squares[ct] = squares[ct] + part[ct][s][w] * part[ct][s][w]
            for w in range(2):
                angle = 2.0 * math.pi / total_len * n_devices * (rev(2 * pair + w, 4) * SUB * RADIX + rev(g, 2))
                cw, sw = math.cos(angle), math.sin(angle)
                zr = zr + (part[0][0][w] * cw + part[0][1][w] * sw)
                zi = zi + (part[0][1][w] * cw - part[0][0][w] * sw)
            (x0r, x0i), (x1r, x1i), (x2r, x2i), (x3r, x3i) = [
                [jnp.concatenate(part[ct][s], 0) for s in range(2)] for ct in range(RADIX)]
            ar, ai, br, bi = x0r + x2r, x0i + x2i, x0r - x2r, x0i - x2i
            cr_, ci_, dr, di = x1r + x3r, x1i + x3i, x1r - x3r, x1i - x3i
            mixed = [(ar + cr_, ai + ci_), (br - di, bi + dr), (ar - cr_, ai - ci_), (br + di, bi - dr)]
            at = pl.ds((g * SUB + pair) * 2 * SUB, 2 * SUB)
            for chunk in range(RADIX):
                for s in range(2):
                    high, low = split_bf16(mixed[chunk][s])
                    bh_ref[chunk, at, s * LANES : (s + 1) * LANES] = high
                    bl_ref[chunk, at, s * LANES : (s + 1) * LANES] = low

    for load in rest:
        load.wait()
    pc, ps = turn_ref[2 * n_devices : 2 * n_devices + SUB, :], turn_ref[2 * n_devices + SUB :, :]
    oc, os_ = turn_ref[pl.ds(slot, 1), :], turn_ref[pl.ds(n_devices + slot, 1), :]
    total = jnp.sum(jnp.sum((squares[0] + squares[1]) + (squares[2] + squares[3]), 0, keepdims=True), 1, keepdims=True)
    yr = jnp.sum(zr * pc + zi * ps, 0, keepdims=True)
    yi = jnp.sum(zi * pc - zr * ps, 0, keepdims=True)
    wr = jnp.sum(yr * oc + yi * os_, 1, keepdims=True)
    wi = jnp.sum(yi * oc - yr * os_, 1, keepdims=True)
    lane = lax.broadcasted_iota(jnp.int32, (1, LANES), 1)
    stat = jnp.where(lane == 0, total, jnp.where(lane == 1, wr, jnp.where(lane == 2, wi, 0.0)))
    sends[0][pl.ds(rows[0] - 1, n_devices, stride=rows[0]), :] = jnp.broadcast_to(stat, (n_devices, LANES))

    dims = (((1,), (1,)), ((), ()))
    for k, chunks in enumerate(PIECES):
        for place, chunk in enumerate(chunks):
            th, tl, bh, bl = th_ref[chunk], tl_ref[chunk], bh_ref[chunk], bl_ref[chunk]
            res = lax.dot_general(th, bh, dims, preferred_element_type=jnp.float32)
            res += lax.dot_general(th, bl, dims, preferred_element_type=jnp.float32)
            res += lax.dot_general(tl, bh, dims, preferred_element_type=jnp.float32)
            for e in range(n_devices):
                for g in range(RADIX):
                    sends[k][pl.ds(e * rows[k] + (place * RADIX + g) * SUB, SUB), :] = (
                        res[e * SUB : (e + 1) * SUB, g * LANES : (g + 1) * LANES])
        if k == 0:
            pl.semaphore_wait(barrier, len(peers))
        send(k)

    for k, chunks in enumerate(PIECES):
        wait_rows(recvs[k], len(peers) * rows[k], recv_sem.at[k])
        own_copy(k).wait()
        if k == 0:
            sums = jnp.sum(recvs[0][pl.ds(rows[0] - 1, n_devices, stride=pitches[0]), :], 0, keepdims=True)
            mean_square = jnp.sum(jnp.where(lane == 0, sums, 0.0), 1, keepdims=True) / total_len
            shifted = mean_square + 1e-06
            factor = lax.rsqrt(shifted)
            factor = factor * (1.5 - 0.5 * shifted * factor * factor)
            checks = jnp.where(lane == 0, mean_square, sums * (factor / math.sqrt(total_len)))
            tot_ref[...] = jnp.broadcast_to(checks, (SUB, LANES))
            factor = jnp.broadcast_to(factor, (SUB, LANES))
            fac_ref[...] = factor
        if k == n_pieces - 1:
            break
        for place, chunk in enumerate(chunks):
            for h in range(SUB):
                base = ((h // 2) * (RADIX - 1) + chunk) * 2 * LANES + h % 2
                for m, v in enumerate(turn_tiles(recvs[k], pitches[k], place, h, n_devices, factor)):
                    field[pl.ds(base + rev(m, 4) * 2 * SUB, SUB, stride=2), :] = v
    for k in range(n_pieces):
        wait_rows(sends[k], len(peers) * rows[k], send_sem)


def finish_kernel(n_devices, pitch, field, last, tot_ref, fac_ref, out_hbm, checks_ref, turned, sem):
    f_rows = 2 * LANES
    many = (RADIX - 1) * f_rows
    stores = []
    for fq in range(RADIX):
        stores.append(pltpu.make_async_copy(
            field.at[pl.ds(fq * many, many)], out_hbm.at[pl.ds(fq * RADIX * f_rows, many)], sem.at[fq]))
        stores[-1].start()
    checks_ref[...] = tot_ref[0:1, 0:3]
    factor = fac_ref[...]
    for h in range(SUB):
        base = h // 2 * f_rows + h % 2
        for m, v in enumerate(turn_tiles(last, pitch, 0, h, n_devices, factor)):
            turned[pl.ds(base + rev(m, 4) * 2 * SUB, SUB, stride=2), :] = v
        if h % 2:
            fq = h // 2
            stores.append(pltpu.make_async_copy(
                turned.at[pl.ds(fq * f_rows, f_rows)],
                out_hbm.at[pl.ds((fq * RADIX + RADIX - 1) * f_rows, f_rows)], sem.at[RADIX + fq]))
            stores[-1].start()
    for store in stores:
        store.wait()


def fast(n_outer, n_inner, amplitudes):
    amp_dev = amplitudes.shape[1]
    n_devices = n_outer * n_inner
    rows_count = amp_dev // COLUMNS
    total_len = amp_dev * n_devices
    view = amplitudes.reshape(2, amp_dev // LANES, LANES).transpose(1, 0, 2).reshape(-1, LANES)
    table, turn = tables(n_devices, total_len)
    th = table.astype(jnp.bfloat16)
    tl = (table - th.astype(np.float32)).astype(jnp.bfloat16)
    hbm, vmem = pl.BlockSpec(memory_space=pltpu.HBM), pl.BlockSpec(memory_space=pltpu.VMEM)
    rows, pitches = pieces_of(n_devices)
    small = pltpu.VMEM((SUB, LANES), jnp.float32)
    f_rows = 2 * LANES
    pair = pltpu.VMEM((RADIX, rows_count, 2 * LANES), jnp.bfloat16)
    scratch = [
        pltpu.VMEM((RADIX * SUB * (LANES + 4), LANES), jnp.float32),
        pltpu.VMEM(th.shape, jnp.bfloat16),
        pltpu.VMEM(tl.shape, jnp.bfloat16),
        pltpu.VMEM(turn.shape, jnp.float32),
        pair,
        pair,
        *[pltpu.VMEM((n_devices * r, LANES), jnp.float32) for r in rows],
        *[pltpu.VMEM((n_devices * p, LANES), jnp.float32) for p in pitches[:-1]],
        pltpu.SemaphoreType.DMA,
        pltpu.SemaphoreType.DMA((len(PIECES),)),
        pltpu.SemaphoreType.DMA((len(PIECES),)),
        pltpu.SemaphoreType.DMA((RADIX + 3,)),
    ]
    parts = pl.pallas_call(
        functools.partial(kernel, n_outer, n_inner, total_len),
        out_shape=(
            pltpu.VMEM((RADIX * (RADIX - 1) * f_rows, LANES), jnp.float32),
            pltpu.VMEM((n_devices * pitches[-1], LANES), jnp.float32),
            small,
            small,
        ),
        in_specs=[hbm] * 4,
        out_specs=(vmem,) * 4,
        scratch_shapes=scratch,
        compiler_params=pltpu.CompilerParams(collective_id=0, has_side_effects=True, vmem_limit_bytes=32_000_000),
    )(view, jnp.asarray(th), jnp.asarray(tl), jnp.asarray(turn))
    field, checks = pl.pallas_call(
        functools.partial(finish_kernel, n_devices, pitches[-1]),
        out_shape=(jax.ShapeDtypeStruct(view.shape, jnp.float32), jax.ShapeDtypeStruct((1, 3), jnp.float32)),
        in_specs=[vmem] * 4,
        out_specs=(hbm, vmem),
        scratch_shapes=[
            pltpu.VMEM((RADIX * f_rows, LANES), jnp.float32),
            pltpu.SemaphoreType.DMA((2 * RADIX,)),
        ],
        compiler_params=pltpu.CompilerParams(vmem_limit_bytes=32_000_000),
    )(*parts)
    result = field.reshape(-1, 2, LANES).transpose(1, 0, 2).reshape(2, amp_dev)
    return result, checks.reshape(3)


def reverse_index(values, count):
    result = jnp.zeros_like(values)
    for bit_pos in range(count):
        result = result | (values >> bit_pos & 1) << count - 1 - bit_pos
    return result


def reversal_table(size, count):
    indices = jnp.arange(size, dtype=jnp.int32)
    return (reverse_index(indices, count)[:, None] == indices[None, :]).astype(jnp.float32)


def check_terms(current, positions, angle_scale):
    angles = positions.astype(jnp.float32) * angle_scale
    cosine = jnp.cos(angles)
    sine = jnp.sin(angles)
    squares = jnp.sum(current * current)
    phase_real = jnp.sum(current[0] * cosine + current[1] * sine)
    phase_imag = jnp.sum(current[1] * cosine - current[0] * sine)
    return (squares, phase_real, phase_imag)


def per_device(amplitudes):
    amp_dev = amplitudes.shape[1]
    n_outer = lax.axis_size("outer")
    n_inner = lax.axis_size("inner")
    outer_bits = n_outer.bit_length() - 1
    inner_bits = n_inner.bit_length() - 1
    global_bits = outer_bits + inner_bits
    local_bits = amp_dev.bit_length() - 1
    n_devices = n_outer * n_inner
    high_count = amp_dev // n_devices
    total_len = amp_dev * n_devices
    columns = 2**WINDOW
    rows_count = amp_dev // columns
    column_ids = jnp.arange(columns, dtype=jnp.int32)
    reversed_ids = reverse_index(column_ids, WINDOW)
    products = column_ids[:, None] * reversed_ids[None, :] % columns
    angles = products.astype(jnp.float32) * (2.0 * math.pi / columns)
    real_part = jnp.cos(angles) / math.sqrt(columns)
    imag_part = jnp.sin(angles) / math.sqrt(columns)
    table = jnp.concatenate(
        [jnp.concatenate([real_part, imag_part], 1), jnp.concatenate([-imag_part, real_part], 1)], 0
    )
    stacked = jnp.concatenate(
        [amplitudes[0].reshape(rows_count, columns), amplitudes[1].reshape(rows_count, columns)], 1
    )
    result = jnp.dot(
        stacked, table, precision=lax.Precision.HIGHEST, preferred_element_type=jnp.float32
    )
    windowed = jnp.stack([result[:, :columns].reshape(-1), result[:, columns:].reshape(-1)])
    device_id = lax.axis_index("outer") * n_inner + lax.axis_index("inner")
    angle_scale = 2.0 * math.pi / total_len
    local_ids = jnp.arange(amp_dev, dtype=jnp.int32)
    positions = reverse_index(device_id * amp_dev + local_ids, local_bits + global_bits)
    totals = lax.psum(check_terms(windowed, positions, angle_scale), ("outer", "inner"))
    device_table = reversal_table(n_devices, global_bits)
    high_table = reversal_table(high_count, local_bits - global_bits)
    grid = windowed.reshape(2, high_count, n_devices)
    ordered = jnp.einsum("pm,shm->sph", device_table, grid, precision=lax.Precision.HIGHEST)
    blocks = ordered.reshape(2, n_outer, n_inner, high_count)
    blocks = lax.all_to_all(
        lax.all_to_all(blocks, "outer", split_axis=1, concat_axis=1, tiled=True),
        "inner",
        split_axis=2,
        concat_axis=2,
        tiled=True,
    )
    received = blocks.reshape(2, n_devices, high_count)
    turned_high = jnp.einsum("qh,sdh->sdq", high_table, received, precision=lax.Precision.HIGHEST)
    placed = jnp.einsum("ed,sdq->sqe", device_table, turned_high, precision=lax.Precision.HIGHEST)
    reversed_field = placed.reshape(2, amp_dev)
    mean_square = totals[0] / total_len
    factor = lax.rsqrt(mean_square + 1e-06)
    scaled = factor / math.sqrt(total_len)
    checks = jnp.stack([mean_square, totals[1] * scaled, totals[2] * scaled])
    return (reversed_field * factor, checks)


def solution(mesh):
    n_outer, n_inner = mesh.shape["outer"], mesh.shape["inner"]

    def body(amplitudes):
        rows_count = amplitudes.shape[1] // COLUMNS
        n_devices = n_outer * n_inner
        if rows_count * n_devices == LANES * LANES and n_devices * SUB == 2 * LANES:
            return fast(n_outer, n_inner, amplitudes)
        return per_device(amplitudes)

    return jax.shard_map(
        body,
        mesh=mesh,
        in_specs=(P(None, ("outer", "inner")),),
        out_specs=(P(None, ("outer", "inner")), P()),
        check_vma=False,
    )
```

```python
import functools
import math

import jax
import jax.numpy as jnp
import numpy as np
from jax import lax
from jax.experimental import pallas as pl
from jax.experimental.pallas import tpu as pltpu
from jax.sharding import PartitionSpec as P

WINDOW = 9
COLUMNS = 2**WINDOW
LANES = 128
SUB = 8
RADIX = COLUMNS // LANES
PIECES = ((0,), (1, 2), (3,))
MESH = pl.DeviceIdType.MESH


def rev(value, count):
    out = 0
    for bit in range(count):
        out |= (value >> bit & 1) << (count - 1 - bit)
    return out


def split_bf16(values):
    high = values.astype(jnp.bfloat16)
    return high, (values - high.astype(np.float32)).astype(jnp.bfloat16)


def tables(n_devices, total_len):
    f = np.arange(COLUMNS).reshape(LANES, RADIX).T
    lane = np.arange(LANES)
    ang = (f[:, :, None] * lane) % COLUMNS * (2.0 * np.pi / COLUMNS)
    c, s = np.cos(ang) / math.sqrt(COLUMNS), np.sin(ang) / math.sqrt(COLUMNS)
    table = np.stack([np.concatenate([c, -s], -1), np.concatenate([s, c], -1)], 2)
    table = table.reshape(RADIX, 2 * LANES, 2 * LANES).astype(np.float32)
    slots = 2.0 * np.pi / total_len * np.arange(n_devices)
    subs = 2.0 * np.pi / total_len * n_devices * RADIX * np.arange(SUB)
    turn = np.zeros((2 * (n_devices + SUB), LANES), np.float32)
    turn[:n_devices], turn[n_devices : 2 * n_devices] = np.cos(slots)[:, None], np.sin(slots)[:, None]
    turn[2 * n_devices : 2 * n_devices + SUB, 1] = np.cos(subs) * math.sqrt(COLUMNS)
    turn[2 * n_devices + SUB :, 1] = np.sin(subs) * math.sqrt(COLUMNS)
    return table, turn


def pieces_of(n_devices):
    rows = [len(chunks) * RADIX * SUB + (k == 0) for k, chunks in enumerate(PIECES)]
    return rows, [r if r % 2 else r + 4 for r in rows]


def turn_tiles(recv, pitch, place, h, n_devices, factor):
    tile = jnp.concatenate(
        [recv[pl.ds((place * RADIX + rev(j, 2)) * SUB + h, n_devices, stride=pitch), :] for j in range(RADIX)], 0)
    turned = tile.T.reshape(LANES // SUB, SUB, LANES)
    return [turned[m] * factor for m in range(LANES // SUB)]


def kernel(n_outer, n_inner, total_len, x_hbm, th_hbm, tl_hbm, turn_hbm, *refs):
    n_pieces = len(PIECES)
    field, last, tot_ref, fac_ref, x_ref, th_ref, tl_ref, turn_ref, bh_ref, bl_ref = refs[:10]
    sends, recvs = refs[10 : 10 + n_pieces], [*refs[10 + n_pieces : 9 + 2 * n_pieces], last]
    send_sem, recv_sem, own_sem, load_sem = refs[9 + 2 * n_pieces :]
    n_devices = n_outer * n_inner
    obits, ibits = n_outer.bit_length() - 1, n_inner.bit_length() - 1
    span = LANES
    q_rows = span + 4

    loads = []
    for g in range(RADIX):
        for q in range(SUB):
            loads.append(pltpu.make_async_copy(
                x_hbm.at[pl.ds((g * SUB + q) * span, span)],
                x_ref.at[pl.ds((g * SUB + rev(q, 3)) * q_rows, span)], load_sem.at[g]))
    rest = [pltpu.make_async_copy(src, dst, load_sem.at[RADIX + k]) for k, (src, dst) in enumerate(
        [(th_hbm, th_ref), (tl_hbm, tl_ref), (turn_hbm, turn_ref)])]
    for load in loads + rest:
        load.start()

    o, i = lax.axis_index("outer"), lax.axis_index("inner")
    me = o * n_inner + i
    slot = 0
    odelta, idelta = [], []
    for k in range(obits):
        bit = o // 2**k % 2
        slot = slot + bit * 2 ** (obits - 1 - k)
        odelta.append((1 - 2 * bit) * 2**k)
    for k in range(ibits):
        bit = i // 2**k % 2
        slot = slot + bit * 2 ** (ibits - 1 - k) * n_outer
        idelta.append((1 - 2 * bit) * 2**k)

    def peer(mo, mi):
        po, pi = o, i
        for k in range(obits):
            if mo >> k & 1:
                po = po + odelta[k]
        for k in range(ibits):
            if mi >> k & 1:
                pi = pi + idelta[k]
        return po, pi

    peers = [peer(mo, mi) for mi in range(n_inner - 1, -1, -1) for mo in range(n_outer) if mo or mi]
    barrier = pltpu.get_barrier_semaphore()
    for p in peers:
        pl.semaphore_signal(barrier, inc=1, device_id=p, device_id_type=MESH)

    rows, pitches = pieces_of(n_devices)

    def send(k):
        dst = recvs[k].at[pl.ds(slot * pitches[k], rows[k])]
        for po, pi in peers:
            pltpu.make_async_remote_copy(
                src_ref=sends[k].at[pl.ds((po * n_inner + pi) * rows[k], rows[k])], dst_ref=dst,
                send_sem=send_sem, recv_sem=recv_sem.at[k],
                device_id=(po, pi), device_id_type=MESH).start()
        own_copy(k).start()

    def own_copy(k):
        return pltpu.make_async_copy(
            sends[k].at[pl.ds(me * rows[k], rows[k])],
            recvs[k].at[pl.ds(slot * pitches[k], rows[k])], own_sem.at[k])

    def wait_rows(ref, count, sem):
        part = ref.at[pl.ds(0, count)]
        pltpu.make_async_copy(part, part, sem).wait()

    zero = jnp.zeros((SUB, LANES), jnp.float32)
    squares, zr, zi = [zero] * 4, zero, zero
    for g in range(RADIX):
        wait_rows(x_ref, SUB * span, load_sem.at[g])
        for pair in range(SUB):
            part = [[[x_ref[pl.ds(g * SUB * q_rows + (2 * pair + w) * SUB + 2 * ct + s, SUB, stride=q_rows), :]
                      for w in range(2)] for s in range(2)] for ct in range(RADIX)]
            for ct in range(RADIX):
                for s in range(2):
                    for w in range(2):
                        squares[ct] = squares[ct] + part[ct][s][w] * part[ct][s][w]
            for w in range(2):
                angle = 2.0 * math.pi / total_len * n_devices * (rev(2 * pair + w, 4) * SUB * RADIX + rev(g, 2))
                cw, sw = math.cos(angle), math.sin(angle)
                zr = zr + (part[0][0][w] * cw + part[0][1][w] * sw)
                zi = zi + (part[0][1][w] * cw - part[0][0][w] * sw)
            (x0r, x0i), (x1r, x1i), (x2r, x2i), (x3r, x3i) = [
                [jnp.concatenate(part[ct][s], 0) for s in range(2)] for ct in range(RADIX)]
            ar, ai, br, bi = x0r + x2r, x0i + x2i, x0r - x2r, x0i - x2i
            cr_, ci_, dr, di = x1r + x3r, x1i + x3i, x1r - x3r, x1i - x3i
            mixed = [(ar + cr_, ai + ci_), (br - di, bi + dr), (ar - cr_, ai - ci_), (br + di, bi - dr)]
            at = pl.ds((g * SUB + pair) * 2 * SUB, 2 * SUB)
            for chunk in range(RADIX):
                for s in range(2):
                    high, low = split_bf16(mixed[chunk][s])
                    bh_ref[chunk, at, s * LANES : (s + 1) * LANES] = high
                    bl_ref[chunk, at, s * LANES : (s + 1) * LANES] = low

    for load in rest:
        load.wait()
    pc, ps = turn_ref[2 * n_devices : 2 * n_devices + SUB, :], turn_ref[2 * n_devices + SUB :, :]
    oc, os_ = turn_ref[pl.ds(slot, 1), :], turn_ref[pl.ds(n_devices + slot, 1), :]
    total = jnp.sum(jnp.sum((squares[0] + squares[1]) + (squares[2] + squares[3]), 0, keepdims=True), 1, keepdims=True)
    yr = jnp.sum(zr * pc + zi * ps, 0, keepdims=True)
    yi = jnp.sum(zi * pc - zr * ps, 0, keepdims=True)
    wr = jnp.sum(yr * oc + yi * os_, 1, keepdims=True)
    wi = jnp.sum(yi * oc - yr * os_, 1, keepdims=True)
    lane = lax.broadcasted_iota(jnp.int32, (1, LANES), 1)
    stat = jnp.where(lane == 0, total, jnp.where(lane == 1, wr, jnp.where(lane == 2, wi, 0.0)))
    sends[0][pl.ds(rows[0] - 1, n_devices, stride=rows[0]), :] = jnp.broadcast_to(stat, (n_devices, LANES))

    dims = (((1,), (1,)), ((), ()))
    for k, chunks in enumerate(PIECES):
        for place, chunk in enumerate(chunks):
            th, tl, bh, bl = th_ref[chunk], tl_ref[chunk], bh_ref[chunk], bl_ref[chunk]
            res = lax.dot_general(th, bh, dims, preferred_element_type=jnp.float32)
            res += lax.dot_general(th, bl, dims, preferred_element_type=jnp.float32)
            res += lax.dot_general(tl, bh, dims, preferred_element_type=jnp.float32)
            for e in range(n_devices):
                for g in range(RADIX):
                    sends[k][pl.ds(e * rows[k] + (place * RADIX + g) * SUB, SUB), :] = (
                        res[e * SUB : (e + 1) * SUB, g * LANES : (g + 1) * LANES])
        if k == 0:
            pl.semaphore_wait(barrier, len(peers))
        send(k)

    for k, chunks in enumerate(PIECES):
        wait_rows(recvs[k], len(peers) * rows[k], recv_sem.at[k])
        own_copy(k).wait()
        if k == 0:
            sums = jnp.sum(recvs[0][pl.ds(rows[0] - 1, n_devices, stride=pitches[0]), :], 0, keepdims=True)
            mean_square = jnp.sum(jnp.where(lane == 0, sums, 0.0), 1, keepdims=True) / total_len
            shifted = mean_square + 1e-06
            factor = lax.rsqrt(shifted)
            factor = factor * (1.5 - 0.5 * shifted * factor * factor)
            checks = jnp.where(lane == 0, mean_square, sums * (factor / math.sqrt(total_len)))
            tot_ref[...] = jnp.broadcast_to(checks, (SUB, LANES))
            factor = jnp.broadcast_to(factor, (SUB, LANES))
            fac_ref[...] = factor
        if k == n_pieces - 1:
            break
        for place, chunk in enumerate(chunks):
            for h in range(SUB):
                base = ((h // 2) * (RADIX - 1) + chunk) * 2 * LANES + h % 2
                for m, v in enumerate(turn_tiles(recvs[k], pitches[k], place, h, n_devices, factor)):
                    field[pl.ds(base + rev(m, 4) * 2 * SUB, SUB, stride=2), :] = v
    for k in range(n_pieces):
        wait_rows(sends[k], len(peers) * rows[k], send_sem)


def finish_kernel(n_devices, pitch, field, last, tot_ref, fac_ref, out_hbm, checks_ref, turned, sem):
    f_rows = 2 * LANES
    many = (RADIX - 1) * f_rows
    stores = []
    for fq in range(RADIX):
        stores.append(pltpu.make_async_copy(
            field.at[pl.ds(fq * many, many)], out_hbm.at[pl.ds(fq * RADIX * f_rows, many)], sem.at[fq]))
        stores[-1].start()
    checks_ref[...] = tot_ref[0:1, 0:3]
    factor = fac_ref[...]
    for h in range(SUB):
        base = h // 2 * f_rows + h % 2
        for m, v in enumerate(turn_tiles(last, pitch, 0, h, n_devices, factor)):
            turned[pl.ds(base + rev(m, 4) * 2 * SUB, SUB, stride=2), :] = v
        if h % 2:
            fq = h // 2
            stores.append(pltpu.make_async_copy(
                turned.at[pl.ds(fq * f_rows, f_rows)],
                out_hbm.at[pl.ds((fq * RADIX + RADIX - 1) * f_rows, f_rows)], sem.at[RADIX + fq]))
            stores[-1].start()
    for store in stores:
        store.wait()


def fast(n_outer, n_inner, amplitudes):
    amp_dev = amplitudes.shape[1]
    n_devices = n_outer * n_inner
    rows_count = amp_dev // COLUMNS
    total_len = amp_dev * n_devices
    view = amplitudes.reshape(2, amp_dev // LANES, LANES).transpose(1, 0, 2).reshape(-1, LANES)
    table, turn = tables(n_devices, total_len)
    th = table.astype(jnp.bfloat16)
    tl = (table - th.astype(np.float32)).astype(jnp.bfloat16)
    hbm, vmem = pl.BlockSpec(memory_space=pltpu.HBM), pl.BlockSpec(memory_space=pltpu.VMEM)
    rows, pitches = pieces_of(n_devices)
    small = pltpu.VMEM((SUB, LANES), jnp.float32)
    f_rows = 2 * LANES
    pair = pltpu.VMEM((RADIX, rows_count, 2 * LANES), jnp.bfloat16)
    scratch = [
        pltpu.VMEM((RADIX * SUB * (LANES + 4), LANES), jnp.float32),
        pltpu.VMEM(th.shape, jnp.bfloat16),
        pltpu.VMEM(tl.shape, jnp.bfloat16),
        pltpu.VMEM(turn.shape, jnp.float32),
        pair,
        pair,
        *[pltpu.VMEM((n_devices * r, LANES), jnp.float32) for r in rows],
        *[pltpu.VMEM((n_devices * p, LANES), jnp.float32) for p in pitches[:-1]],
        pltpu.SemaphoreType.DMA,
        pltpu.SemaphoreType.DMA((len(PIECES),)),
        pltpu.SemaphoreType.DMA((len(PIECES),)),
        pltpu.SemaphoreType.DMA((RADIX + 3,)),
    ]
    parts = pl.pallas_call(
        functools.partial(kernel, n_outer, n_inner, total_len),
        out_shape=(
            pltpu.VMEM((RADIX * (RADIX - 1) * f_rows, LANES), jnp.float32),
            pltpu.VMEM((n_devices * pitches[-1], LANES), jnp.float32),
            small,
            small,
        ),
        in_specs=[hbm] * 4,
        out_specs=(vmem,) * 4,
        scratch_shapes=scratch,
        compiler_params=pltpu.CompilerParams(collective_id=0, has_side_effects=True, vmem_limit_bytes=32_000_000),
    )(*[pltpu.with_memory_space_constraint(v, pltpu.HBM) for v in (view, jnp.asarray(th), jnp.asarray(tl), jnp.asarray(turn))])
    field, checks = pl.pallas_call(
        functools.partial(finish_kernel, n_devices, pitches[-1]),
        out_shape=(jax.ShapeDtypeStruct(view.shape, jnp.float32), jax.ShapeDtypeStruct((1, 3), jnp.float32)),
        in_specs=[vmem] * 4,
        out_specs=(hbm, vmem),
        scratch_shapes=[
            pltpu.VMEM((RADIX * f_rows, LANES), jnp.float32),
            pltpu.SemaphoreType.DMA((2 * RADIX,)),
        ],
        compiler_params=pltpu.CompilerParams(vmem_limit_bytes=32_000_000),
    )(*parts)
    result = field.reshape(-1, 2, LANES).transpose(1, 0, 2).reshape(2, amp_dev)
    return result, checks.reshape(3)


def reverse_index(values, count):
    result = jnp.zeros_like(values)
    for bit_pos in range(count):
        result = result | (values >> bit_pos & 1) << count - 1 - bit_pos
    return result


def reversal_table(size, count):
    indices = jnp.arange(size, dtype=jnp.int32)
    return (reverse_index(indices, count)[:, None] == indices[None, :]).astype(jnp.float32)


def check_terms(current, positions, angle_scale):
    angles = positions.astype(jnp.float32) * angle_scale
    cosine = jnp.cos(angles)
    sine = jnp.sin(angles)
    squares = jnp.sum(current * current)
    phase_real = jnp.sum(current[0] * cosine + current[1] * sine)
    phase_imag = jnp.sum(current[1] * cosine - current[0] * sine)
    return (squares, phase_real, phase_imag)


def per_device(amplitudes):
    amp_dev = amplitudes.shape[1]
    n_outer = lax.axis_size("outer")
    n_inner = lax.axis_size("inner")
    outer_bits = n_outer.bit_length() - 1
    inner_bits = n_inner.bit_length() - 1
    global_bits = outer_bits + inner_bits
    local_bits = amp_dev.bit_length() - 1
    n_devices = n_outer * n_inner
    high_count = amp_dev // n_devices
    total_len = amp_dev * n_devices
    columns = 2**WINDOW
    rows_count = amp_dev // columns
    column_ids = jnp.arange(columns, dtype=jnp.int32)
    reversed_ids = reverse_index(column_ids, WINDOW)
    products = column_ids[:, None] * reversed_ids[None, :] % columns
    angles = products.astype(jnp.float32) * (2.0 * math.pi / columns)
    real_part = jnp.cos(angles) / math.sqrt(columns)
    imag_part = jnp.sin(angles) / math.sqrt(columns)
    table = jnp.concatenate(
        [jnp.concatenate([real_part, imag_part], 1), jnp.concatenate([-imag_part, real_part], 1)], 0
    )
    stacked = jnp.concatenate(
        [amplitudes[0].reshape(rows_count, columns), amplitudes[1].reshape(rows_count, columns)], 1
    )
    result = jnp.dot(
        stacked, table, precision=lax.Precision.HIGHEST, preferred_element_type=jnp.float32
    )
    windowed = jnp.stack([result[:, :columns].reshape(-1), result[:, columns:].reshape(-1)])
    device_id = lax.axis_index("outer") * n_inner + lax.axis_index("inner")
    angle_scale = 2.0 * math.pi / total_len
    local_ids = jnp.arange(amp_dev, dtype=jnp.int32)
    positions = reverse_index(device_id * amp_dev + local_ids, local_bits + global_bits)
    totals = lax.psum(check_terms(windowed, positions, angle_scale), ("outer", "inner"))
    device_table = reversal_table(n_devices, global_bits)
    high_table = reversal_table(high_count, local_bits - global_bits)
    grid = windowed.reshape(2, high_count, n_devices)
    ordered = jnp.einsum("pm,shm->sph", device_table, grid, precision=lax.Precision.HIGHEST)
    blocks = ordered.reshape(2, n_outer, n_inner, high_count)
    blocks = lax.all_to_all(
        lax.all_to_all(blocks, "outer", split_axis=1, concat_axis=1, tiled=True),
        "inner",
        split_axis=2,
        concat_axis=2,
        tiled=True,
    )
    received = blocks.reshape(2, n_devices, high_count)
    turned_high = jnp.einsum("qh,sdh->sdq", high_table, received, precision=lax.Precision.HIGHEST)
    placed = jnp.einsum("ed,sdq->sqe", device_table, turned_high, precision=lax.Precision.HIGHEST)
    reversed_field = placed.reshape(2, amp_dev)
    mean_square = totals[0] / total_len
    factor = lax.rsqrt(mean_square + 1e-06)
    scaled = factor / math.sqrt(total_len)
    checks = jnp.stack([mean_square, totals[1] * scaled, totals[2] * scaled])
    return (reversed_field * factor, checks)


def solution(mesh):
    n_outer, n_inner = mesh.shape["outer"], mesh.shape["inner"]

    def body(amplitudes):
        rows_count = amplitudes.shape[1] // COLUMNS
        n_devices = n_outer * n_inner
        if rows_count * n_devices == LANES * LANES and n_devices * SUB == 2 * LANES:
            return fast(n_outer, n_inner, amplitudes)
        return per_device(amplitudes)

    return jax.shard_map(
        body,
        mesh=mesh,
        in_specs=(P(None, ("outer", "inner")),),
        out_specs=(P(None, ("outer", "inner")), P()),
        check_vma=False,
    )
```

```python
import functools
import itertools
import math

import jax
import jax.numpy as jnp
import numpy as np
from jax import lax
from jax.experimental import pallas as pl
from jax.experimental.pallas import tpu as pltpu
from jax.sharding import PartitionSpec as P

WINDOW = 9
COLUMNS = 2**WINDOW
LANES = 128
SUB = 8
RADIX = COLUMNS // LANES
PIECES = ((0,), (1, 2), (3,))
STAT = 1
MESH = pl.DeviceIdType.MESH


def rev(value, count):
    out = 0
    for bit in range(count):
        out |= (value >> bit & 1) << (count - 1 - bit)
    return out


def split_bf16(values):
    high = values.astype(jnp.bfloat16)
    return high, (values - high.astype(np.float32)).astype(jnp.bfloat16)


def tables(n_devices, total_len):
    f = np.arange(COLUMNS).reshape(LANES, RADIX).T
    lane = np.arange(LANES)
    ang = (f[:, :, None] * lane) % COLUMNS * (2.0 * np.pi / COLUMNS)
    c, s = np.cos(ang) / math.sqrt(COLUMNS), np.sin(ang) / math.sqrt(COLUMNS)
    table = np.stack([np.concatenate([c, -s], -1), np.concatenate([s, c], -1)], 2)
    table = table.reshape(RADIX, 2 * LANES, 2 * LANES).astype(np.float32)
    slots = 2.0 * np.pi / total_len * np.arange(n_devices)
    subs = 2.0 * np.pi / total_len * n_devices * RADIX * np.arange(SUB)
    turn = np.zeros((2 * (n_devices + SUB), LANES), np.float32)
    turn[:n_devices], turn[n_devices : 2 * n_devices] = np.cos(slots)[:, None], np.sin(slots)[:, None]
    turn[2 * n_devices : 2 * n_devices + SUB, 1] = np.cos(subs) * math.sqrt(COLUMNS)
    turn[2 * n_devices + SUB :, 1] = np.sin(subs) * math.sqrt(COLUMNS)
    return table, turn


def pieces_of(n_devices):
    rows = [len(chunks) * RADIX * SUB + (k == STAT) for k, chunks in enumerate(PIECES)]
    return rows, [r if r % 2 else r + 4 for r in rows]


def turn_tiles(recv, pitch, place, h, n_devices, factor):
    tile = jnp.concatenate(
        [recv[pl.ds((place * RADIX + rev(j, 2)) * SUB + h, n_devices, stride=pitch), :] for j in range(RADIX)], 0)
    turned = tile.T.reshape(LANES // SUB, SUB, LANES)
    return [turned[m] * factor for m in range(LANES // SUB)]


def kernel(n_outer, n_inner, total_len, x_hbm, th_hbm, tl_hbm, turn_hbm, *refs):
    n_pieces = len(PIECES)
    field, last, tot_ref, fac_ref, x_ref, th_ref, tl_ref, turn_ref, bh_ref, bl_ref = refs[:10]
    sends, recvs = refs[10 : 10 + n_pieces], [*refs[10 + n_pieces : 9 + 2 * n_pieces], last]
    send_sem, recv_sem, own_sem, load_sem = refs[9 + 2 * n_pieces :]
    n_devices = n_outer * n_inner
    obits, ibits = n_outer.bit_length() - 1, n_inner.bit_length() - 1
    span = LANES
    q_rows = span + 4

    loads = []
    for g in range(RADIX):
        for q in range(SUB):
            loads.append(pltpu.make_async_copy(
                x_hbm.at[pl.ds((g * SUB + q) * span, span)],
                x_ref.at[pl.ds((g * SUB + rev(q, 3)) * q_rows, span)], load_sem.at[g]))
    rest = [pltpu.make_async_copy(src, dst, load_sem.at[RADIX + k]) for k, (src, dst) in enumerate(
        [(th_hbm, th_ref), (tl_hbm, tl_ref), (turn_hbm, turn_ref)])]
    for load in loads + rest:
        load.start()

    o, i = lax.axis_index("outer"), lax.axis_index("inner")
    me = o * n_inner + i
    slot = 0
    odelta, idelta = [], []
    for k in range(obits):
        bit = o // 2**k % 2
        slot = slot + bit * 2 ** (obits - 1 - k)
        odelta.append((1 - 2 * bit) * 2**k)
    for k in range(ibits):
        bit = i // 2**k % 2
        slot = slot + bit * 2 ** (ibits - 1 - k) * n_outer
        idelta.append((1 - 2 * bit) * 2**k)

    def peer(mo, mi):
        po, pi = o, i
        for k in range(obits):
            if mo >> k & 1:
                po = po + odelta[k]
        for k in range(ibits):
            if mi >> k & 1:
                pi = pi + idelta[k]
        return po, pi

    half = n_inner // 2
    high = i // half
    far = []
    for t in range(half):
        pi = high * t + (1 - high) * (n_inner - 1 - t)
        far += [(peer(mo, 0)[0], pi) for mo in range(n_outer)]
    near = [peer(mo, mi) for mi in range(half - 1, -1, -1) for mo in range(n_outer) if mo or mi]
    peers = [p for pair in itertools.zip_longest(far, near) for p in pair if p is not None]
    barrier = pltpu.get_barrier_semaphore()
    for p in peers:
        pl.semaphore_signal(barrier, inc=1, device_id=p, device_id_type=MESH)

    rows, pitches = pieces_of(n_devices)

    def send(k):
        dst = recvs[k].at[pl.ds(slot * pitches[k], rows[k])]
        for po, pi in peers:
            pltpu.make_async_remote_copy(
                src_ref=sends[k].at[pl.ds((po * n_inner + pi) * rows[k], rows[k])], dst_ref=dst,
                send_sem=send_sem, recv_sem=recv_sem.at[k],
                device_id=(po, pi), device_id_type=MESH).start()
        own_copy(k).start()

    def own_copy(k):
        return pltpu.make_async_copy(
            sends[k].at[pl.ds(me * rows[k], rows[k])],
            recvs[k].at[pl.ds(slot * pitches[k], rows[k])], own_sem.at[k])

    def wait_rows(ref, count, sem):
        part = ref.at[pl.ds(0, count)]
        pltpu.make_async_copy(part, part, sem).wait()

    def rows_of(g, pair, ct, s):
        return [x_ref[pl.ds(g * SUB * q_rows + (2 * pair + w) * SUB + 2 * ct + s, SUB, stride=q_rows), :] for w in range(2)]

    def keep(chunk, g, pair, values):
        at = pl.ds((g * SUB + pair) * 2 * SUB, 2 * SUB)
        for s, value in enumerate(values):
            high, low = split_bf16(value)
            bh_ref[chunk, at, s * LANES : (s + 1) * LANES] = high
            bl_ref[chunk, at, s * LANES : (s + 1) * LANES] = low

    dims = (((1,), (1,)), ((), ()))

    def transform(k, place, chunk, groups):
        at = pl.ds(groups[0] * LANES, len(groups) * LANES)
        th, tl, bh, bl = th_ref[chunk], tl_ref[chunk], bh_ref[chunk, at, :], bl_ref[chunk, at, :]
        res = lax.dot_general(th, bh, dims, preferred_element_type=jnp.float32)
        res += lax.dot_general(th, bl, dims, preferred_element_type=jnp.float32)
        res += lax.dot_general(tl, bh, dims, preferred_element_type=jnp.float32)
        for e in range(n_devices):
            for n, g in enumerate(groups):
                sends[k][pl.ds(e * rows[k] + (place * RADIX + g) * SUB, SUB), :] = (
                    res[e * SUB : (e + 1) * SUB, n * LANES : (n + 1) * LANES])

    for g in range(RADIX):
        wait_rows(x_ref, SUB * span, load_sem.at[g])
        for pair in range(SUB):
            keep(0, g, pair, [
                jnp.concatenate([(a + c) + (b + d) for a, b, c, d in zip(*[rows_of(g, pair, ct, s) for ct in range(RADIX)])], 0)
                for s in range(2)])
        if g == 0:
            for load in rest:
                load.wait()
        if g % 2:
            transform(0, 0, 0, (g - 1, g))
    pl.semaphore_wait(barrier, len(peers))
    send(0)

    zero = jnp.zeros((SUB, LANES), jnp.float32)
    squares, zr, zi = [zero] * 4, zero, zero
    for g in range(RADIX):
        for pair in range(SUB):
            part = [[rows_of(g, pair, ct, s) for s in range(2)] for ct in range(RADIX)]
            for ct in range(RADIX):
                for s in range(2):
                    for w in range(2):
                        squares[ct] = squares[ct] + part[ct][s][w] * part[ct][s][w]
            for w in range(2):
                angle = 2.0 * math.pi / total_len * n_devices * (rev(2 * pair + w, 4) * SUB * RADIX + rev(g, 2))
                cw, sw = math.cos(angle), math.sin(angle)
                zr = zr + (part[0][0][w] * cw + part[0][1][w] * sw)
                zi = zi + (part[0][1][w] * cw - part[0][0][w] * sw)
            (x0r, x0i), (x1r, x1i), (x2r, x2i), (x3r, x3i) = [
                [jnp.concatenate(part[ct][s], 0) for s in range(2)] for ct in range(RADIX)]
            br, bi, dr, di = x0r - x2r, x0i - x2i, x1r - x3r, x1i - x3i
            keep(1, g, pair, (br - di, bi + dr))
            keep(2, g, pair, ((x0r + x2r) - (x1r + x3r), (x0i + x2i) - (x1i + x3i)))
            keep(3, g, pair, (br + di, bi - dr))

    pc, ps = turn_ref[2 * n_devices : 2 * n_devices + SUB, :], turn_ref[2 * n_devices + SUB :, :]
    oc, os_ = turn_ref[pl.ds(slot, 1), :], turn_ref[pl.ds(n_devices + slot, 1), :]
    total = jnp.sum(jnp.sum((squares[0] + squares[1]) + (squares[2] + squares[3]), 0, keepdims=True), 1, keepdims=True)
    yr = jnp.sum(zr * pc + zi * ps, 0, keepdims=True)
    yi = jnp.sum(zi * pc - zr * ps, 0, keepdims=True)
    wr = jnp.sum(yr * oc + yi * os_, 1, keepdims=True)
    wi = jnp.sum(yi * oc - yr * os_, 1, keepdims=True)
    lane = lax.broadcasted_iota(jnp.int32, (1, LANES), 1)
    stat = jnp.where(lane == 0, total, jnp.where(lane == 1, wr, jnp.where(lane == 2, wi, 0.0)))
    sends[STAT][pl.ds(rows[STAT] - 1, n_devices, stride=rows[STAT]), :] = jnp.broadcast_to(stat, (n_devices, LANES))

    for k, chunks in list(enumerate(PIECES))[1:]:
        for place, chunk in enumerate(chunks):
            transform(k, place, chunk, range(RADIX))
        send(k)

    for k, chunks in enumerate(PIECES):
        wait_rows(recvs[k], len(peers) * rows[k], recv_sem.at[k])
        own_copy(k).wait()
        if k == STAT:
            sums = jnp.sum(recvs[k][pl.ds(rows[k] - 1, n_devices, stride=pitches[k]), :], 0, keepdims=True)
            mean_square = jnp.sum(jnp.where(lane == 0, sums, 0.0), 1, keepdims=True) / total_len
            shifted = mean_square + 1e-06
            factor = lax.rsqrt(shifted)
            factor = factor * (1.5 - 0.5 * shifted * factor * factor)
            checks = jnp.where(lane == 0, mean_square, sums * (factor / math.sqrt(total_len)))
            tot_ref[...] = jnp.broadcast_to(checks, (SUB, LANES))
            factor = jnp.broadcast_to(factor, (SUB, LANES))
            fac_ref[...] = factor
        ready = range(STAT + 1) if k == STAT else [k] if STAT < k < n_pieces - 1 else []
        for kk in ready:
            for place, chunk in enumerate(PIECES[kk]):
                for h in range(SUB):
                    base = ((h // 2) * (RADIX - 1) + chunk) * 2 * LANES + h % 2
                    for m, v in enumerate(turn_tiles(recvs[kk], pitches[kk], place, h, n_devices, factor)):
                        field[pl.ds(base + rev(m, 4) * 2 * SUB, SUB, stride=2), :] = v
    for k in range(n_pieces):
        wait_rows(sends[k], len(peers) * rows[k], send_sem)


def finish_kernel(n_devices, pitch, field, last, tot_ref, fac_ref, out_hbm, checks_ref, turned, sem):
    f_rows = 2 * LANES
    many = (RADIX - 1) * f_rows
    stores = []
    for fq in range(RADIX):
        stores.append(pltpu.make_async_copy(
            field.at[pl.ds(fq * many, many)], out_hbm.at[pl.ds(fq * RADIX * f_rows, many)], sem.at[fq]))
        stores[-1].start()
    checks_ref[...] = tot_ref[0:1, 0:3]
    factor = fac_ref[...]
    for h in range(SUB):
        base = h // 2 * f_rows + h % 2
        for m, v in enumerate(turn_tiles(last, pitch, 0, h, n_devices, factor)):
            turned[pl.ds(base + rev(m, 4) * 2 * SUB, SUB, stride=2), :] = v
        if h % 2:
            fq = h // 2
            stores.append(pltpu.make_async_copy(
                turned.at[pl.ds(fq * f_rows, f_rows)],
                out_hbm.at[pl.ds((fq * RADIX + RADIX - 1) * f_rows, f_rows)], sem.at[RADIX + fq]))
            stores[-1].start()
    for store in stores:
        store.wait()


def fast(n_outer, n_inner, amplitudes):
    amp_dev = amplitudes.shape[1]
    n_devices = n_outer * n_inner
    rows_count = amp_dev // COLUMNS
    total_len = amp_dev * n_devices
    view = amplitudes.reshape(2, amp_dev // LANES, LANES).transpose(1, 0, 2).reshape(-1, LANES)
    table, turn = tables(n_devices, total_len)
    th = table.astype(jnp.bfloat16)
    tl = (table - th.astype(np.float32)).astype(jnp.bfloat16)
    hbm, vmem = pl.BlockSpec(memory_space=pltpu.HBM), pl.BlockSpec(memory_space=pltpu.VMEM)
    rows, pitches = pieces_of(n_devices)
    small = pltpu.VMEM((SUB, LANES), jnp.float32)
    f_rows = 2 * LANES
    pair = pltpu.VMEM((RADIX, rows_count, 2 * LANES), jnp.bfloat16)
    scratch = [
        pltpu.VMEM((RADIX * SUB * (LANES + 4), LANES), jnp.float32),
        pltpu.VMEM(th.shape, jnp.bfloat16),
        pltpu.VMEM(tl.shape, jnp.bfloat16),
        pltpu.VMEM(turn.shape, jnp.float32),
        pair,
        pair,
        *[pltpu.VMEM((n_devices * r, LANES), jnp.float32) for r in rows],
        *[pltpu.VMEM((n_devices * p, LANES), jnp.float32) for p in pitches[:-1]],
        pltpu.SemaphoreType.DMA,
        pltpu.SemaphoreType.DMA((len(PIECES),)),
        pltpu.SemaphoreType.DMA((len(PIECES),)),
        pltpu.SemaphoreType.DMA((RADIX + 3,)),
    ]
    parts = pl.pallas_call(
        functools.partial(kernel, n_outer, n_inner, total_len),
        out_shape=(
            pltpu.VMEM((RADIX * (RADIX - 1) * f_rows, LANES), jnp.float32),
            pltpu.VMEM((n_devices * pitches[-1], LANES), jnp.float32),
            small,
            small,
        ),
        in_specs=[hbm] * 4,
        out_specs=(vmem,) * 4,
        scratch_shapes=scratch,
        compiler_params=pltpu.CompilerParams(collective_id=0, has_side_effects=True, vmem_limit_bytes=32_000_000),
    )(*[pltpu.with_memory_space_constraint(v, pltpu.HBM) for v in (view, jnp.asarray(th), jnp.asarray(tl), jnp.asarray(turn))])
    field, checks = pl.pallas_call(
        functools.partial(finish_kernel, n_devices, pitches[-1]),
        out_shape=(jax.ShapeDtypeStruct(view.shape, jnp.float32), jax.ShapeDtypeStruct((1, 3), jnp.float32)),
        in_specs=[vmem] * 4,
        out_specs=(hbm, vmem),
        scratch_shapes=[
            pltpu.VMEM((RADIX * f_rows, LANES), jnp.float32),
            pltpu.SemaphoreType.DMA((2 * RADIX,)),
        ],
        compiler_params=pltpu.CompilerParams(vmem_limit_bytes=32_000_000),
    )(*parts)
    result = field.reshape(-1, 2, LANES).transpose(1, 0, 2).reshape(2, amp_dev)
    return result, checks.reshape(3)


def reverse_index(values, count):
    result = jnp.zeros_like(values)
    for bit_pos in range(count):
        result = result | (values >> bit_pos & 1) << count - 1 - bit_pos
    return result


def reversal_table(size, count):
    indices = jnp.arange(size, dtype=jnp.int32)
    return (reverse_index(indices, count)[:, None] == indices[None, :]).astype(jnp.float32)


def check_terms(current, positions, angle_scale):
    angles = positions.astype(jnp.float32) * angle_scale
    cosine = jnp.cos(angles)
    sine = jnp.sin(angles)
    squares = jnp.sum(current * current)
    phase_real = jnp.sum(current[0] * cosine + current[1] * sine)
    phase_imag = jnp.sum(current[1] * cosine - current[0] * sine)
    return (squares, phase_real, phase_imag)


def per_device(amplitudes):
    amp_dev = amplitudes.shape[1]
    n_outer = lax.axis_size("outer")
    n_inner = lax.axis_size("inner")
    outer_bits = n_outer.bit_length() - 1
    inner_bits = n_inner.bit_length() - 1
    global_bits = outer_bits + inner_bits
    local_bits = amp_dev.bit_length() - 1
    n_devices = n_outer * n_inner
    high_count = amp_dev // n_devices
    total_len = amp_dev * n_devices
    columns = 2**WINDOW
    rows_count = amp_dev // columns
    column_ids = jnp.arange(columns, dtype=jnp.int32)
    reversed_ids = reverse_index(column_ids, WINDOW)
    products = column_ids[:, None] * reversed_ids[None, :] % columns
    angles = products.astype(jnp.float32) * (2.0 * math.pi / columns)
    real_part = jnp.cos(angles) / math.sqrt(columns)
    imag_part = jnp.sin(angles) / math.sqrt(columns)
    table = jnp.concatenate(
        [jnp.concatenate([real_part, imag_part], 1), jnp.concatenate([-imag_part, real_part], 1)], 0
    )
    stacked = jnp.concatenate(
        [amplitudes[0].reshape(rows_count, columns), amplitudes[1].reshape(rows_count, columns)], 1
    )
    result = jnp.dot(
        stacked, table, precision=lax.Precision.HIGHEST, preferred_element_type=jnp.float32
    )
    windowed = jnp.stack([result[:, :columns].reshape(-1), result[:, columns:].reshape(-1)])
    device_id = lax.axis_index("outer") * n_inner + lax.axis_index("inner")
    angle_scale = 2.0 * math.pi / total_len
    local_ids = jnp.arange(amp_dev, dtype=jnp.int32)
    positions = reverse_index(device_id * amp_dev + local_ids, local_bits + global_bits)
    totals = lax.psum(check_terms(windowed, positions, angle_scale), ("outer", "inner"))
    device_table = reversal_table(n_devices, global_bits)
    high_table = reversal_table(high_count, local_bits - global_bits)
    grid = windowed.reshape(2, high_count, n_devices)
    ordered = jnp.einsum("pm,shm->sph", device_table, grid, precision=lax.Precision.HIGHEST)
    blocks = ordered.reshape(2, n_outer, n_inner, high_count)
    blocks = lax.all_to_all(
        lax.all_to_all(blocks, "outer", split_axis=1, concat_axis=1, tiled=True),
        "inner",
        split_axis=2,
        concat_axis=2,
        tiled=True,
    )
    received = blocks.reshape(2, n_devices, high_count)
    turned_high = jnp.einsum("qh,sdh->sdq", high_table, received, precision=lax.Precision.HIGHEST)
    placed = jnp.einsum("ed,sdq->sqe", device_table, turned_high, precision=lax.Precision.HIGHEST)
    reversed_field = placed.reshape(2, amp_dev)
    mean_square = totals[0] / total_len
    factor = lax.rsqrt(mean_square + 1e-06)
    scaled = factor / math.sqrt(total_len)
    checks = jnp.stack([mean_square, totals[1] * scaled, totals[2] * scaled])
    return (reversed_field * factor, checks)


def solution(mesh):
    n_outer, n_inner = mesh.shape["outer"], mesh.shape["inner"]

    def body(amplitudes):
        rows_count = amplitudes.shape[1] // COLUMNS
        n_devices = n_outer * n_inner
        if rows_count * n_devices == LANES * LANES and n_devices * SUB == 2 * LANES:
            return fast(n_outer, n_inner, amplitudes)
        return per_device(amplitudes)

    return jax.shard_map(
        body,
        mesh=mesh,
        in_specs=(P(None, ("outer", "inner")),),
        out_specs=(P(None, ("outer", "inner")), P()),
        check_vma=False,
    )
```

```python
import functools
import itertools
import math

import jax
import jax.numpy as jnp
import numpy as np
from jax import lax
from jax.experimental import pallas as pl
from jax.experimental.pallas import tpu as pltpu
from jax.sharding import PartitionSpec as P

WINDOW = 9
COLUMNS = 2**WINDOW
LANES = 128
SUB = 8
RADIX = COLUMNS // LANES
PIECES = ((0,), (1, 2), (3,))
STAT = 1
MESH = pl.DeviceIdType.MESH


def rev(value, count):
    out = 0
    for bit in range(count):
        out |= (value >> bit & 1) << (count - 1 - bit)
    return out


def split_bf16(values):
    high = values.astype(jnp.bfloat16)
    return high, (values - high.astype(np.float32)).astype(jnp.bfloat16)


def tables(n_devices, total_len):
    f = np.arange(COLUMNS).reshape(LANES, RADIX).T
    lane = np.arange(LANES)
    ang = (f[:, :, None] * lane) % COLUMNS * (2.0 * np.pi / COLUMNS)
    c, s = np.cos(ang) / math.sqrt(COLUMNS), np.sin(ang) / math.sqrt(COLUMNS)
    table = np.stack([np.concatenate([c, -s], -1), np.concatenate([s, c], -1)], 2)
    table = table.reshape(RADIX, 2 * LANES, 2 * LANES).astype(np.float32)
    slots = 2.0 * np.pi / total_len * np.arange(n_devices)
    subs = 2.0 * np.pi / total_len * n_devices * RADIX * np.arange(SUB)
    turn = np.zeros((2 * (n_devices + SUB), LANES), np.float32)
    turn[:n_devices], turn[n_devices : 2 * n_devices] = np.cos(slots)[:, None], np.sin(slots)[:, None]
    turn[2 * n_devices : 2 * n_devices + SUB, 1] = np.cos(subs) * math.sqrt(COLUMNS)
    turn[2 * n_devices + SUB :, 1] = np.sin(subs) * math.sqrt(COLUMNS)
    return table, turn


def pieces_of(n_devices):
    rows = [len(chunks) * RADIX * SUB + (k == STAT) for k, chunks in enumerate(PIECES)]
    return rows, [r if r % 2 else r + 4 for r in rows]


def turn_tiles(recv, pitch, place, h, n_devices, factor):
    tile = jnp.concatenate(
        [recv[pl.ds((place * RADIX + rev(j, 2)) * SUB + h, n_devices, stride=pitch), :] for j in range(RADIX)], 0)
    turned = tile.T.reshape(LANES // SUB, SUB, LANES)
    return [turned[m] * factor for m in range(LANES // SUB)]


def kernel(n_outer, n_inner, total_len, x_hbm, th_hbm, tl_hbm, turn_hbm, *refs):
    n_pieces = len(PIECES)
    field, last, tot_ref, fac_ref, x_ref, th_ref, tl_ref, turn_ref, bh_ref, bl_ref = refs[:10]
    sends, recvs = refs[10 : 10 + n_pieces], [*refs[10 + n_pieces : 9 + 2 * n_pieces], last]
    send_sem, recv_sem, own_sem, load_sem, second_sem, third_sem = refs[9 + 2 * n_pieces :]
    n_devices = n_outer * n_inner
    obits, ibits = n_outer.bit_length() - 1, n_inner.bit_length() - 1
    span = LANES
    q_rows = span + 4

    loads = []
    for g in range(RADIX):
        for q in range(SUB):
            loads.append(pltpu.make_async_copy(
                x_hbm.at[pl.ds((g * SUB + q) * span, span)],
                x_ref.at[pl.ds((g * SUB + rev(q, 3)) * q_rows, span)], load_sem.at[g]))
    rest = [pltpu.make_async_copy(src, dst, load_sem.at[RADIX + k]) for k, (src, dst) in enumerate(
        [(th_hbm, th_ref), (tl_hbm, tl_ref), (turn_hbm, turn_ref)])]
    for load in loads + rest:
        load.start()

    o, i = lax.axis_index("outer"), lax.axis_index("inner")
    me = o * n_inner + i
    slot = 0
    odelta, idelta = [], []
    for k in range(obits):
        bit = o // 2**k % 2
        slot = slot + bit * 2 ** (obits - 1 - k)
        odelta.append((1 - 2 * bit) * 2**k)
    for k in range(ibits):
        bit = i // 2**k % 2
        slot = slot + bit * 2 ** (ibits - 1 - k) * n_outer
        idelta.append((1 - 2 * bit) * 2**k)

    def peer(mo, mi):
        po, pi = o, i
        for k in range(obits):
            if mo >> k & 1:
                po = po + odelta[k]
        for k in range(ibits):
            if mi >> k & 1:
                pi = pi + idelta[k]
        return po, pi

    wide = n_inner // 4
    level, place_in = i // wide, i % wide
    high = level // 2
    across = level + 1 - 2 * (level % 2)
    group = n_outer * wide

    def members(at):
        return [(peer(mo, 0)[0], at * wide + lax.rem(place_in + t, wide)) for t in range(wide) for mo in range(n_outer)]

    def pairs(far, near):
        return [p for pair in itertools.zip_longest(far, near) for p in pair if p is not None]

    own = members(level)[1:]
    first = pairs(members(2 - high), own) + members((1 - high) * across)
    second = members(high * across + (1 - high) * 3)
    order = pairs(members((1 - high) * 3) + members(2 - high), own + members(across))

    barrier = pltpu.get_barrier_semaphore()

    def greet(ring, at, who=None):
        for p in members(at) if who is None else who:
            pl.semaphore_signal(ring, inc=1, device_id=p, device_id_type=MESH)

    greet(barrier, level, own)
    for later in range(1, 4):
        pl.when((level < later) & (later > 1) | (high == 0) & (later == 1))(
            functools.partial(greet, barrier, across if later == 1 else later))

    def meet():
        pl.semaphore_wait(barrier, group - 1 + jnp.where(high == 0, group, level * group))
        for later, sem in ((2, second_sem), (3, third_sem)):
            for earlier in range(later):
                pl.when(level == later)(functools.partial(greet, sem, earlier))
        pl.when(high == 0)(lambda: pl.semaphore_wait(second_sem, group))

    def meet_last():
        pl.when(level < 3)(lambda: pl.semaphore_wait(third_sem, group))

    rows, pitches = pieces_of(n_devices)

    def send(k, peers):
        dst = recvs[k].at[pl.ds(slot * pitches[k], rows[k])]
        for po, pi in peers:
            pltpu.make_async_remote_copy(
                src_ref=sends[k].at[pl.ds((po * n_inner + pi) * rows[k], rows[k])], dst_ref=dst,
                send_sem=send_sem, recv_sem=recv_sem.at[k],
                device_id=(po, pi), device_id_type=MESH).start()

    def own_copy(k):
        return pltpu.make_async_copy(
            sends[k].at[pl.ds(me * rows[k], rows[k])],
            recvs[k].at[pl.ds(slot * pitches[k], rows[k])], own_sem.at[k])

    def wait_rows(ref, count, sem):
        part = ref.at[pl.ds(0, count)]
        pltpu.make_async_copy(part, part, sem).wait()

    def rows_of(g, pair, ct, s):
        return [x_ref[pl.ds(g * SUB * q_rows + (2 * pair + w) * SUB + 2 * ct + s, SUB, stride=q_rows), :] for w in range(2)]

    def keep(chunk, g, pair, values):
        at = pl.ds((g * SUB + pair) * 2 * SUB, 2 * SUB)
        for s, value in enumerate(values):
            high, low = split_bf16(value)
            bh_ref[chunk, at, s * LANES : (s + 1) * LANES] = high
            bl_ref[chunk, at, s * LANES : (s + 1) * LANES] = low

    dims = (((1,), (1,)), ((), ()))

    def transform(k, place, chunk, groups):
        at = pl.ds(groups[0] * LANES, len(groups) * LANES)
        th, tl, bh, bl = th_ref[chunk], tl_ref[chunk], bh_ref[chunk, at, :], bl_ref[chunk, at, :]
        res = lax.dot_general(th, bh, dims, preferred_element_type=jnp.float32)
        res += lax.dot_general(th, bl, dims, preferred_element_type=jnp.float32)
        res += lax.dot_general(tl, bh, dims, preferred_element_type=jnp.float32)
        for e in range(n_devices):
            for n, g in enumerate(groups):
                sends[k][pl.ds(e * rows[k] + (place * RADIX + g) * SUB, SUB), :] = (
                    res[e * SUB : (e + 1) * SUB, n * LANES : (n + 1) * LANES])

    for g in range(RADIX):
        wait_rows(x_ref, SUB * span, load_sem.at[g])
        for pair in range(SUB):
            keep(0, g, pair, [
                jnp.concatenate([(a + c) + (b + d) for a, b, c, d in zip(*[rows_of(g, pair, ct, s) for ct in range(RADIX)])], 0)
                for s in range(2)])
        if g == 0:
            for load in rest:
                load.wait()
        if g % 2:
            transform(0, 0, 0, (g - 1, g))
    meet()
    send(0, first)
    meet_last()
    send(0, second)
    own_copy(0).start()

    zero = jnp.zeros((SUB, LANES), jnp.float32)
    squares, zr, zi = [zero] * 4, zero, zero
    for g in range(RADIX):
        for pair in range(SUB):
            part = [[rows_of(g, pair, ct, s) for s in range(2)] for ct in range(RADIX)]
            for ct in range(RADIX):
                for s in range(2):
                    for w in range(2):
                        squares[ct] = squares[ct] + part[ct][s][w] * part[ct][s][w]
            for w in range(2):
                angle = 2.0 * math.pi / total_len * n_devices * (rev(2 * pair + w, 4) * SUB * RADIX + rev(g, 2))
                cw, sw = math.cos(angle), math.sin(angle)
                zr = zr + (part[0][0][w] * cw + part[0][1][w] * sw)
                zi = zi + (part[0][1][w] * cw - part[0][0][w] * sw)
            (x0r, x0i), (x1r, x1i), (x2r, x2i), (x3r, x3i) = [
                [jnp.concatenate(part[ct][s], 0) for s in range(2)] for ct in range(RADIX)]
            br, bi, dr, di = x0r - x2r, x0i - x2i, x1r - x3r, x1i - x3i
            keep(1, g, pair, (br - di, bi + dr))
            keep(2, g, pair, ((x0r + x2r) - (x1r + x3r), (x0i + x2i) - (x1i + x3i)))
            keep(3, g, pair, (br + di, bi - dr))

    pc, ps = turn_ref[2 * n_devices : 2 * n_devices + SUB, :], turn_ref[2 * n_devices + SUB :, :]
    oc, os_ = turn_ref[pl.ds(slot, 1), :], turn_ref[pl.ds(n_devices + slot, 1), :]
    total = jnp.sum(jnp.sum((squares[0] + squares[1]) + (squares[2] + squares[3]), 0, keepdims=True), 1, keepdims=True)
    yr = jnp.sum(zr * pc + zi * ps, 0, keepdims=True)
    yi = jnp.sum(zi * pc - zr * ps, 0, keepdims=True)
    wr = jnp.sum(yr * oc + yi * os_, 1, keepdims=True)
    wi = jnp.sum(yi * oc - yr * os_, 1, keepdims=True)
    lane = lax.broadcasted_iota(jnp.int32, (1, LANES), 1)
    stat = jnp.where(lane == 0, total, jnp.where(lane == 1, wr, jnp.where(lane == 2, wi, 0.0)))
    sends[STAT][pl.ds(rows[STAT] - 1, n_devices, stride=rows[STAT]), :] = jnp.broadcast_to(stat, (n_devices, LANES))

    for k, chunks in list(enumerate(PIECES))[1:]:
        for place, chunk in enumerate(chunks):
            transform(k, place, chunk, range(RADIX))
        send(k, order)
        own_copy(k).start()

    for k, chunks in enumerate(PIECES):
        wait_rows(recvs[k], (n_devices - 1) * rows[k], recv_sem.at[k])
        own_copy(k).wait()
        if k == STAT:
            sums = jnp.sum(recvs[k][pl.ds(rows[k] - 1, n_devices, stride=pitches[k]), :], 0, keepdims=True)
            mean_square = jnp.sum(jnp.where(lane == 0, sums, 0.0), 1, keepdims=True) / total_len
            shifted = mean_square + 1e-06
            factor = lax.rsqrt(shifted)
            factor = factor * (1.5 - 0.5 * shifted * factor * factor)
            checks = jnp.where(lane == 0, mean_square, sums * (factor / math.sqrt(total_len)))
            tot_ref[...] = jnp.broadcast_to(checks, (SUB, LANES))
            factor = jnp.broadcast_to(factor, (SUB, LANES))
            fac_ref[...] = factor
        ready = range(STAT + 1) if k == STAT else [k] if STAT < k < n_pieces - 1 else []
        for kk in ready:
            for place, chunk in enumerate(PIECES[kk]):
                for h in range(SUB):
                    base = ((h // 2) * (RADIX - 1) + chunk) * 2 * LANES + h % 2
                    for m, v in enumerate(turn_tiles(recvs[kk], pitches[kk], place, h, n_devices, factor)):
                        field[pl.ds(base + rev(m, 4) * 2 * SUB, SUB, stride=2), :] = v
    for k in range(n_pieces):
        wait_rows(sends[k], (n_devices - 1) * rows[k], send_sem)


def finish_kernel(n_devices, pitch, field, last, tot_ref, fac_ref, out_hbm, checks_hbm, turned, checks_ref, sem):
    f_rows = 2 * LANES
    many = (RADIX - 1) * f_rows
    stores = []
    for fq in range(RADIX):
        stores.append(pltpu.make_async_copy(
            field.at[pl.ds(fq * many, many)], out_hbm.at[pl.ds(fq * RADIX * f_rows, many)], sem.at[fq]))
        stores[-1].start()
    checks_ref[...] = tot_ref[0:1, 0:3]
    stores.append(pltpu.make_async_copy(checks_ref, checks_hbm, sem.at[2 * RADIX]))
    stores[-1].start()
    factor = fac_ref[...]
    for h in range(SUB):
        base = h // 2 * f_rows + h % 2
        for m, v in enumerate(turn_tiles(last, pitch, 0, h, n_devices, factor)):
            turned[pl.ds(base + rev(m, 4) * 2 * SUB, SUB, stride=2), :] = v
        if h % 2:
            fq = h // 2
            stores.append(pltpu.make_async_copy(
                turned.at[pl.ds(fq * f_rows, f_rows)],
                out_hbm.at[pl.ds((fq * RADIX + RADIX - 1) * f_rows, f_rows)], sem.at[RADIX + fq]))
            stores[-1].start()
    for store in stores:
        store.wait()


def fast(n_outer, n_inner, amplitudes):
    amp_dev = amplitudes.shape[1]
    n_devices = n_outer * n_inner
    rows_count = amp_dev // COLUMNS
    total_len = amp_dev * n_devices
    view = amplitudes.reshape(2, amp_dev // LANES, LANES).transpose(1, 0, 2).reshape(-1, LANES)
    table, turn = tables(n_devices, total_len)
    th = table.astype(jnp.bfloat16)
    tl = (table - th.astype(np.float32)).astype(jnp.bfloat16)
    hbm, vmem = pl.BlockSpec(memory_space=pltpu.HBM), pl.BlockSpec(memory_space=pltpu.VMEM)
    rows, pitches = pieces_of(n_devices)
    small = pltpu.VMEM((SUB, LANES), jnp.float32)
    f_rows = 2 * LANES
    pair = pltpu.VMEM((RADIX, rows_count, 2 * LANES), jnp.bfloat16)
    scratch = [
        pltpu.VMEM((RADIX * SUB * (LANES + 4), LANES), jnp.float32),
        pltpu.VMEM(th.shape, jnp.bfloat16),
        pltpu.VMEM(tl.shape, jnp.bfloat16),
        pltpu.VMEM(turn.shape, jnp.float32),
        pair,
        pair,
        *[pltpu.VMEM((n_devices * r, LANES), jnp.float32) for r in rows],
        *[pltpu.VMEM((n_devices * p, LANES), jnp.float32) for p in pitches[:-1]],
        pltpu.SemaphoreType.DMA,
        pltpu.SemaphoreType.DMA((len(PIECES),)),
        pltpu.SemaphoreType.DMA((len(PIECES),)),
        pltpu.SemaphoreType.DMA((RADIX + 3,)),
        pltpu.SemaphoreType.REGULAR,
        pltpu.SemaphoreType.REGULAR,
    ]
    parts = pl.pallas_call(
        functools.partial(kernel, n_outer, n_inner, total_len),
        out_shape=(
            pltpu.VMEM((RADIX * (RADIX - 1) * f_rows, LANES), jnp.float32),
            pltpu.VMEM((n_devices * pitches[-1], LANES), jnp.float32),
            small,
            small,
        ),
        in_specs=[hbm] * 4,
        out_specs=(vmem,) * 4,
        scratch_shapes=scratch,
        compiler_params=pltpu.CompilerParams(collective_id=0, has_side_effects=True, vmem_limit_bytes=32_000_000),
    )(*[pltpu.with_memory_space_constraint(v, pltpu.HBM) for v in (view, jnp.asarray(th), jnp.asarray(tl), jnp.asarray(turn))])
    field, checks = pl.pallas_call(
        functools.partial(finish_kernel, n_devices, pitches[-1]),
        out_shape=(jax.ShapeDtypeStruct(view.shape, jnp.float32), jax.ShapeDtypeStruct((1, 3), jnp.float32)),
        in_specs=[vmem] * 4,
        out_specs=(hbm, hbm),
        scratch_shapes=[
            pltpu.VMEM((RADIX * f_rows, LANES), jnp.float32),
            pltpu.VMEM((1, 3), jnp.float32),
            pltpu.SemaphoreType.DMA((2 * RADIX + 1,)),
        ],
        compiler_params=pltpu.CompilerParams(vmem_limit_bytes=32_000_000),
    )(*parts)
    result = field.reshape(-1, 2, LANES).transpose(1, 0, 2).reshape(2, amp_dev)
    return result, checks.reshape(3)


def reverse_index(values, count):
    result = jnp.zeros_like(values)
    for bit_pos in range(count):
        result = result | (values >> bit_pos & 1) << count - 1 - bit_pos
    return result


def reversal_table(size, count):
    indices = jnp.arange(size, dtype=jnp.int32)
    return (reverse_index(indices, count)[:, None] == indices[None, :]).astype(jnp.float32)


def check_terms(current, positions, angle_scale):
    angles = positions.astype(jnp.float32) * angle_scale
    cosine = jnp.cos(angles)
    sine = jnp.sin(angles)
    squares = jnp.sum(current * current)
    phase_real = jnp.sum(current[0] * cosine + current[1] * sine)
    phase_imag = jnp.sum(current[1] * cosine - current[0] * sine)
    return (squares, phase_real, phase_imag)


def per_device(amplitudes):
    amp_dev = amplitudes.shape[1]
    n_outer = lax.axis_size("outer")
    n_inner = lax.axis_size("inner")
    outer_bits = n_outer.bit_length() - 1
    inner_bits = n_inner.bit_length() - 1
    global_bits = outer_bits + inner_bits
    local_bits = amp_dev.bit_length() - 1
    n_devices = n_outer * n_inner
    high_count = amp_dev // n_devices
    total_len = amp_dev * n_devices
    columns = 2**WINDOW
    rows_count = amp_dev // columns
    column_ids = jnp.arange(columns, dtype=jnp.int32)
    reversed_ids = reverse_index(column_ids, WINDOW)
    products = column_ids[:, None] * reversed_ids[None, :] % columns
    angles = products.astype(jnp.float32) * (2.0 * math.pi / columns)
    real_part = jnp.cos(angles) / math.sqrt(columns)
    imag_part = jnp.sin(angles) / math.sqrt(columns)
    table = jnp.concatenate(
        [jnp.concatenate([real_part, imag_part], 1), jnp.concatenate([-imag_part, real_part], 1)], 0
    )
    stacked = jnp.concatenate(
        [amplitudes[0].reshape(rows_count, columns), amplitudes[1].reshape(rows_count, columns)], 1
    )
    result = jnp.dot(
        stacked, table, precision=lax.Precision.HIGHEST, preferred_element_type=jnp.float32
    )
    windowed = jnp.stack([result[:, :columns].reshape(-1), result[:, columns:].reshape(-1)])
    device_id = lax.axis_index("outer") * n_inner + lax.axis_index("inner")
    angle_scale = 2.0 * math.pi / total_len
    local_ids = jnp.arange(amp_dev, dtype=jnp.int32)
    positions = reverse_index(device_id * amp_dev + local_ids, local_bits + global_bits)
    totals = lax.psum(check_terms(windowed, positions, angle_scale), ("outer", "inner"))
    device_table = reversal_table(n_devices, global_bits)
    high_table = reversal_table(high_count, local_bits - global_bits)
    grid = windowed.reshape(2, high_count, n_devices)
    ordered = jnp.einsum("pm,shm->sph", device_table, grid, precision=lax.Precision.HIGHEST)
    blocks = ordered.reshape(2, n_outer, n_inner, high_count)
    blocks = lax.all_to_all(
        lax.all_to_all(blocks, "outer", split_axis=1, concat_axis=1, tiled=True),
        "inner",
        split_axis=2,
        concat_axis=2,
        tiled=True,
    )
    received = blocks.reshape(2, n_devices, high_count)
    turned_high = jnp.einsum("qh,sdh->sdq", high_table, received, precision=lax.Precision.HIGHEST)
    placed = jnp.einsum("ed,sdq->sqe", device_table, turned_high, precision=lax.Precision.HIGHEST)
    reversed_field = placed.reshape(2, amp_dev)
    mean_square = totals[0] / total_len
    factor = lax.rsqrt(mean_square + 1e-06)
    scaled = factor / math.sqrt(total_len)
    checks = jnp.stack([mean_square, totals[1] * scaled, totals[2] * scaled])
    return (reversed_field * factor, checks)


def solution(mesh):
    n_outer, n_inner = mesh.shape["outer"], mesh.shape["inner"]

    def body(amplitudes):
        rows_count = amplitudes.shape[1] // COLUMNS
        n_devices = n_outer * n_inner
        if rows_count * n_devices == LANES * LANES and n_devices * SUB == 2 * LANES and n_inner % 4 == 0:
            return fast(n_outer, n_inner, amplitudes)
        return per_device(amplitudes)

    return jax.shard_map(
        body,
        mesh=mesh,
        in_specs=(P(None, ("outer", "inner")),),
        out_specs=(P(None, ("outer", "inner")), P()),
        check_vma=False,
    )
```

```python
import functools
import itertools
import math

import jax
import jax.numpy as jnp
import numpy as np
from jax import lax
from jax.experimental import pallas as pl
from jax.experimental.pallas import tpu as pltpu
from jax.sharding import PartitionSpec as P

WINDOW = 9
COLUMNS = 2**WINDOW
LANES = 128
SUB = 8
RADIX = COLUMNS // LANES
PIECES = ((0,), (1, 2), (3,))
STAT = 1
MESH = pl.DeviceIdType.MESH


def rev(value, count):
    out = 0
    for bit in range(count):
        out |= (value >> bit & 1) << (count - 1 - bit)
    return out


def split_bf16(values):
    high = values.astype(jnp.bfloat16)
    return high, (values - high.astype(np.float32)).astype(jnp.bfloat16)


def tables(n_devices, total_len):
    f = np.arange(COLUMNS).reshape(LANES, RADIX).T
    lane = np.arange(LANES)
    ang = (f[:, :, None] * lane) % COLUMNS * (2.0 * np.pi / COLUMNS)
    c, s = np.cos(ang) / math.sqrt(COLUMNS), np.sin(ang) / math.sqrt(COLUMNS)
    table = np.stack([np.concatenate([c, -s], -1), np.concatenate([s, c], -1)], 2)
    table = table.reshape(RADIX, 2 * LANES, 2 * LANES).astype(np.float32)
    slots = 2.0 * np.pi / total_len * np.arange(n_devices)
    subs = 2.0 * np.pi / total_len * n_devices * RADIX * np.arange(SUB)
    turn = np.zeros((2 * (n_devices + SUB), LANES), np.float32)
    turn[:n_devices], turn[n_devices : 2 * n_devices] = np.cos(slots)[:, None], np.sin(slots)[:, None]
    turn[2 * n_devices : 2 * n_devices + SUB, 1] = np.cos(subs) * math.sqrt(COLUMNS)
    turn[2 * n_devices + SUB :, 1] = np.sin(subs) * math.sqrt(COLUMNS)
    return table, turn


def pieces_of(n_devices):
    rows = [len(chunks) * RADIX * SUB + (k == STAT) for k, chunks in enumerate(PIECES)]
    return rows, [r if r % 2 else r + 4 for r in rows]


def turn_tiles(recv, pitch, place, h, n_devices, factor):
    tile = jnp.concatenate(
        [recv[pl.ds((place * RADIX + rev(j, 2)) * SUB + h, n_devices, stride=pitch), :] for j in range(RADIX)], 0)
    turned = tile.T.reshape(LANES // SUB, SUB, LANES)
    return [turned[m] * factor for m in range(LANES // SUB)]


def kernel(n_outer, n_inner, total_len, x_hbm, th_hbm, tl_hbm, turn_hbm, *refs):
    n_pieces = len(PIECES)
    field, last, tot_ref, fac_ref, x_ref, th_ref, tl_ref, turn_ref, bh_ref, bl_ref = refs[:10]
    sends, recvs = refs[10 : 10 + n_pieces], [*refs[10 + n_pieces : 9 + 2 * n_pieces], last]
    send_sem, recv_sem, own_sem, load_sem, last_sem = refs[9 + 2 * n_pieces :]
    n_devices = n_outer * n_inner
    obits, ibits = n_outer.bit_length() - 1, n_inner.bit_length() - 1
    span = LANES
    q_rows = span + 4

    loads = []
    for g in range(RADIX):
        for q in range(SUB):
            loads.append(pltpu.make_async_copy(
                x_hbm.at[pl.ds((g * SUB + q) * span, span)],
                x_ref.at[pl.ds((g * SUB + rev(q, 3)) * q_rows, span)], load_sem.at[g]))
    rest = [pltpu.make_async_copy(src, dst, load_sem.at[RADIX + k]) for k, (src, dst) in enumerate(
        [(th_hbm, th_ref), (tl_hbm, tl_ref), (turn_hbm, turn_ref)])]
    for load in loads + rest:
        load.start()

    o, i = lax.axis_index("outer"), lax.axis_index("inner")
    me = o * n_inner + i
    slot = 0
    odelta, idelta = [], []
    for k in range(obits):
        bit = o // 2**k % 2
        slot = slot + bit * 2 ** (obits - 1 - k)
        odelta.append((1 - 2 * bit) * 2**k)
    for k in range(ibits):
        bit = i // 2**k % 2
        slot = slot + bit * 2 ** (ibits - 1 - k) * n_outer
        idelta.append((1 - 2 * bit) * 2**k)

    def peer(mo, mi):
        po, pi = o, i
        for k in range(obits):
            if mo >> k & 1:
                po = po + odelta[k]
        for k in range(ibits):
            if mi >> k & 1:
                pi = pi + idelta[k]
        return po, pi

    wide = n_inner // 4
    level, place_in = i // wide, i % wide
    high = level // 2
    across = level + 1 - 2 * (level % 2)
    group = n_outer * wide

    def members(at):
        return [(peer(mo, 0)[0], at * wide + lax.rem(place_in + t, wide)) for t in range(wide) for mo in range(n_outer)]

    def pairs(far, near):
        return [p for pair in itertools.zip_longest(far, near) for p in pair if p is not None]

    own = members(level)[1:]
    first = pairs(members(2 - high), own) + members((1 - high) * across)
    second = members(high * across + (1 - high) * 3)
    order = pairs(members((1 - high) * 3) + members(2 - high), own + members(across))

    barrier = pltpu.get_barrier_semaphore()

    def greet(ring, at, who=None):
        for p in members(at) if who is None else who:
            pl.semaphore_signal(ring, inc=1, device_id=p, device_id_type=MESH)

    greet(barrier, level, own)
    for t in range(1, 4):
        pl.when(level < 3)(functools.partial(greet, barrier, lax.rem(level + t, 4)))

    def meet():
        pl.semaphore_wait(barrier, 3 * group - 1 + group * (level // 3))
        for earlier in (2, 1, 0):
            pl.when(level == 3)(functools.partial(greet, last_sem, earlier))

    def meet_last():
        pl.when(level < 3)(lambda: pl.semaphore_wait(last_sem, group))

    rows, pitches = pieces_of(n_devices)

    def send(k, peers):
        dst = recvs[k].at[pl.ds(slot * pitches[k], rows[k])]
        for po, pi in peers:
            pltpu.make_async_remote_copy(
                src_ref=sends[k].at[pl.ds((po * n_inner + pi) * rows[k], rows[k])], dst_ref=dst,
                send_sem=send_sem, recv_sem=recv_sem.at[k],
                device_id=(po, pi), device_id_type=MESH).start()

    def own_copy(k):
        return pltpu.make_async_copy(
            sends[k].at[pl.ds(me * rows[k], rows[k])],
            recvs[k].at[pl.ds(slot * pitches[k], rows[k])], own_sem.at[k])

    def wait_rows(ref, count, sem):
        part = ref.at[pl.ds(0, count)]
        pltpu.make_async_copy(part, part, sem).wait()

    def rows_of(g, pair, ct, s):
        return [x_ref[pl.ds(g * SUB * q_rows + (2 * pair + w) * SUB + 2 * ct + s, SUB, stride=q_rows), :] for w in range(2)]

    def keep(chunk, g, pair, values):
        at = pl.ds((g * SUB + pair) * 2 * SUB, 2 * SUB)
        for s, value in enumerate(values):
            high, low = split_bf16(value)
            bh_ref[chunk, at, s * LANES : (s + 1) * LANES] = high
            bl_ref[chunk, at, s * LANES : (s + 1) * LANES] = low

    dims = (((1,), (1,)), ((), ()))

    def transform(k, place, chunk, groups):
        at = pl.ds(groups[0] * LANES, len(groups) * LANES)
        th, tl, bh, bl = th_ref[chunk], tl_ref[chunk], bh_ref[chunk, at, :], bl_ref[chunk, at, :]
        res = lax.dot_general(th, bh, dims, preferred_element_type=jnp.float32)
        res += lax.dot_general(th, bl, dims, preferred_element_type=jnp.float32)
        res += lax.dot_general(tl, bh, dims, preferred_element_type=jnp.float32)
        for e in range(n_devices):
            for n, g in enumerate(groups):
                sends[k][pl.ds(e * rows[k] + (place * RADIX + g) * SUB, SUB), :] = (
                    res[e * SUB : (e + 1) * SUB, n * LANES : (n + 1) * LANES])

    for g in range(RADIX):
        wait_rows(x_ref, SUB * span, load_sem.at[g])
        for pair in range(SUB):
            keep(0, g, pair, [
                jnp.concatenate([(a + c) + (b + d) for a, b, c, d in zip(*[rows_of(g, pair, ct, s) for ct in range(RADIX)])], 0)
                for s in range(2)])
        if g == 0:
            for load in rest:
                load.wait()
        if g % 2:
            transform(0, 0, 0, (g - 1, g))
    meet()
    send(0, first)
    own_copy(0).start()

    zero = jnp.zeros((SUB, LANES), jnp.float32)
    squares, zr, zi = [zero] * 4, zero, zero
    for g in range(RADIX):
        for pair in range(SUB):
            part = [[rows_of(g, pair, ct, s) for s in range(2)] for ct in range(RADIX)]
            for ct in range(RADIX):
                for s in range(2):
                    for w in range(2):
                        squares[ct] = squares[ct] + part[ct][s][w] * part[ct][s][w]
            for w in range(2):
                angle = 2.0 * math.pi / total_len * n_devices * (rev(2 * pair + w, 4) * SUB * RADIX + rev(g, 2))
                cw, sw = math.cos(angle), math.sin(angle)
                zr = zr + (part[0][0][w] * cw + part[0][1][w] * sw)
                zi = zi + (part[0][1][w] * cw - part[0][0][w] * sw)
            (x0r, x0i), (x1r, x1i), (x2r, x2i), (x3r, x3i) = [
                [jnp.concatenate(part[ct][s], 0) for s in range(2)] for ct in range(RADIX)]
            br, bi, dr, di = x0r - x2r, x0i - x2i, x1r - x3r, x1i - x3i
            keep(1, g, pair, (br - di, bi + dr))
            keep(2, g, pair, ((x0r + x2r) - (x1r + x3r), (x0i + x2i) - (x1i + x3i)))
            keep(3, g, pair, (br + di, bi - dr))

    pc, ps = turn_ref[2 * n_devices : 2 * n_devices + SUB, :], turn_ref[2 * n_devices + SUB :, :]
    oc, os_ = turn_ref[pl.ds(slot, 1), :], turn_ref[pl.ds(n_devices + slot, 1), :]
    total = jnp.sum(jnp.sum((squares[0] + squares[1]) + (squares[2] + squares[3]), 0, keepdims=True), 1, keepdims=True)
    yr = jnp.sum(zr * pc + zi * ps, 0, keepdims=True)
    yi = jnp.sum(zi * pc - zr * ps, 0, keepdims=True)
    wr = jnp.sum(yr * oc + yi * os_, 1, keepdims=True)
    wi = jnp.sum(yi * oc - yr * os_, 1, keepdims=True)
    lane = lax.broadcasted_iota(jnp.int32, (1, LANES), 1)
    stat = jnp.where(lane == 0, total, jnp.where(lane == 1, wr, jnp.where(lane == 2, wi, 0.0)))
    sends[STAT][pl.ds(rows[STAT] - 1, n_devices, stride=rows[STAT]), :] = jnp.broadcast_to(stat, (n_devices, LANES))

    for k, chunks in list(enumerate(PIECES))[1:]:
        for place, chunk in enumerate(chunks):
            transform(k, place, chunk, range(RADIX))
        if k == 1:
            meet_last()
            send(0, second)
        send(k, order)
        own_copy(k).start()

    for k, chunks in enumerate(PIECES):
        wait_rows(recvs[k], (n_devices - 1) * rows[k], recv_sem.at[k])
        own_copy(k).wait()
        if k == STAT:
            sums = jnp.sum(recvs[k][pl.ds(rows[k] - 1, n_devices, stride=pitches[k]), :], 0, keepdims=True)
            mean_square = jnp.sum(jnp.where(lane == 0, sums, 0.0), 1, keepdims=True) / total_len
            shifted = mean_square + 1e-06
            factor = lax.rsqrt(shifted)
            factor = factor * (1.5 - 0.5 * shifted * factor * factor)
            checks = jnp.where(lane == 0, mean_square, sums * (factor / math.sqrt(total_len)))
            tot_ref[...] = jnp.broadcast_to(checks, (SUB, LANES))
            factor = jnp.broadcast_to(factor, (SUB, LANES))
            fac_ref[...] = factor
        ready = range(STAT + 1) if k == STAT else [k] if STAT < k < n_pieces - 1 else []
        for kk in ready:
            for place, chunk in enumerate(PIECES[kk]):
                for h in range(SUB):
                    base = ((h // 2) * (RADIX - 1) + chunk) * 2 * LANES + h % 2
                    for m, v in enumerate(turn_tiles(recvs[kk], pitches[kk], place, h, n_devices, factor)):
                        field[pl.ds(base + rev(m, 4) * 2 * SUB, SUB, stride=2), :] = v
    for k in range(n_pieces):
        wait_rows(sends[k], (n_devices - 1) * rows[k], send_sem)


def finish_kernel(n_devices, pitch, field, last, tot_ref, fac_ref, out_hbm, checks_hbm, turned, checks_ref, sem):
    f_rows = 2 * LANES
    many = (RADIX - 1) * f_rows
    stores = []
    for fq in range(RADIX):
        stores.append(pltpu.make_async_copy(
            field.at[pl.ds(fq * many, many)], out_hbm.at[pl.ds(fq * RADIX * f_rows, many)], sem.at[fq]))
        stores[-1].start()
    checks_ref[...] = tot_ref[0:1, 0:3]
    stores.append(pltpu.make_async_copy(checks_ref, checks_hbm, sem.at[2 * RADIX]))
    stores[-1].start()
    factor = fac_ref[...]
    for h in range(SUB):
        base = h // 2 * f_rows + h % 2
        for m, v in enumerate(turn_tiles(last, pitch, 0, h, n_devices, factor)):
            turned[pl.ds(base + rev(m, 4) * 2 * SUB, SUB, stride=2), :] = v
        if h % 2:
            fq = h // 2
            stores.append(pltpu.make_async_copy(
                turned.at[pl.ds(fq * f_rows, f_rows)],
                out_hbm.at[pl.ds((fq * RADIX + RADIX - 1) * f_rows, f_rows)], sem.at[RADIX + fq]))
            stores[-1].start()
    for store in stores:
        store.wait()


def fast(n_outer, n_inner, amplitudes):
    amp_dev = amplitudes.shape[1]
    n_devices = n_outer * n_inner
    rows_count = amp_dev // COLUMNS
    total_len = amp_dev * n_devices
    view = amplitudes.reshape(2, amp_dev // LANES, LANES).transpose(1, 0, 2).reshape(-1, LANES)
    table, turn = tables(n_devices, total_len)
    th = table.astype(jnp.bfloat16)
    tl = (table - th.astype(np.float32)).astype(jnp.bfloat16)
    hbm, vmem = pl.BlockSpec(memory_space=pltpu.HBM), pl.BlockSpec(memory_space=pltpu.VMEM)
    rows, pitches = pieces_of(n_devices)
    small = pltpu.VMEM((SUB, LANES), jnp.float32)
    f_rows = 2 * LANES
    pair = pltpu.VMEM((RADIX, rows_count, 2 * LANES), jnp.bfloat16)
    scratch = [
        pltpu.VMEM((RADIX * SUB * (LANES + 4), LANES), jnp.float32),
        pltpu.VMEM(th.shape, jnp.bfloat16),
        pltpu.VMEM(tl.shape, jnp.bfloat16),
        pltpu.VMEM(turn.shape, jnp.float32),
        pair,
        pair,
        *[pltpu.VMEM((n_devices * r, LANES), jnp.float32) for r in rows],
        *[pltpu.VMEM((n_devices * p, LANES), jnp.float32) for p in pitches[:-1]],
        pltpu.SemaphoreType.DMA,
        pltpu.SemaphoreType.DMA((len(PIECES),)),
        pltpu.SemaphoreType.DMA((len(PIECES),)),
        pltpu.SemaphoreType.DMA((RADIX + 3,)),
        pltpu.SemaphoreType.REGULAR,
    ]
    parts = pl.pallas_call(
        functools.partial(kernel, n_outer, n_inner, total_len),
        out_shape=(
            pltpu.VMEM((RADIX * (RADIX - 1) * f_rows, LANES), jnp.float32),
            pltpu.VMEM((n_devices * pitches[-1], LANES), jnp.float32),
            small,
            small,
        ),
        in_specs=[hbm] * 4,
        out_specs=(vmem,) * 4,
        scratch_shapes=scratch,
        compiler_params=pltpu.CompilerParams(collective_id=0, has_side_effects=True, vmem_limit_bytes=32_000_000),
    )(*[pltpu.with_memory_space_constraint(v, pltpu.HBM) for v in (view, jnp.asarray(th), jnp.asarray(tl), jnp.asarray(turn))])
    field, checks = pl.pallas_call(
        functools.partial(finish_kernel, n_devices, pitches[-1]),
        out_shape=(jax.ShapeDtypeStruct(view.shape, jnp.float32), jax.ShapeDtypeStruct((1, 3), jnp.float32)),
        in_specs=[vmem] * 4,
        out_specs=(hbm, hbm),
        scratch_shapes=[
            pltpu.VMEM((RADIX * f_rows, LANES), jnp.float32),
            pltpu.VMEM((1, 3), jnp.float32),
            pltpu.SemaphoreType.DMA((2 * RADIX + 1,)),
        ],
        compiler_params=pltpu.CompilerParams(vmem_limit_bytes=32_000_000),
    )(*parts)
    result = field.reshape(-1, 2, LANES).transpose(1, 0, 2).reshape(2, amp_dev)
    return result, checks.reshape(3)


def reverse_index(values, count):
    result = jnp.zeros_like(values)
    for bit_pos in range(count):
        result = result | (values >> bit_pos & 1) << count - 1 - bit_pos
    return result


def reversal_table(size, count):
    indices = jnp.arange(size, dtype=jnp.int32)
    return (reverse_index(indices, count)[:, None] == indices[None, :]).astype(jnp.float32)


def check_terms(current, positions, angle_scale):
    angles = positions.astype(jnp.float32) * angle_scale
    cosine = jnp.cos(angles)
    sine = jnp.sin(angles)
    squares = jnp.sum(current * current)
    phase_real = jnp.sum(current[0] * cosine + current[1] * sine)
    phase_imag = jnp.sum(current[1] * cosine - current[0] * sine)
    return (squares, phase_real, phase_imag)


def per_device(amplitudes):
    amp_dev = amplitudes.shape[1]
    n_outer = lax.axis_size("outer")
    n_inner = lax.axis_size("inner")
    outer_bits = n_outer.bit_length() - 1
    inner_bits = n_inner.bit_length() - 1
    global_bits = outer_bits + inner_bits
    local_bits = amp_dev.bit_length() - 1
    n_devices = n_outer * n_inner
    high_count = amp_dev // n_devices
    total_len = amp_dev * n_devices
    columns = 2**WINDOW
    rows_count = amp_dev // columns
    column_ids = jnp.arange(columns, dtype=jnp.int32)
    reversed_ids = reverse_index(column_ids, WINDOW)
    products = column_ids[:, None] * reversed_ids[None, :] % columns
    angles = products.astype(jnp.float32) * (2.0 * math.pi / columns)
    real_part = jnp.cos(angles) / math.sqrt(columns)
    imag_part = jnp.sin(angles) / math.sqrt(columns)
    table = jnp.concatenate(
        [jnp.concatenate([real_part, imag_part], 1), jnp.concatenate([-imag_part, real_part], 1)], 0
    )
    stacked = jnp.concatenate(
        [amplitudes[0].reshape(rows_count, columns), amplitudes[1].reshape(rows_count, columns)], 1
    )
    result = jnp.dot(
        stacked, table, precision=lax.Precision.HIGHEST, preferred_element_type=jnp.float32
    )
    windowed = jnp.stack([result[:, :columns].reshape(-1), result[:, columns:].reshape(-1)])
    device_id = lax.axis_index("outer") * n_inner + lax.axis_index("inner")
    angle_scale = 2.0 * math.pi / total_len
    local_ids = jnp.arange(amp_dev, dtype=jnp.int32)
    positions = reverse_index(device_id * amp_dev + local_ids, local_bits + global_bits)
    totals = lax.psum(check_terms(windowed, positions, angle_scale), ("outer", "inner"))
    device_table = reversal_table(n_devices, global_bits)
    high_table = reversal_table(high_count, local_bits - global_bits)
    grid = windowed.reshape(2, high_count, n_devices)
    ordered = jnp.einsum("pm,shm->sph", device_table, grid, precision=lax.Precision.HIGHEST)
    blocks = ordered.reshape(2, n_outer, n_inner, high_count)
    blocks = lax.all_to_all(
        lax.all_to_all(blocks, "outer", split_axis=1, concat_axis=1, tiled=True),
        "inner",
        split_axis=2,
        concat_axis=2,
        tiled=True,
    )
    received = blocks.reshape(2, n_devices, high_count)
    turned_high = jnp.einsum("qh,sdh->sdq", high_table, received, precision=lax.Precision.HIGHEST)
    placed = jnp.einsum("ed,sdq->sqe", device_table, turned_high, precision=lax.Precision.HIGHEST)
    reversed_field = placed.reshape(2, amp_dev)
    mean_square = totals[0] / total_len
    factor = lax.rsqrt(mean_square + 1e-06)
    scaled = factor / math.sqrt(total_len)
    checks = jnp.stack([mean_square, totals[1] * scaled, totals[2] * scaled])
    return (reversed_field * factor, checks)


def solution(mesh):
    n_outer, n_inner = mesh.shape["outer"], mesh.shape["inner"]

    def body(amplitudes):
        rows_count = amplitudes.shape[1] // COLUMNS
        n_devices = n_outer * n_inner
        if rows_count * n_devices == LANES * LANES and n_devices * SUB == 2 * LANES and n_inner % 4 == 0:
            return fast(n_outer, n_inner, amplitudes)
        return per_device(amplitudes)

    return jax.shard_map(
        body,
        mesh=mesh,
        in_specs=(P(None, ("outer", "inner")),),
        out_specs=(P(None, ("outer", "inner")), P()),
        check_vma=False,
    )
```

```python
import functools
import itertools
import math

import jax
import jax.numpy as jnp
import numpy as np
from jax import lax
from jax.experimental import pallas as pl
from jax.experimental.pallas import tpu as pltpu
from jax.sharding import PartitionSpec as P

WINDOW = 9
COLUMNS = 2**WINDOW
LANES = 128
SUB = 8
RADIX = COLUMNS // LANES
PIECES = ((0,), (1, 2), (3,))
STAT = 1
MESH = pl.DeviceIdType.MESH


def rev(value, count):
    out = 0
    for bit in range(count):
        out |= (value >> bit & 1) << (count - 1 - bit)
    return out


def split_bf16(values):
    high = values.astype(jnp.bfloat16)
    return high, (values - high.astype(np.float32)).astype(jnp.bfloat16)


def tables(n_devices, total_len):
    f = np.arange(COLUMNS).reshape(LANES, RADIX).T
    lane = np.arange(LANES)
    ang = (f[:, :, None] * lane) % COLUMNS * (2.0 * np.pi / COLUMNS)
    c, s = np.cos(ang) / math.sqrt(COLUMNS), np.sin(ang) / math.sqrt(COLUMNS)
    table = np.stack([np.concatenate([c, -s], -1), np.concatenate([s, c], -1)], 2)
    table = table.reshape(RADIX, 2 * LANES, 2 * LANES).astype(np.float32)
    slots = 2.0 * np.pi / total_len * np.arange(n_devices)
    subs = 2.0 * np.pi / total_len * n_devices * RADIX * np.arange(SUB)
    turn = np.zeros((2 * (n_devices + SUB), LANES), np.float32)
    turn[:n_devices], turn[n_devices : 2 * n_devices] = np.cos(slots)[:, None], np.sin(slots)[:, None]
    turn[2 * n_devices : 2 * n_devices + SUB, 1] = np.cos(subs) * math.sqrt(COLUMNS)
    turn[2 * n_devices + SUB :, 1] = np.sin(subs) * math.sqrt(COLUMNS)
    return table, turn


def pieces_of(n_devices):
    rows = [len(chunks) * RADIX * SUB + (k == STAT) for k, chunks in enumerate(PIECES)]
    return rows, [r if r % 2 else r + 4 for r in rows]


def turn_tiles(recv, pitch, place, h, n_devices, factor):
    tile = jnp.concatenate(
        [recv[pl.ds((place * RADIX + rev(j, 2)) * SUB + h, n_devices, stride=pitch), :] for j in range(RADIX)], 0)
    turned = tile.T.reshape(LANES // SUB, SUB, LANES)
    return [turned[m] * factor for m in range(LANES // SUB)]


def kernel(n_outer, n_inner, total_len, x_hbm, th_hbm, tl_hbm, turn_hbm, *refs):
    n_pieces = len(PIECES)
    field, last, tot_ref, fac_ref, x_ref, th_ref, tl_ref, turn_ref, bh_ref, bl_ref = refs[:10]
    sends, recvs = refs[10 : 10 + n_pieces], [*refs[10 + n_pieces : 9 + 2 * n_pieces], last]
    send_sem, recv_sem, own_sem, load_sem, last_sem = refs[9 + 2 * n_pieces :]
    n_devices = n_outer * n_inner
    obits, ibits = n_outer.bit_length() - 1, n_inner.bit_length() - 1
    span = LANES
    q_rows = span + 4

    loads = []
    for g in range(RADIX):
        for q in range(SUB):
            loads.append(pltpu.make_async_copy(
                x_hbm.at[pl.ds((g * SUB + q) * span, span)],
                x_ref.at[pl.ds((g * SUB + rev(q, 3)) * q_rows, span)], load_sem.at[g]))
    rest = [pltpu.make_async_copy(src, dst, load_sem.at[RADIX + k]) for k, (src, dst) in enumerate(
        [(th_hbm, th_ref), (tl_hbm, tl_ref), (turn_hbm, turn_ref)])]
    for load in loads + rest:
        load.start()

    o, i = lax.axis_index("outer"), lax.axis_index("inner")
    me = o * n_inner + i
    slot = 0
    odelta, idelta = [], []
    for k in range(obits):
        bit = o // 2**k % 2
        slot = slot + bit * 2 ** (obits - 1 - k)
        odelta.append((1 - 2 * bit) * 2**k)
    for k in range(ibits):
        bit = i // 2**k % 2
        slot = slot + bit * 2 ** (ibits - 1 - k) * n_outer
        idelta.append((1 - 2 * bit) * 2**k)

    def peer(mo, mi):
        po, pi = o, i
        for k in range(obits):
            if mo >> k & 1:
                po = po + odelta[k]
        for k in range(ibits):
            if mi >> k & 1:
                pi = pi + idelta[k]
        return po, pi

    wide = n_inner // 4
    level, place_in = i // wide, i % wide
    high = level // 2
    across = level + 1 - 2 * (level % 2)
    group = n_outer * wide

    def members(at):
        return [(peer(mo, 0)[0], at * wide + lax.rem(place_in + t, wide)) for t in range(wide) for mo in range(n_outer)]

    def ranked(at):
        return [(o2 + c, at * wide + t) for o2 in range(0, n_outer, 2) for t in range(wide) for c in range(2)]

    def pairs(far, near):
        return [p for pair in itertools.zip_longest(far, near) for p in pair if p is not None]

    own = members(level)[1:]
    first = pairs(ranked(2 - high), own) + members((1 - high) * across)
    second = ranked(high * across + (1 - high) * 3)
    order = pairs(ranked((1 - high) * 3) + ranked(2 - high), own + members(across))

    barrier = pltpu.get_barrier_semaphore()

    def greet(ring, at, who=None):
        for p in members(at) if who is None else who:
            pl.semaphore_signal(ring, inc=1, device_id=p, device_id_type=MESH)

    greet(barrier, level, own)
    for t in range(1, 4):
        pl.when(level < 3)(functools.partial(greet, barrier, lax.rem(level + t, 4)))

    def meet():
        pl.semaphore_wait(barrier, 3 * group - 1 + group * (level // 3))
        for earlier in (2, 1, 0):
            pl.when(level == 3)(functools.partial(greet, last_sem, earlier))

    def meet_last():
        pl.when(level < 3)(lambda: pl.semaphore_wait(last_sem, group))

    rows, pitches = pieces_of(n_devices)

    def send(k, peers):
        dst = recvs[k].at[pl.ds(slot * pitches[k], rows[k])]
        for po, pi in peers:
            pltpu.make_async_remote_copy(
                src_ref=sends[k].at[pl.ds((po * n_inner + pi) * rows[k], rows[k])], dst_ref=dst,
                send_sem=send_sem, recv_sem=recv_sem.at[k],
                device_id=(po, pi), device_id_type=MESH).start()

    def own_copy(k):
        return pltpu.make_async_copy(
            sends[k].at[pl.ds(me * rows[k], rows[k])],
            recvs[k].at[pl.ds(slot * pitches[k], rows[k])], own_sem.at[k])

    def wait_rows(ref, count, sem):
        part = ref.at[pl.ds(0, count)]
        pltpu.make_async_copy(part, part, sem).wait()

    def rows_of(g, pair, ct, s):
        return [x_ref[pl.ds(g * SUB * q_rows + (2 * pair + w) * SUB + 2 * ct + s, SUB, stride=q_rows), :] for w in range(2)]

    def keep(chunk, g, pair, values):
        at = pl.ds((g * SUB + pair) * 2 * SUB, 2 * SUB)
        for s, value in enumerate(values):
            high, low = split_bf16(value)
            bh_ref[chunk, at, s * LANES : (s + 1) * LANES] = high
            bl_ref[chunk, at, s * LANES : (s + 1) * LANES] = low

    dims = (((1,), (1,)), ((), ()))

    def transform(k, place, chunk, groups):
        at = pl.ds(groups[0] * LANES, len(groups) * LANES)
        th, tl, bh, bl = th_ref[chunk], tl_ref[chunk], bh_ref[chunk, at, :], bl_ref[chunk, at, :]
        res = lax.dot_general(th, bh, dims, preferred_element_type=jnp.float32)
        res += lax.dot_general(th, bl, dims, preferred_element_type=jnp.float32)
        res += lax.dot_general(tl, bh, dims, preferred_element_type=jnp.float32)
        for e in range(n_devices):
            for n, g in enumerate(groups):
                sends[k][pl.ds(e * rows[k] + (place * RADIX + g) * SUB, SUB), :] = (
                    res[e * SUB : (e + 1) * SUB, n * LANES : (n + 1) * LANES])

    for g in range(RADIX):
        wait_rows(x_ref, SUB * span, load_sem.at[g])
        for pair in range(SUB):
            keep(0, g, pair, [
                jnp.concatenate([(a + c) + (b + d) for a, b, c, d in zip(*[rows_of(g, pair, ct, s) for ct in range(RADIX)])], 0)
                for s in range(2)])
        if g == 0:
            for load in rest:
                load.wait()
        if g % 2:
            transform(0, 0, 0, (g - 1, g))
    meet()
    send(0, first)
    own_copy(0).start()

    zero = jnp.zeros((SUB, LANES), jnp.float32)
    squares, zr, zi = [zero] * 4, zero, zero
    for g in range(RADIX):
        for pair in range(SUB):
            part = [[rows_of(g, pair, ct, s) for s in range(2)] for ct in range(RADIX)]
            for ct in range(RADIX):
                for s in range(2):
                    for w in range(2):
                        squares[ct] = squares[ct] + part[ct][s][w] * part[ct][s][w]
            for w in range(2):
                angle = 2.0 * math.pi / total_len * n_devices * (rev(2 * pair + w, 4) * SUB * RADIX + rev(g, 2))
                cw, sw = math.cos(angle), math.sin(angle)
                zr = zr + (part[0][0][w] * cw + part[0][1][w] * sw)
                zi = zi + (part[0][1][w] * cw - part[0][0][w] * sw)
            (x0r, x0i), (x1r, x1i), (x2r, x2i), (x3r, x3i) = [
                [jnp.concatenate(part[ct][s], 0) for s in range(2)] for ct in range(RADIX)]
            br, bi, dr, di = x0r - x2r, x0i - x2i, x1r - x3r, x1i - x3i
            keep(1, g, pair, (br - di, bi + dr))
            keep(2, g, pair, ((x0r + x2r) - (x1r + x3r), (x0i + x2i) - (x1i + x3i)))
            keep(3, g, pair, (br + di, bi - dr))

    pc, ps = turn_ref[2 * n_devices : 2 * n_devices + SUB, :], turn_ref[2 * n_devices + SUB :, :]
    oc, os_ = turn_ref[pl.ds(slot, 1), :], turn_ref[pl.ds(n_devices + slot, 1), :]
    total = jnp.sum(jnp.sum((squares[0] + squares[1]) + (squares[2] + squares[3]), 0, keepdims=True), 1, keepdims=True)
    yr = jnp.sum(zr * pc + zi * ps, 0, keepdims=True)
    yi = jnp.sum(zi * pc - zr * ps, 0, keepdims=True)
    wr = jnp.sum(yr * oc + yi * os_, 1, keepdims=True)
    wi = jnp.sum(yi * oc - yr * os_, 1, keepdims=True)
    lane = lax.broadcasted_iota(jnp.int32, (1, LANES), 1)
    stat = jnp.where(lane == 0, total, jnp.where(lane == 1, wr, jnp.where(lane == 2, wi, 0.0)))
    sends[STAT][pl.ds(rows[STAT] - 1, n_devices, stride=rows[STAT]), :] = jnp.broadcast_to(stat, (n_devices, LANES))

    for k, chunks in list(enumerate(PIECES))[1:]:
        for place, chunk in enumerate(chunks):
            transform(k, place, chunk, range(RADIX))
        if k == 1:
            meet_last()
            send(0, second)
        send(k, order)
        own_copy(k).start()

    for k, chunks in enumerate(PIECES):
        wait_rows(recvs[k], (n_devices - 1) * rows[k], recv_sem.at[k])
        own_copy(k).wait()
        if k == STAT:
            sums = jnp.sum(recvs[k][pl.ds(rows[k] - 1, n_devices, stride=pitches[k]), :], 0, keepdims=True)
            mean_square = jnp.sum(jnp.where(lane == 0, sums, 0.0), 1, keepdims=True) / total_len
            shifted = mean_square + 1e-06
            factor = lax.rsqrt(shifted)
            factor = factor * (1.5 - 0.5 * shifted * factor * factor)
            checks = jnp.where(lane == 0, mean_square, sums * (factor / math.sqrt(total_len)))
            tot_ref[...] = jnp.broadcast_to(checks, (SUB, LANES))
            factor = jnp.broadcast_to(factor, (SUB, LANES))
            fac_ref[...] = factor
        ready = range(STAT + 1) if k == STAT else [k] if STAT < k < n_pieces - 1 else []
        for kk in ready:
            for place, chunk in enumerate(PIECES[kk]):
                for h in range(SUB):
                    base = ((h // 2) * (RADIX - 1) + chunk) * 2 * LANES + h % 2
                    for m, v in enumerate(turn_tiles(recvs[kk], pitches[kk], place, h, n_devices, factor)):
                        field[pl.ds(base + rev(m, 4) * 2 * SUB, SUB, stride=2), :] = v
    for k in range(n_pieces):
        wait_rows(sends[k], (n_devices - 1) * rows[k], send_sem)


def finish_kernel(n_devices, pitch, field, last, tot_ref, fac_ref, out_hbm, checks_hbm, turned, checks_ref, sem):
    f_rows = 2 * LANES
    many = (RADIX - 1) * f_rows
    stores = []
    for fq in range(RADIX):
        stores.append(pltpu.make_async_copy(
            field.at[pl.ds(fq * many, many)], out_hbm.at[pl.ds(fq * RADIX * f_rows, many)], sem.at[fq]))
        stores[-1].start()
    checks_ref[...] = tot_ref[0:1, 0:3]
    stores.append(pltpu.make_async_copy(checks_ref, checks_hbm, sem.at[2 * RADIX]))
    stores[-1].start()
    factor = fac_ref[...]
    for h in range(SUB):
        base = h // 2 * f_rows + h % 2
        for m, v in enumerate(turn_tiles(last, pitch, 0, h, n_devices, factor)):
            turned[pl.ds(base + rev(m, 4) * 2 * SUB, SUB, stride=2), :] = v
        if h % 2:
            fq = h // 2
            stores.append(pltpu.make_async_copy(
                turned.at[pl.ds(fq * f_rows, f_rows)],
                out_hbm.at[pl.ds((fq * RADIX + RADIX - 1) * f_rows, f_rows)], sem.at[RADIX + fq]))
            stores[-1].start()
    for store in stores:
        store.wait()


def fast(n_outer, n_inner, amplitudes):
    amp_dev = amplitudes.shape[1]
    n_devices = n_outer * n_inner
    rows_count = amp_dev // COLUMNS
    total_len = amp_dev * n_devices
    view = amplitudes.reshape(2, amp_dev // LANES, LANES).transpose(1, 0, 2).reshape(-1, LANES)
    table, turn = tables(n_devices, total_len)
    th = table.astype(jnp.bfloat16)
    tl = (table - th.astype(np.float32)).astype(jnp.bfloat16)
    hbm, vmem = pl.BlockSpec(memory_space=pltpu.HBM), pl.BlockSpec(memory_space=pltpu.VMEM)
    rows, pitches = pieces_of(n_devices)
    small = pltpu.VMEM((SUB, LANES), jnp.float32)
    f_rows = 2 * LANES
    pair = pltpu.VMEM((RADIX, rows_count, 2 * LANES), jnp.bfloat16)
    scratch = [
        pltpu.VMEM((RADIX * SUB * (LANES + 4), LANES), jnp.float32),
        pltpu.VMEM(th.shape, jnp.bfloat16),
        pltpu.VMEM(tl.shape, jnp.bfloat16),
        pltpu.VMEM(turn.shape, jnp.float32),
        pair,
        pair,
        *[pltpu.VMEM((n_devices * r, LANES), jnp.float32) for r in rows],
        *[pltpu.VMEM((n_devices * p, LANES), jnp.float32) for p in pitches[:-1]],
        pltpu.SemaphoreType.DMA,
        pltpu.SemaphoreType.DMA((len(PIECES),)),
        pltpu.SemaphoreType.DMA((len(PIECES),)),
        pltpu.SemaphoreType.DMA((RADIX + 3,)),
        pltpu.SemaphoreType.REGULAR,
    ]
    parts = pl.pallas_call(
        functools.partial(kernel, n_outer, n_inner, total_len),
        out_shape=(
            pltpu.VMEM((RADIX * (RADIX - 1) * f_rows, LANES), jnp.float32),
            pltpu.VMEM((n_devices * pitches[-1], LANES), jnp.float32),
            small,
            small,
        ),
        in_specs=[hbm] * 4,
        out_specs=(vmem,) * 4,
        scratch_shapes=scratch,
        compiler_params=pltpu.CompilerParams(collective_id=0, has_side_effects=True, vmem_limit_bytes=32_000_000),
    )(*[pltpu.with_memory_space_constraint(v, pltpu.HBM) for v in (view, jnp.asarray(th), jnp.asarray(tl), jnp.asarray(turn))])
    field, checks = pl.pallas_call(
        functools.partial(finish_kernel, n_devices, pitches[-1]),
        out_shape=(jax.ShapeDtypeStruct(view.shape, jnp.float32), jax.ShapeDtypeStruct((1, 3), jnp.float32)),
        in_specs=[vmem] * 4,
        out_specs=(hbm, hbm),
        scratch_shapes=[
            pltpu.VMEM((RADIX * f_rows, LANES), jnp.float32),
            pltpu.VMEM((1, 3), jnp.float32),
            pltpu.SemaphoreType.DMA((2 * RADIX + 1,)),
        ],
        compiler_params=pltpu.CompilerParams(vmem_limit_bytes=32_000_000),
    )(*parts)
    result = field.reshape(-1, 2, LANES).transpose(1, 0, 2).reshape(2, amp_dev)
    return result, checks.reshape(3)


def reverse_index(values, count):
    result = jnp.zeros_like(values)
    for bit_pos in range(count):
        result = result | (values >> bit_pos & 1) << count - 1 - bit_pos
    return result


def reversal_table(size, count):
    indices = jnp.arange(size, dtype=jnp.int32)
    return (reverse_index(indices, count)[:, None] == indices[None, :]).astype(jnp.float32)


def check_terms(current, positions, angle_scale):
    angles = positions.astype(jnp.float32) * angle_scale
    cosine = jnp.cos(angles)
    sine = jnp.sin(angles)
    squares = jnp.sum(current * current)
    phase_real = jnp.sum(current[0] * cosine + current[1] * sine)
    phase_imag = jnp.sum(current[1] * cosine - current[0] * sine)
    return (squares, phase_real, phase_imag)


def per_device(amplitudes):
    amp_dev = amplitudes.shape[1]
    n_outer = lax.axis_size("outer")
    n_inner = lax.axis_size("inner")
    outer_bits = n_outer.bit_length() - 1
    inner_bits = n_inner.bit_length() - 1
    global_bits = outer_bits + inner_bits
    local_bits = amp_dev.bit_length() - 1
    n_devices = n_outer * n_inner
    high_count = amp_dev // n_devices
    total_len = amp_dev * n_devices
    columns = 2**WINDOW
    rows_count = amp_dev // columns
    column_ids = jnp.arange(columns, dtype=jnp.int32)
    reversed_ids = reverse_index(column_ids, WINDOW)
    products = column_ids[:, None] * reversed_ids[None, :] % columns
    angles = products.astype(jnp.float32) * (2.0 * math.pi / columns)
    real_part = jnp.cos(angles) / math.sqrt(columns)
    imag_part = jnp.sin(angles) / math.sqrt(columns)
    table = jnp.concatenate(
        [jnp.concatenate([real_part, imag_part], 1), jnp.concatenate([-imag_part, real_part], 1)], 0
    )
    stacked = jnp.concatenate(
        [amplitudes[0].reshape(rows_count, columns), amplitudes[1].reshape(rows_count, columns)], 1
    )
    result = jnp.dot(
        stacked, table, precision=lax.Precision.HIGHEST, preferred_element_type=jnp.float32
    )
    windowed = jnp.stack([result[:, :columns].reshape(-1), result[:, columns:].reshape(-1)])
    device_id = lax.axis_index("outer") * n_inner + lax.axis_index("inner")
    angle_scale = 2.0 * math.pi / total_len
    local_ids = jnp.arange(amp_dev, dtype=jnp.int32)
    positions = reverse_index(device_id * amp_dev + local_ids, local_bits + global_bits)
    totals = lax.psum(check_terms(windowed, positions, angle_scale), ("outer", "inner"))
    device_table = reversal_table(n_devices, global_bits)
    high_table = reversal_table(high_count, local_bits - global_bits)
    grid = windowed.reshape(2, high_count, n_devices)
    ordered = jnp.einsum("pm,shm->sph", device_table, grid, precision=lax.Precision.HIGHEST)
    blocks = ordered.reshape(2, n_outer, n_inner, high_count)
    blocks = lax.all_to_all(
        lax.all_to_all(blocks, "outer", split_axis=1, concat_axis=1, tiled=True),
        "inner",
        split_axis=2,
        concat_axis=2,
        tiled=True,
    )
    received = blocks.reshape(2, n_devices, high_count)
    turned_high = jnp.einsum("qh,sdh->sdq", high_table, received, precision=lax.Precision.HIGHEST)
    placed = jnp.einsum("ed,sdq->sqe", device_table, turned_high, precision=lax.Precision.HIGHEST)
    reversed_field = placed.reshape(2, amp_dev)
    mean_square = totals[0] / total_len
    factor = lax.rsqrt(mean_square + 1e-06)
    scaled = factor / math.sqrt(total_len)
    checks = jnp.stack([mean_square, totals[1] * scaled, totals[2] * scaled])
    return (reversed_field * factor, checks)


def solution(mesh):
    n_outer, n_inner = mesh.shape["outer"], mesh.shape["inner"]

    def body(amplitudes):
        rows_count = amplitudes.shape[1] // COLUMNS
        n_devices = n_outer * n_inner
        if rows_count * n_devices == LANES * LANES and n_devices * SUB == 2 * LANES and n_inner % 4 == 0:
            return fast(n_outer, n_inner, amplitudes)
        return per_device(amplitudes)

    return jax.shard_map(
        body,
        mesh=mesh,
        in_specs=(P(None, ("outer", "inner")),),
        out_specs=(P(None, ("outer", "inner")), P()),
        check_vma=False,
    )
```

```python
import functools
import itertools
import math

import jax
import jax.numpy as jnp
import numpy as np
from jax import lax
from jax.experimental import pallas as pl
from jax.experimental.pallas import tpu as pltpu
from jax.sharding import PartitionSpec as P

WINDOW = 9
COLUMNS = 2**WINDOW
LANES = 128
SUB = 8
RADIX = COLUMNS // LANES
PIECES = ((0,), (1, 2), (3,))
STAT = 1
MESH = pl.DeviceIdType.MESH


def rev(value, count):
    out = 0
    for bit in range(count):
        out |= (value >> bit & 1) << (count - 1 - bit)
    return out


def split_bf16(values):
    high = values.astype(jnp.bfloat16)
    return high, (values - high.astype(np.float32)).astype(jnp.bfloat16)


def tables(n_devices, total_len):
    f = np.arange(COLUMNS).reshape(LANES, RADIX).T
    lane = np.arange(LANES)
    ang = (f[:, :, None] * lane) % COLUMNS * (2.0 * np.pi / COLUMNS)
    c, s = np.cos(ang) / math.sqrt(COLUMNS), np.sin(ang) / math.sqrt(COLUMNS)
    table = np.stack([np.concatenate([c, -s], -1), np.concatenate([s, c], -1)], 2)
    table = table.reshape(RADIX, 2 * LANES, 2 * LANES).astype(np.float32)
    slots = 2.0 * np.pi / total_len * np.arange(n_devices)
    subs = 2.0 * np.pi / total_len * n_devices * RADIX * np.arange(SUB)
    turn = np.zeros((2 * (n_devices + SUB), LANES), np.float32)
    turn[:n_devices], turn[n_devices : 2 * n_devices] = np.cos(slots)[:, None], np.sin(slots)[:, None]
    turn[2 * n_devices : 2 * n_devices + SUB, 1] = np.cos(subs) * math.sqrt(COLUMNS)
    turn[2 * n_devices + SUB :, 1] = np.sin(subs) * math.sqrt(COLUMNS)
    return table, turn


def pieces_of(n_devices):
    rows = [len(chunks) * RADIX * SUB for chunks in PIECES]
    return rows, [r + 4 for r in rows]


def turn_tiles(recv, pitch, place, h, n_devices, factor):
    tile = jnp.concatenate(
        [recv[pl.ds((place * RADIX + rev(j, 2)) * SUB + h, n_devices, stride=pitch), :] for j in range(RADIX)], 0)
    turned = tile.T.reshape(LANES // SUB, SUB, LANES)
    return [turned[m] * factor for m in range(LANES // SUB)]


def kernel(n_outer, n_inner, total_len, x_hbm, th_hbm, tl_hbm, turn_hbm, *refs):
    n_pieces = len(PIECES)
    field, last, tot_ref, fac_ref, x_ref, th_ref, tl_ref, turn_ref, bh_ref, bl_ref = refs[:10]
    sends, recvs = refs[10 : 10 + n_pieces], [*refs[10 + n_pieces : 9 + 2 * n_pieces], last]
    near_ref, half_ref, far_ref, send_sem, recv_sem, own_sem, load_sem, last_sem, stat_sem = refs[9 + 2 * n_pieces :]
    n_devices = n_outer * n_inner
    obits, ibits = n_outer.bit_length() - 1, n_inner.bit_length() - 1
    span = LANES
    q_rows = span + 4

    loads = []
    for g in range(RADIX):
        for q in range(SUB):
            loads.append(pltpu.make_async_copy(
                x_hbm.at[pl.ds((g * SUB + q) * span, span)],
                x_ref.at[pl.ds((g * SUB + rev(q, 3)) * q_rows, span)], load_sem.at[g]))
    head = [pltpu.make_async_copy(src.at[0], dst.at[0], load_sem.at[RADIX]) for src, dst in ((th_hbm, th_ref), (tl_hbm, tl_ref))]
    rest = [pltpu.make_async_copy(src.at[pl.ds(1, RADIX - 1)], dst.at[pl.ds(1, RADIX - 1)], load_sem.at[RADIX + 1])
            for src, dst in ((th_hbm, th_ref), (tl_hbm, tl_ref))]
    rest.append(pltpu.make_async_copy(turn_hbm, turn_ref, load_sem.at[RADIX + 2]))
    for load in loads[: 2 * SUB] + head:
        load.start()

    o, i = lax.axis_index("outer"), lax.axis_index("inner")
    me = o * n_inner + i
    slot = 0
    odelta, idelta = [], []
    for k in range(obits):
        bit = o // 2**k % 2
        slot = slot + bit * 2 ** (obits - 1 - k)
        odelta.append((1 - 2 * bit) * 2**k)
    for k in range(ibits):
        bit = i // 2**k % 2
        slot = slot + bit * 2 ** (ibits - 1 - k) * n_outer
        idelta.append((1 - 2 * bit) * 2**k)

    def peer(mo, mi):
        po, pi = o, i
        for k in range(obits):
            if mo >> k & 1:
                po = po + odelta[k]
        for k in range(ibits):
            if mi >> k & 1:
                pi = pi + idelta[k]
        return po, pi

    wide = n_inner // 4
    level, place_in = i // wide, i % wide
    half = n_inner // 2
    high = level // 2
    across = level + 1 - 2 * (level % 2)
    group = n_outer * wide

    def members(at):
        return [(peer(mo, 0)[0], at * wide + lax.rem(place_in + t, wide)) for t in range(wide) for mo in range(n_outer)]

    def ranked(at):
        return [(o2 + c, at * wide + t) for o2 in range(0, n_outer, 2) for t in range(wide) for c in range(2)]

    def pairs(far, near):
        return [p for pair in itertools.zip_longest(far, near) for p in pair if p is not None]

    own = members(level)[1:]
    first = pairs(ranked(2 - high), own) + members((1 - high) * across)
    second = ranked(high * across + (1 - high) * 3)
    order = pairs(ranked((1 - high) * 3) + ranked(2 - high), own + members(across))

    barrier = pltpu.get_barrier_semaphore()

    def greet(ring, at, who=None):
        for p in members(at) if who is None else who:
            pl.semaphore_signal(ring, inc=1, device_id=p, device_id_type=MESH)

    for at in (2 - high, (1 - high) * 3, across):
        pl.when(level < 3)(functools.partial(greet, barrier, at))
    greet(barrier, level, own)
    for load in loads[2 * SUB :] + rest:
        load.start()

    def meet():
        pl.semaphore_wait(barrier, 3 * group - 1 + group * (level // 3))

    def answer():
        for earlier in (2, 1, 0):
            pl.when(level == 3)(functools.partial(greet, last_sem, earlier))

    def meet_last():
        pl.when(level < 3)(lambda: pl.semaphore_wait(last_sem, group))

    rows, pitches = pieces_of(n_devices)

    def send(k, peers):
        dst = recvs[k].at[pl.ds(slot * pitches[k], rows[k])]
        for po, pi in peers:
            pltpu.make_async_remote_copy(
                src_ref=sends[k].at[pl.ds((po * n_inner + pi) * rows[k], rows[k])], dst_ref=dst,
                send_sem=send_sem, recv_sem=recv_sem.at[k],
                device_id=(po, pi), device_id_type=MESH).start()

    def own_copy(k):
        return pltpu.make_async_copy(
            sends[k].at[pl.ds(me * rows[k], rows[k])],
            recvs[k].at[pl.ds(slot * pitches[k], rows[k])], own_sem.at[k])

    def wait_rows(ref, count, sem):
        part = ref.at[pl.ds(0, count)]
        pltpu.make_async_copy(part, part, sem).wait()

    def rows_of(g, pair, ct, s):
        return [x_ref[pl.ds(g * SUB * q_rows + (2 * pair + w) * SUB + 2 * ct + s, SUB, stride=q_rows), :] for w in range(2)]

    def keep(chunk, g, pair, values):
        at = pl.ds((g * SUB + pair) * 2 * SUB, 2 * SUB)
        for s, value in enumerate(values):
            high, low = split_bf16(value)
            bh_ref[chunk, at, s * LANES : (s + 1) * LANES] = high
            bl_ref[chunk, at, s * LANES : (s + 1) * LANES] = low

    dims = (((1,), (1,)), ((), ()))

    def transform(k, place, chunk, groups):
        at = pl.ds(groups[0] * LANES, len(groups) * LANES)
        th, tl, bh, bl = th_ref[chunk], tl_ref[chunk], bh_ref[chunk, at, :], bl_ref[chunk, at, :]
        res = lax.dot_general(th, bh, dims, preferred_element_type=jnp.float32)
        res += lax.dot_general(th, bl, dims, preferred_element_type=jnp.float32)
        res += lax.dot_general(tl, bh, dims, preferred_element_type=jnp.float32)
        for e in range(n_devices):
            for n, g in enumerate(groups):
                sends[k][pl.ds(e * rows[k] + (place * RADIX + g) * SUB, SUB), :] = (
                    res[e * SUB : (e + 1) * SUB, n * LANES : (n + 1) * LANES])

    for g in range(RADIX):
        wait_rows(x_ref, SUB * span, load_sem.at[g])
        for pair in range(SUB):
            keep(0, g, pair, [
                jnp.concatenate([(a + c) + (b + d) for a, b, c, d in zip(*[rows_of(g, pair, ct, s) for ct in range(RADIX)])], 0)
                for s in range(2)])
        if g == 1:
            wait_rows(th_ref, 1, load_sem.at[RADIX])
            wait_rows(tl_ref, 1, load_sem.at[RADIX])
        if g % 2:
            transform(0, 0, 0, (g - 1, g))
    meet()
    send(0, first)
    answer()
    own_copy(0).start()

    zero = jnp.zeros((SUB, LANES), jnp.float32)
    squares, zr, zi = [zero] * 4, zero, zero
    for g in range(RADIX):
        for pair in range(SUB):
            part = [[rows_of(g, pair, ct, s) for s in range(2)] for ct in range(RADIX)]
            for ct in range(RADIX):
                for s in range(2):
                    for w in range(2):
                        squares[ct] = squares[ct] + part[ct][s][w] * part[ct][s][w]
            for w in range(2):
                angle = 2.0 * math.pi / total_len * n_devices * (rev(2 * pair + w, 4) * SUB * RADIX + rev(g, 2))
                cw, sw = math.cos(angle), math.sin(angle)
                zr = zr + (part[0][0][w] * cw + part[0][1][w] * sw)
                zi = zi + (part[0][1][w] * cw - part[0][0][w] * sw)
            (x0r, x0i), (x1r, x1i), (x2r, x2i), (x3r, x3i) = [
                [jnp.concatenate(part[ct][s], 0) for s in range(2)] for ct in range(RADIX)]
            br, bi, dr, di = x0r - x2r, x0i - x2i, x1r - x3r, x1i - x3i
            keep(1, g, pair, (br - di, bi + dr))
            keep(2, g, pair, ((x0r + x2r) - (x1r + x3r), (x0i + x2i) - (x1i + x3i)))
            keep(3, g, pair, (br + di, bi - dr))

    for ref in (th_ref, tl_ref):
        wait_rows(ref, RADIX - 1, load_sem.at[RADIX + 1])
    rest[-1].wait()
    pc, ps = turn_ref[2 * n_devices : 2 * n_devices + SUB, :], turn_ref[2 * n_devices + SUB :, :]
    oc, os_ = turn_ref[pl.ds(slot, 1), :], turn_ref[pl.ds(n_devices + slot, 1), :]
    total = jnp.sum(jnp.sum((squares[0] + squares[1]) + (squares[2] + squares[3]), 0, keepdims=True), 1, keepdims=True)
    yr = jnp.sum(zr * pc + zi * ps, 0, keepdims=True)
    yi = jnp.sum(zi * pc - zr * ps, 0, keepdims=True)
    wr = jnp.sum(yr * oc + yi * os_, 1, keepdims=True)
    wi = jnp.sum(yi * oc - yr * os_, 1, keepdims=True)
    lane = lax.broadcasted_iota(jnp.int32, (1, LANES), 1)
    stat = jnp.where(lane == 0, total, jnp.where(lane == 1, wr, jnp.where(lane == 2, wi, 0.0)))
    mine = pl.ds(o * half + i % half, 1)
    near_ref[mine, :] = stat

    def send_row(src, dst, sem, to):
        pltpu.make_async_remote_copy(
            src_ref=src, dst_ref=dst, send_sem=send_sem, recv_sem=stat_sem.at[sem],
            device_id=to, device_id_type=MESH).start()

    for k, chunks in list(enumerate(PIECES))[1:]:
        for place, chunk in enumerate(chunks):
            transform(k, place, chunk, range(RADIX))
        if k == 1:
            meet_last()
            send(0, second)
            for to in own + members(across):
                send_row(near_ref.at[mine], near_ref.at[mine], 0, to)
        if k == n_pieces - 1:
            wait_rows(near_ref, half * n_outer - 1, stat_sem.at[0])
            half_ref[...] = jnp.sum(near_ref[...], 0, keepdims=True)
            send_row(half_ref, far_ref, 1, peer(0, half))
        send(k, order)
        own_copy(k).start()

    for k, chunks in enumerate(PIECES):
        wait_rows(recvs[k], (n_devices - 1) * rows[k], recv_sem.at[k])
        own_copy(k).wait()
        if k == STAT:
            wait_rows(far_ref, 1, stat_sem.at[1])
            sums = half_ref[...] + far_ref[...]
            mean_square = jnp.sum(jnp.where(lane == 0, sums, 0.0), 1, keepdims=True) / total_len
            shifted = mean_square + 1e-06
            factor = lax.rsqrt(shifted)
            factor = factor * (1.5 - 0.5 * shifted * factor * factor)
            checks = jnp.where(lane == 0, mean_square, sums * (factor / math.sqrt(total_len)))
            tot_ref[...] = jnp.broadcast_to(checks, (SUB, LANES))
            factor = jnp.broadcast_to(factor, (SUB, LANES))
            fac_ref[...] = factor
        ready = range(STAT + 1) if k == STAT else [k] if STAT < k < n_pieces - 1 else []
        for kk in ready:
            for place, chunk in enumerate(PIECES[kk]):
                for h in range(SUB):
                    base = ((h // 2) * (RADIX - 1) + chunk) * 2 * LANES + h % 2
                    for m, v in enumerate(turn_tiles(recvs[kk], pitches[kk], place, h, n_devices, factor)):
                        field[pl.ds(base + rev(m, 4) * 2 * SUB, SUB, stride=2), :] = v
    for k in range(n_pieces):
        wait_rows(sends[k], (n_devices - 1) * rows[k], send_sem)
    wait_rows(near_ref, half * n_outer, send_sem)


def finish_kernel(n_devices, pitch, field, last, tot_ref, fac_ref, out_hbm, checks_hbm, turned, checks_ref, sem):
    f_rows = 2 * LANES
    many = (RADIX - 1) * f_rows
    stores = []
    for fq in range(RADIX):
        stores.append(pltpu.make_async_copy(
            field.at[pl.ds(fq * many, many)], out_hbm.at[pl.ds(fq * RADIX * f_rows, many)], sem.at[fq]))
        stores[-1].start()
    checks_ref[...] = tot_ref[0:1, 0:3]
    stores.append(pltpu.make_async_copy(checks_ref, checks_hbm, sem.at[2 * RADIX]))
    stores[-1].start()
    factor = fac_ref[...]
    for h in range(SUB):
        base = h // 2 * f_rows + h % 2
        for m, v in enumerate(turn_tiles(last, pitch, 0, h, n_devices, factor)):
            turned[pl.ds(base + rev(m, 4) * 2 * SUB, SUB, stride=2), :] = v
        if h % 2:
            fq = h // 2
            stores.append(pltpu.make_async_copy(
                turned.at[pl.ds(fq * f_rows, f_rows)],
                out_hbm.at[pl.ds((fq * RADIX + RADIX - 1) * f_rows, f_rows)], sem.at[RADIX + fq]))
            stores[-1].start()
    for store in stores:
        store.wait()


def fast(n_outer, n_inner, amplitudes):
    amp_dev = amplitudes.shape[1]
    n_devices = n_outer * n_inner
    rows_count = amp_dev // COLUMNS
    total_len = amp_dev * n_devices
    view = amplitudes.reshape(2, amp_dev // LANES, LANES).transpose(1, 0, 2).reshape(-1, LANES)
    table, turn = tables(n_devices, total_len)
    th = table.astype(jnp.bfloat16)
    tl = (table - th.astype(np.float32)).astype(jnp.bfloat16)
    hbm, vmem = pl.BlockSpec(memory_space=pltpu.HBM), pl.BlockSpec(memory_space=pltpu.VMEM)
    rows, pitches = pieces_of(n_devices)
    small = pltpu.VMEM((SUB, LANES), jnp.float32)
    f_rows = 2 * LANES
    pair = pltpu.VMEM((RADIX, rows_count, 2 * LANES), jnp.bfloat16)
    scratch = [
        pltpu.VMEM((RADIX * SUB * (LANES + 4), LANES), jnp.float32),
        pltpu.VMEM(th.shape, jnp.bfloat16),
        pltpu.VMEM(tl.shape, jnp.bfloat16),
        pltpu.VMEM(turn.shape, jnp.float32),
        pair,
        pair,
        *[pltpu.VMEM((n_devices * r, LANES), jnp.float32) for r in rows],
        *[pltpu.VMEM((n_devices * p, LANES), jnp.float32) for p in pitches[:-1]],
        pltpu.VMEM((n_devices // 2, LANES), jnp.float32),
        pltpu.VMEM((1, LANES), jnp.float32),
        pltpu.VMEM((1, LANES), jnp.float32),
        pltpu.SemaphoreType.DMA,
        pltpu.SemaphoreType.DMA((len(PIECES),)),
        pltpu.SemaphoreType.DMA((len(PIECES),)),
        pltpu.SemaphoreType.DMA((RADIX + 3,)),
        pltpu.SemaphoreType.REGULAR,
        pltpu.SemaphoreType.DMA((2,)),
    ]
    parts = pl.pallas_call(
        functools.partial(kernel, n_outer, n_inner, total_len),
        out_shape=(
            pltpu.VMEM((RADIX * (RADIX - 1) * f_rows, LANES), jnp.float32),
            pltpu.VMEM((n_devices * pitches[-1], LANES), jnp.float32),
            small,
            small,
        ),
        in_specs=[hbm] * 4,
        out_specs=(vmem,) * 4,
        scratch_shapes=scratch,
        compiler_params=pltpu.CompilerParams(collective_id=0, has_side_effects=True, vmem_limit_bytes=32_000_000),
    )(*[pltpu.with_memory_space_constraint(v, pltpu.HBM) for v in (view, jnp.asarray(th), jnp.asarray(tl), jnp.asarray(turn))])
    field, checks = pl.pallas_call(
        functools.partial(finish_kernel, n_devices, pitches[-1]),
        out_shape=(jax.ShapeDtypeStruct(view.shape, jnp.float32), jax.ShapeDtypeStruct((1, 3), jnp.float32)),
        in_specs=[vmem] * 4,
        out_specs=(hbm, hbm),
        scratch_shapes=[
            pltpu.VMEM((RADIX * f_rows, LANES), jnp.float32),
            pltpu.VMEM((1, 3), jnp.float32),
            pltpu.SemaphoreType.DMA((2 * RADIX + 1,)),
        ],
        compiler_params=pltpu.CompilerParams(vmem_limit_bytes=32_000_000),
    )(*parts)
    result = field.reshape(-1, 2, LANES).transpose(1, 0, 2).reshape(2, amp_dev)
    return result, checks.reshape(3)


def reverse_index(values, count):
    result = jnp.zeros_like(values)
    for bit_pos in range(count):
        result = result | (values >> bit_pos & 1) << count - 1 - bit_pos
    return result


def reversal_table(size, count):
    indices = jnp.arange(size, dtype=jnp.int32)
    return (reverse_index(indices, count)[:, None] == indices[None, :]).astype(jnp.float32)


def check_terms(current, positions, angle_scale):
    angles = positions.astype(jnp.float32) * angle_scale
    cosine = jnp.cos(angles)
    sine = jnp.sin(angles)
    squares = jnp.sum(current * current)
    phase_real = jnp.sum(current[0] * cosine + current[1] * sine)
    phase_imag = jnp.sum(current[1] * cosine - current[0] * sine)
    return (squares, phase_real, phase_imag)


def per_device(amplitudes):
    amp_dev = amplitudes.shape[1]
    n_outer = lax.axis_size("outer")
    n_inner = lax.axis_size("inner")
    outer_bits = n_outer.bit_length() - 1
    inner_bits = n_inner.bit_length() - 1
    global_bits = outer_bits + inner_bits
    local_bits = amp_dev.bit_length() - 1
    n_devices = n_outer * n_inner
    high_count = amp_dev // n_devices
    total_len = amp_dev * n_devices
    columns = 2**WINDOW
    rows_count = amp_dev // columns
    column_ids = jnp.arange(columns, dtype=jnp.int32)
    reversed_ids = reverse_index(column_ids, WINDOW)
    products = column_ids[:, None] * reversed_ids[None, :] % columns
    angles = products.astype(jnp.float32) * (2.0 * math.pi / columns)
    real_part = jnp.cos(angles) / math.sqrt(columns)
    imag_part = jnp.sin(angles) / math.sqrt(columns)
    table = jnp.concatenate(
        [jnp.concatenate([real_part, imag_part], 1), jnp.concatenate([-imag_part, real_part], 1)], 0
    )
    stacked = jnp.concatenate(
        [amplitudes[0].reshape(rows_count, columns), amplitudes[1].reshape(rows_count, columns)], 1
    )
    result = jnp.dot(
        stacked, table, precision=lax.Precision.HIGHEST, preferred_element_type=jnp.float32
    )
    windowed = jnp.stack([result[:, :columns].reshape(-1), result[:, columns:].reshape(-1)])
    device_id = lax.axis_index("outer") * n_inner + lax.axis_index("inner")
    angle_scale = 2.0 * math.pi / total_len
    local_ids = jnp.arange(amp_dev, dtype=jnp.int32)
    positions = reverse_index(device_id * amp_dev + local_ids, local_bits + global_bits)
    totals = lax.psum(check_terms(windowed, positions, angle_scale), ("outer", "inner"))
    device_table = reversal_table(n_devices, global_bits)
    high_table = reversal_table(high_count, local_bits - global_bits)
    grid = windowed.reshape(2, high_count, n_devices)
    ordered = jnp.einsum("pm,shm->sph", device_table, grid, precision=lax.Precision.HIGHEST)
    blocks = ordered.reshape(2, n_outer, n_inner, high_count)
    blocks = lax.all_to_all(
        lax.all_to_all(blocks, "outer", split_axis=1, concat_axis=1, tiled=True),
        "inner",
        split_axis=2,
        concat_axis=2,
        tiled=True,
    )
    received = blocks.reshape(2, n_devices, high_count)
    turned_high = jnp.einsum("qh,sdh->sdq", high_table, received, precision=lax.Precision.HIGHEST)
    placed = jnp.einsum("ed,sdq->sqe", device_table, turned_high, precision=lax.Precision.HIGHEST)
    reversed_field = placed.reshape(2, amp_dev)
    mean_square = totals[0] / total_len
    factor = lax.rsqrt(mean_square + 1e-06)
    scaled = factor / math.sqrt(total_len)
    checks = jnp.stack([mean_square, totals[1] * scaled, totals[2] * scaled])
    return (reversed_field * factor, checks)


def solution(mesh):
    n_outer, n_inner = mesh.shape["outer"], mesh.shape["inner"]

    def body(amplitudes):
        rows_count = amplitudes.shape[1] // COLUMNS
        n_devices = n_outer * n_inner
        if rows_count * n_devices == LANES * LANES and n_devices * SUB == 2 * LANES and n_inner % 4 == 0:
            return fast(n_outer, n_inner, amplitudes)
        return per_device(amplitudes)

    return jax.shard_map(
        body,
        mesh=mesh,
        in_specs=(P(None, ("outer", "inner")),),
        out_specs=(P(None, ("outer", "inner")), P()),
        check_vma=False,
    )
```

```python
import functools
import itertools
import math

import jax
import jax.numpy as jnp
import numpy as np
from jax import lax
from jax.experimental import pallas as pl
from jax.experimental.pallas import tpu as pltpu
from jax.sharding import PartitionSpec as P

WINDOW = 9
COLUMNS = 2**WINDOW
LANES = 128
SUB = 8
RADIX = COLUMNS // LANES
PIECES = ((0,), (1, 2), (3,))
STAT = 1
MESH = pl.DeviceIdType.MESH


def rev(value, count):
    out = 0
    for bit in range(count):
        out |= (value >> bit & 1) << (count - 1 - bit)
    return out


def split_bf16(values):
    high = values.astype(jnp.bfloat16)
    return high, (values - high.astype(np.float32)).astype(jnp.bfloat16)


def tables(n_devices, total_len):
    f = np.arange(COLUMNS).reshape(LANES, RADIX).T
    lane = np.arange(LANES)
    ang = (f[:, :, None] * lane) % COLUMNS * (2.0 * np.pi / COLUMNS)
    c, s = np.cos(ang) / math.sqrt(COLUMNS), np.sin(ang) / math.sqrt(COLUMNS)
    table = np.stack([np.concatenate([c, -s], -1), np.concatenate([s, c], -1)], 2)
    table = table.reshape(RADIX, 2 * LANES, 2 * LANES).astype(np.float32)
    slots = 2.0 * np.pi / total_len * np.arange(n_devices)
    subs = 2.0 * np.pi / total_len * n_devices * RADIX * np.arange(SUB)
    turn = np.zeros((2 * (n_devices + SUB), LANES), np.float32)
    turn[:n_devices], turn[n_devices : 2 * n_devices] = np.cos(slots)[:, None], np.sin(slots)[:, None]
    turn[2 * n_devices : 2 * n_devices + SUB, 1] = np.cos(subs) * math.sqrt(COLUMNS)
    turn[2 * n_devices + SUB :, 1] = np.sin(subs) * math.sqrt(COLUMNS)
    return table, turn


def pieces_of(n_devices):
    rows = [len(chunks) * RADIX * SUB for chunks in PIECES]
    return rows, [r + 4 for r in rows]


def turn_tiles(recv, pitch, place, h, n_devices, factor):
    tile = jnp.concatenate(
        [recv[pl.ds((place * RADIX + rev(j, 2)) * SUB + h, n_devices, stride=pitch), :] for j in range(RADIX)], 0)
    turned = tile.T.reshape(LANES // SUB, SUB, LANES)
    return [turned[m] * factor for m in range(LANES // SUB)]


def kernel(n_outer, n_inner, total_len, x_hbm, th_hbm, tl_hbm, turn_hbm, *refs):
    n_pieces = len(PIECES)
    field, last, tot_ref, fac_ref, x_ref, th_ref, tl_ref, turn_ref, bh_ref, bl_ref = refs[:10]
    sends, recvs = refs[10 : 10 + n_pieces], [*refs[10 + n_pieces : 9 + 2 * n_pieces], last]
    near_ref, half_ref, far_ref, send_sem, recv_sem, own_sem, load_sem, last_sem, stat_sem = refs[9 + 2 * n_pieces :]
    n_devices = n_outer * n_inner
    obits, ibits = n_outer.bit_length() - 1, n_inner.bit_length() - 1
    span = LANES
    q_rows = span + 4

    loads = []
    for g in range(RADIX):
        for q in range(SUB):
            loads.append(pltpu.make_async_copy(
                x_hbm.at[pl.ds((g * SUB + q) * span, span)],
                x_ref.at[pl.ds((g * SUB + rev(q, 3)) * q_rows, span)], load_sem.at[g]))
    head = [pltpu.make_async_copy(src.at[0], dst.at[0], load_sem.at[RADIX]) for src, dst in ((th_hbm, th_ref), (tl_hbm, tl_ref))]
    rest = [pltpu.make_async_copy(src.at[pl.ds(1, RADIX - 1)], dst.at[pl.ds(1, RADIX - 1)], load_sem.at[RADIX + 1])
            for src, dst in ((th_hbm, th_ref), (tl_hbm, tl_ref))]
    rest.append(pltpu.make_async_copy(turn_hbm, turn_ref, load_sem.at[RADIX + 2]))
    for load in loads[: 2 * SUB] + head:
        load.start()

    o, i = lax.axis_index("outer"), lax.axis_index("inner")
    me = o * n_inner + i
    slot = 0
    odelta, idelta = [], []
    for k in range(obits):
        bit = o // 2**k % 2
        slot = slot + bit * 2 ** (obits - 1 - k)
        odelta.append((1 - 2 * bit) * 2**k)
    for k in range(ibits):
        bit = i // 2**k % 2
        slot = slot + bit * 2 ** (ibits - 1 - k) * n_outer
        idelta.append((1 - 2 * bit) * 2**k)

    def peer(mo, mi):
        po, pi = o, i
        for k in range(obits):
            if mo >> k & 1:
                po = po + odelta[k]
        for k in range(ibits):
            if mi >> k & 1:
                pi = pi + idelta[k]
        return po, pi

    wide = n_inner // 4
    level, place_in = i // wide, i % wide
    half = n_inner // 2
    high = level // 2
    across = level + 1 - 2 * (level % 2)
    group = n_outer * wide

    def members(at):
        return [(peer(mo, 0)[0], at * wide + lax.rem(place_in + t, wide)) for t in range(wide) for mo in range(n_outer)]

    def ranked(at):
        return [(o2 + c, at * wide + t) for o2 in range(0, n_outer, 2) for t in range(wide) for c in range(2)]

    def pairs(far, near):
        return [p for pair in itertools.zip_longest(far, near) for p in pair if p is not None]

    own = members(level)[1:]
    first = ranked(2 - high)[:-2]
    then = members((1 - high) * across)
    second = ranked(2 - high)[-2:] + pairs(ranked(high * across + (1 - high) * 3), own)
    order = ranked((1 - high) * 3) + ranked(2 - high) + own + members(across)
    left = pairs(ranked((1 - high) * 3) + ranked(2 - high)[-2:], own + members(across))

    barrier = pltpu.get_barrier_semaphore()

    def greet(ring, at, who=None):
        for p in members(at) if who is None else who:
            pl.semaphore_signal(ring, inc=1, device_id=p, device_id_type=MESH)

    tail = ranked(2)[-2:] + ranked(3)
    late = (level == 3) | (level == 2) & (o >= n_outer - 2) & (place_in == wide - 1)
    for at in (2 - high, (1 - high) * 3, across):
        pl.when(~late)(functools.partial(greet, barrier, at))
    pl.when(~late)(functools.partial(greet, barrier, level, own))
    for p in tail:
        pl.when(late & ((p[0] != o) | (p[1] != i)))(functools.partial(greet, barrier, level, [p]))
    for load in loads[2 * SUB :] + rest:
        load.start()

    def meet():
        pl.semaphore_wait(barrier, n_devices - 1 - len(tail) + len(tail) * late.astype(jnp.int32))

    def answer():
        for p in ranked(0) + ranked(1) + ranked(2)[:-2]:
            pl.when(late)(functools.partial(greet, last_sem, level, [p]))

    def meet_last():
        pl.when(~late)(lambda: pl.semaphore_wait(last_sem, len(tail)))

    rows, pitches = pieces_of(n_devices)

    def send(k, peers):
        dst = recvs[k].at[pl.ds(slot * pitches[k], rows[k])]
        for po, pi in peers:
            pltpu.make_async_remote_copy(
                src_ref=sends[k].at[pl.ds((po * n_inner + pi) * rows[k], rows[k])], dst_ref=dst,
                send_sem=send_sem, recv_sem=recv_sem.at[k],
                device_id=(po, pi), device_id_type=MESH).start()

    def own_copy(k):
        return pltpu.make_async_copy(
            sends[k].at[pl.ds(me * rows[k], rows[k])],
            recvs[k].at[pl.ds(slot * pitches[k], rows[k])], own_sem.at[k])

    def wait_rows(ref, count, sem):
        part = ref.at[pl.ds(0, count)]
        pltpu.make_async_copy(part, part, sem).wait()

    def rows_of(g, pair, ct, s):
        return [x_ref[pl.ds(g * SUB * q_rows + (2 * pair + w) * SUB + 2 * ct + s, SUB, stride=q_rows), :] for w in range(2)]

    def keep(chunk, g, pair, values):
        at = pl.ds((g * SUB + pair) * 2 * SUB, 2 * SUB)
        for s, value in enumerate(values):
            high, low = split_bf16(value)
            bh_ref[chunk, at, s * LANES : (s + 1) * LANES] = high
            bl_ref[chunk, at, s * LANES : (s + 1) * LANES] = low

    dims = (((1,), (1,)), ((), ()))

    def transform(k, place, chunk, groups, side=None):
        at = pl.ds(groups[0] * LANES, len(groups) * LANES)
        th, tl, bh, bl = th_ref[chunk], tl_ref[chunk], bh_ref[chunk, at, :], bl_ref[chunk, at, :]
        starts = range(n_devices)
        if side is not None:
            count = half * SUB
            heads = [o2 * n_inner + side * half for o2 in range(n_outer)]
            th, tl = [jnp.concatenate([ref[chunk, pl.ds(pl.multiple_of(e * SUB, count), count), :] for e in heads], 0)
                      for ref in (th_ref, tl_ref)]
            starts = [e + n for e in heads for n in range(half)]
        res = lax.dot_general(th, bh, dims, preferred_element_type=jnp.float32)
        res += lax.dot_general(th, bl, dims, preferred_element_type=jnp.float32)
        res += lax.dot_general(tl, bh, dims, preferred_element_type=jnp.float32)
        for m, e in enumerate(starts):
            for n, g in enumerate(groups):
                sends[k][pl.ds(pl.multiple_of(e * rows[k] + (place * RADIX + g) * SUB, SUB), SUB), :] = (
                    res[m * SUB : (m + 1) * SUB, n * LANES : (n + 1) * LANES])

    for g in range(RADIX):
        wait_rows(x_ref, SUB * span, load_sem.at[g])
        for pair in range(SUB):
            keep(0, g, pair, [
                jnp.concatenate([(a + c) + (b + d) for a, b, c, d in zip(*[rows_of(g, pair, ct, s) for ct in range(RADIX)])], 0)
                for s in range(2)])
        if g == 1:
            wait_rows(th_ref, 1, load_sem.at[RADIX])
            wait_rows(tl_ref, 1, load_sem.at[RADIX])
        if g % 2:
            transform(0, 0, 0, (g - 1, g), 1 - high)
    meet()
    send(0, first)
    answer()
    transform(0, 0, 0, range(RADIX), high)
    send(0, then)
    own_copy(0).start()

    zero = jnp.zeros((SUB, LANES), jnp.float32)
    squares, zr, zi = [zero] * 4, zero, zero
    for g in range(RADIX):
        for pair in range(SUB):
            part = [[rows_of(g, pair, ct, s) for s in range(2)] for ct in range(RADIX)]
            for ct in range(RADIX):
                for s in range(2):
                    for w in range(2):
                        squares[ct] = squares[ct] + part[ct][s][w] * part[ct][s][w]
            for w in range(2):
                angle = 2.0 * math.pi / total_len * n_devices * (rev(2 * pair + w, 4) * SUB * RADIX + rev(g, 2))
                cw, sw = math.cos(angle), math.sin(angle)
                zr = zr + (part[0][0][w] * cw + part[0][1][w] * sw)
                zi = zi + (part[0][1][w] * cw - part[0][0][w] * sw)
            (x0r, x0i), (x1r, x1i), (x2r, x2i), (x3r, x3i) = [
                [jnp.concatenate(part[ct][s], 0) for s in range(2)] for ct in range(RADIX)]
            br, bi, dr, di = x0r - x2r, x0i - x2i, x1r - x3r, x1i - x3i
            keep(1, g, pair, (br - di, bi + dr))
            keep(2, g, pair, ((x0r + x2r) - (x1r + x3r), (x0i + x2i) - (x1i + x3i)))
            keep(3, g, pair, (br + di, bi - dr))

    for ref in (th_ref, tl_ref):
        wait_rows(ref, RADIX - 1, load_sem.at[RADIX + 1])
    rest[-1].wait()
    pc, ps = turn_ref[2 * n_devices : 2 * n_devices + SUB, :], turn_ref[2 * n_devices + SUB :, :]
    oc, os_ = turn_ref[pl.ds(slot, 1), :], turn_ref[pl.ds(n_devices + slot, 1), :]
    total = jnp.sum(jnp.sum((squares[0] + squares[1]) + (squares[2] + squares[3]), 0, keepdims=True), 1, keepdims=True)
    yr = jnp.sum(zr * pc + zi * ps, 0, keepdims=True)
    yi = jnp.sum(zi * pc - zr * ps, 0, keepdims=True)
    wr = jnp.sum(yr * oc + yi * os_, 1, keepdims=True)
    wi = jnp.sum(yi * oc - yr * os_, 1, keepdims=True)
    lane = lax.broadcasted_iota(jnp.int32, (1, LANES), 1)
    stat = jnp.where(lane == 0, total, jnp.where(lane == 1, wr, jnp.where(lane == 2, wi, 0.0)))
    mine = pl.ds(o * half + i % half, 1)
    near_ref[mine, :] = stat

    def send_row(src, dst, sem, to):
        pltpu.make_async_remote_copy(
            src_ref=src, dst_ref=dst, send_sem=send_sem, recv_sem=stat_sem.at[sem],
            device_id=to, device_id_type=MESH).start()

    for k, chunks in list(enumerate(PIECES))[1:]:
        for place, chunk in enumerate(chunks):
            transform(k, place, chunk, range(RADIX))
        if k == 1:
            send(1, first)
            meet_last()
            send(0, second)
            for to in own + members(across):
                send_row(near_ref.at[mine], near_ref.at[mine], 0, to)
        if k == n_pieces - 1:
            wait_rows(near_ref, half * n_outer - 1, stat_sem.at[0])
            half_ref[...] = jnp.sum(near_ref[...], 0, keepdims=True)
            send_row(half_ref, far_ref, 1, peer(0, half))
        send(k, left if k == 1 else order)
        own_copy(k).start()

    for k, chunks in enumerate(PIECES):
        wait_rows(recvs[k], (n_devices - 1) * rows[k], recv_sem.at[k])
        own_copy(k).wait()
        if k == STAT:
            wait_rows(far_ref, 1, stat_sem.at[1])
            sums = half_ref[...] + far_ref[...]
            mean_square = jnp.sum(jnp.where(lane == 0, sums, 0.0), 1, keepdims=True) / total_len
            shifted = mean_square + 1e-06
            factor = lax.rsqrt(shifted)
            factor = factor * (1.5 - 0.5 * shifted * factor * factor)
            checks = jnp.where(lane == 0, mean_square, sums * (factor / math.sqrt(total_len)))
            tot_ref[...] = jnp.broadcast_to(checks, (SUB, LANES))
            factor = jnp.broadcast_to(factor, (SUB, LANES))
            fac_ref[...] = factor
        ready = range(STAT + 1) if k == STAT else [k] if STAT < k < n_pieces - 1 else []
        for kk in ready:
            for place, chunk in enumerate(PIECES[kk]):
                for h in range(SUB):
                    base = ((h // 2) * (RADIX - 1) + chunk) * 2 * LANES + h % 2
                    for m, v in enumerate(turn_tiles(recvs[kk], pitches[kk], place, h, n_devices, factor)):
                        field[pl.ds(base + rev(m, 4) * 2 * SUB, SUB, stride=2), :] = v
    for k in range(n_pieces):
        wait_rows(sends[k], (n_devices - 1) * rows[k], send_sem)
    wait_rows(near_ref, half * n_outer, send_sem)


def finish_kernel(n_devices, pitch, field, last, tot_ref, fac_ref, out_hbm, checks_hbm, turned, checks_ref, sem):
    f_rows = 2 * LANES
    many = (RADIX - 1) * f_rows
    stores = []
    for fq in range(RADIX):
        stores.append(pltpu.make_async_copy(
            field.at[pl.ds(fq * many, many)], out_hbm.at[pl.ds(fq * RADIX * f_rows, many)], sem.at[fq]))
        stores[-1].start()
    checks_ref[...] = tot_ref[0:1, 0:3]
    stores.append(pltpu.make_async_copy(checks_ref, checks_hbm, sem.at[2 * RADIX]))
    stores[-1].start()
    factor = fac_ref[...]
    for h in range(SUB):
        base = h // 2 * f_rows + h % 2
        for m, v in enumerate(turn_tiles(last, pitch, 0, h, n_devices, factor)):
            turned[pl.ds(base + rev(m, 4) * 2 * SUB, SUB, stride=2), :] = v
        if h % 2:
            fq = h // 2
            stores.append(pltpu.make_async_copy(
                turned.at[pl.ds(fq * f_rows, f_rows)],
                out_hbm.at[pl.ds((fq * RADIX + RADIX - 1) * f_rows, f_rows)], sem.at[RADIX + fq]))
            stores[-1].start()
    for store in stores:
        store.wait()


def fast(n_outer, n_inner, amplitudes):
    amp_dev = amplitudes.shape[1]
    n_devices = n_outer * n_inner
    rows_count = amp_dev // COLUMNS
    total_len = amp_dev * n_devices
    view = amplitudes.reshape(2, amp_dev // LANES, LANES).transpose(1, 0, 2).reshape(-1, LANES)
    table, turn = tables(n_devices, total_len)
    th = table.astype(jnp.bfloat16)
    tl = (table - th.astype(np.float32)).astype(jnp.bfloat16)
    hbm, vmem = pl.BlockSpec(memory_space=pltpu.HBM), pl.BlockSpec(memory_space=pltpu.VMEM)
    rows, pitches = pieces_of(n_devices)
    small = pltpu.VMEM((SUB, LANES), jnp.float32)
    f_rows = 2 * LANES
    pair = pltpu.VMEM((RADIX, rows_count, 2 * LANES), jnp.bfloat16)
    scratch = [
        pltpu.VMEM((RADIX * SUB * (LANES + 4), LANES), jnp.float32),
        pltpu.VMEM(th.shape, jnp.bfloat16),
        pltpu.VMEM(tl.shape, jnp.bfloat16),
        pltpu.VMEM(turn.shape, jnp.float32),
        pair,
        pair,
        *[pltpu.VMEM((n_devices * r, LANES), jnp.float32) for r in rows],
        *[pltpu.VMEM((n_devices * p, LANES), jnp.float32) for p in pitches[:-1]],
        pltpu.VMEM((n_devices // 2, LANES), jnp.float32),
        pltpu.VMEM((1, LANES), jnp.float32),
        pltpu.VMEM((1, LANES), jnp.float32),
        pltpu.SemaphoreType.DMA,
        pltpu.SemaphoreType.DMA((len(PIECES),)),
        pltpu.SemaphoreType.DMA((len(PIECES),)),
        pltpu.SemaphoreType.DMA((RADIX + 3,)),
        pltpu.SemaphoreType.REGULAR,
        pltpu.SemaphoreType.DMA((2,)),
    ]
    parts = pl.pallas_call(
        functools.partial(kernel, n_outer, n_inner, total_len),
        out_shape=(
            pltpu.VMEM((RADIX * (RADIX - 1) * f_rows, LANES), jnp.float32),
            pltpu.VMEM((n_devices * pitches[-1], LANES), jnp.float32),
            small,
            small,
        ),
        in_specs=[hbm] * 4,
        out_specs=(vmem,) * 4,
        scratch_shapes=scratch,
        compiler_params=pltpu.CompilerParams(collective_id=0, has_side_effects=True, vmem_limit_bytes=32_000_000),
    )(*[pltpu.with_memory_space_constraint(v, pltpu.HBM) for v in (view, jnp.asarray(th), jnp.asarray(tl), jnp.asarray(turn))])
    field, checks = pl.pallas_call(
        functools.partial(finish_kernel, n_devices, pitches[-1]),
        out_shape=(jax.ShapeDtypeStruct(view.shape, jnp.float32), jax.ShapeDtypeStruct((1, 3), jnp.float32)),
        in_specs=[vmem] * 4,
        out_specs=(hbm, hbm),
        scratch_shapes=[
            pltpu.VMEM((RADIX * f_rows, LANES), jnp.float32),
            pltpu.VMEM((1, 3), jnp.float32),
            pltpu.SemaphoreType.DMA((2 * RADIX + 1,)),
        ],
        compiler_params=pltpu.CompilerParams(vmem_limit_bytes=32_000_000),
    )(*parts)
    result = field.reshape(-1, 2, LANES).transpose(1, 0, 2).reshape(2, amp_dev)
    return result, checks.reshape(3)


def reverse_index(values, count):
    result = jnp.zeros_like(values)
    for bit_pos in range(count):
        result = result | (values >> bit_pos & 1) << count - 1 - bit_pos
    return result


def reversal_table(size, count):
    indices = jnp.arange(size, dtype=jnp.int32)
    return (reverse_index(indices, count)[:, None] == indices[None, :]).astype(jnp.float32)


def check_terms(current, positions, angle_scale):
    angles = positions.astype(jnp.float32) * angle_scale
    cosine = jnp.cos(angles)
    sine = jnp.sin(angles)
    squares = jnp.sum(current * current)
    phase_real = jnp.sum(current[0] * cosine + current[1] * sine)
    phase_imag = jnp.sum(current[1] * cosine - current[0] * sine)
    return (squares, phase_real, phase_imag)


def per_device(amplitudes):
    amp_dev = amplitudes.shape[1]
    n_outer = lax.axis_size("outer")
    n_inner = lax.axis_size("inner")
    outer_bits = n_outer.bit_length() - 1
    inner_bits = n_inner.bit_length() - 1
    global_bits = outer_bits + inner_bits
    local_bits = amp_dev.bit_length() - 1
    n_devices = n_outer * n_inner
    high_count = amp_dev // n_devices
    total_len = amp_dev * n_devices
    columns = 2**WINDOW
    rows_count = amp_dev // columns
    column_ids = jnp.arange(columns, dtype=jnp.int32)
    reversed_ids = reverse_index(column_ids, WINDOW)
    products = column_ids[:, None] * reversed_ids[None, :] % columns
    angles = products.astype(jnp.float32) * (2.0 * math.pi / columns)
    real_part = jnp.cos(angles) / math.sqrt(columns)
    imag_part = jnp.sin(angles) / math.sqrt(columns)
    table = jnp.concatenate(
        [jnp.concatenate([real_part, imag_part], 1), jnp.concatenate([-imag_part, real_part], 1)], 0
    )
    stacked = jnp.concatenate(
        [amplitudes[0].reshape(rows_count, columns), amplitudes[1].reshape(rows_count, columns)], 1
    )
    result = jnp.dot(
        stacked, table, precision=lax.Precision.HIGHEST, preferred_element_type=jnp.float32
    )
    windowed = jnp.stack([result[:, :columns].reshape(-1), result[:, columns:].reshape(-1)])
    device_id = lax.axis_index("outer") * n_inner + lax.axis_index("inner")
    angle_scale = 2.0 * math.pi / total_len
    local_ids = jnp.arange(amp_dev, dtype=jnp.int32)
    positions = reverse_index(device_id * amp_dev + local_ids, local_bits + global_bits)
    totals = lax.psum(check_terms(windowed, positions, angle_scale), ("outer", "inner"))
    device_table = reversal_table(n_devices, global_bits)
    high_table = reversal_table(high_count, local_bits - global_bits)
    grid = windowed.reshape(2, high_count, n_devices)
    ordered = jnp.einsum("pm,shm->sph", device_table, grid, precision=lax.Precision.HIGHEST)
    blocks = ordered.reshape(2, n_outer, n_inner, high_count)
    blocks = lax.all_to_all(
        lax.all_to_all(blocks, "outer", split_axis=1, concat_axis=1, tiled=True),
        "inner",
        split_axis=2,
        concat_axis=2,
        tiled=True,
    )
    received = blocks.reshape(2, n_devices, high_count)
    turned_high = jnp.einsum("qh,sdh->sdq", high_table, received, precision=lax.Precision.HIGHEST)
    placed = jnp.einsum("ed,sdq->sqe", device_table, turned_high, precision=lax.Precision.HIGHEST)
    reversed_field = placed.reshape(2, amp_dev)
    mean_square = totals[0] / total_len
    factor = lax.rsqrt(mean_square + 1e-06)
    scaled = factor / math.sqrt(total_len)
    checks = jnp.stack([mean_square, totals[1] * scaled, totals[2] * scaled])
    return (reversed_field * factor, checks)


def solution(mesh):
    n_outer, n_inner = mesh.shape["outer"], mesh.shape["inner"]

    def body(amplitudes):
        rows_count = amplitudes.shape[1] // COLUMNS
        n_devices = n_outer * n_inner
        if rows_count * n_devices == LANES * LANES and n_devices * SUB == 2 * LANES and n_inner % 4 == 0:
            return fast(n_outer, n_inner, amplitudes)
        return per_device(amplitudes)

    return jax.shard_map(
        body,
        mesh=mesh,
        in_specs=(P(None, ("outer", "inner")),),
        out_specs=(P(None, ("outer", "inner")), P()),
        check_vma=False,
    )
```

```python
import functools
import itertools
import math

import jax
import jax.numpy as jnp
import numpy as np
from jax import lax
from jax.experimental import pallas as pl
from jax.experimental.pallas import tpu as pltpu
from jax.sharding import PartitionSpec as P

WINDOW = 9
COLUMNS = 2**WINDOW
LANES = 128
SUB = 8
RADIX = COLUMNS // LANES
PIECES = ((0,), (1, 2), (3,))
STAT = 1
MESH = pl.DeviceIdType.MESH


def rev(value, count):
    out = 0
    for bit in range(count):
        out |= (value >> bit & 1) << (count - 1 - bit)
    return out


def split_bf16(values):
    high = values.astype(jnp.bfloat16)
    return high, (values - high.astype(np.float32)).astype(jnp.bfloat16)


def tables(n_devices, total_len):
    f = np.arange(COLUMNS).reshape(LANES, RADIX).T
    lane = np.arange(LANES)
    ang = (f[:, :, None] * lane) % COLUMNS * (2.0 * np.pi / COLUMNS)
    c, s = np.cos(ang) / math.sqrt(COLUMNS), np.sin(ang) / math.sqrt(COLUMNS)
    table = np.stack([np.concatenate([c, -s], -1), np.concatenate([s, c], -1)], 2)
    table = table.reshape(RADIX, 2 * LANES, 2 * LANES).astype(np.float32)
    slots = 2.0 * np.pi / total_len * np.arange(n_devices)
    subs = 2.0 * np.pi / total_len * n_devices * RADIX * np.arange(SUB)
    turn = np.zeros((2 * (n_devices + SUB), LANES), np.float32)
    turn[:n_devices], turn[n_devices : 2 * n_devices] = np.cos(slots)[:, None], np.sin(slots)[:, None]
    turn[2 * n_devices : 2 * n_devices + SUB, 1] = np.cos(subs) * math.sqrt(COLUMNS)
    turn[2 * n_devices + SUB :, 1] = np.sin(subs) * math.sqrt(COLUMNS)
    return table, turn


def pieces_of(n_devices):
    rows = [len(chunks) * RADIX * SUB for chunks in PIECES]
    return rows, [r + 4 for r in rows]


def turn_tiles(recv, pitch, place, h, n_devices, factor):
    tile = jnp.concatenate(
        [recv[pl.ds((place * RADIX + rev(j, 2)) * SUB + h, n_devices, stride=pitch), :] for j in range(RADIX)], 0)
    turned = tile.T.reshape(LANES // SUB, SUB, LANES)
    return [turned[m] * factor for m in range(LANES // SUB)]


def kernel(n_outer, n_inner, total_len, x_hbm, th_hbm, tl_hbm, turn_hbm, *refs):
    n_pieces = len(PIECES)
    field, last, tot_ref, fac_ref, x_ref, th_ref, tl_ref, turn_ref, bh_ref, bl_ref = refs[:10]
    sends, recvs = refs[10 : 10 + n_pieces], [*refs[10 + n_pieces : 9 + 2 * n_pieces], last]
    near_ref, half_ref, far_ref, send_sem, recv_sem, own_sem, load_sem, last_sem, stat_sem = refs[9 + 2 * n_pieces :]
    n_devices = n_outer * n_inner
    obits, ibits = n_outer.bit_length() - 1, n_inner.bit_length() - 1
    span = LANES
    q_rows = span + 4

    loads = []
    for g in range(RADIX):
        for q in range(SUB):
            loads.append(pltpu.make_async_copy(
                x_hbm.at[pl.ds((g * SUB + q) * span, span)],
                x_ref.at[pl.ds((g * SUB + rev(q, 3)) * q_rows, span)], load_sem.at[g]))
    head = [pltpu.make_async_copy(src.at[0], dst.at[0], load_sem.at[RADIX]) for src, dst in ((th_hbm, th_ref), (tl_hbm, tl_ref))]
    rest = [pltpu.make_async_copy(src.at[pl.ds(1, RADIX - 1)], dst.at[pl.ds(1, RADIX - 1)], load_sem.at[RADIX + 1])
            for src, dst in ((th_hbm, th_ref), (tl_hbm, tl_ref))]
    rest.append(pltpu.make_async_copy(turn_hbm, turn_ref, load_sem.at[RADIX + 2]))
    for load in loads[: 2 * SUB] + head:
        load.start()

    o, i = lax.axis_index("outer"), lax.axis_index("inner")
    me = o * n_inner + i
    slot = 0
    odelta, idelta = [], []
    for k in range(obits):
        bit = o // 2**k % 2
        slot = slot + bit * 2 ** (obits - 1 - k)
        odelta.append((1 - 2 * bit) * 2**k)
    for k in range(ibits):
        bit = i // 2**k % 2
        slot = slot + bit * 2 ** (ibits - 1 - k) * n_outer
        idelta.append((1 - 2 * bit) * 2**k)

    def peer(mo, mi):
        po, pi = o, i
        for k in range(obits):
            if mo >> k & 1:
                po = po + odelta[k]
        for k in range(ibits):
            if mi >> k & 1:
                pi = pi + idelta[k]
        return po, pi

    wide = n_inner // 4
    level, place_in = i // wide, i % wide
    half = n_inner // 2
    high = level // 2
    across = level + 1 - 2 * (level % 2)
    group = n_outer * wide

    def members(at):
        return [(peer(mo, 0)[0], at * wide + lax.rem(place_in + t, wide)) for t in range(wide) for mo in range(n_outer)]

    def ranked(at):
        return [(o2 + c, at * wide + t) for o2 in range(0, n_outer, 2) for t in range(wide) for c in range(2)]

    def pairs(far, near):
        return [p for pair in itertools.zip_longest(far, near) for p in pair if p is not None]

    own = members(level)[1:]
    first = ranked(2 - high)[:-2]
    then = members((1 - high) * across)
    second = ranked(2 - high)[-2:] + pairs(ranked(high * across + (1 - high) * 3), own)
    order = ranked((1 - high) * 3) + ranked(2 - high) + own + members(across)
    left = pairs(ranked((1 - high) * 3) + ranked(2 - high)[-2:], own + members(across))

    barrier = pltpu.get_barrier_semaphore()

    def greet(ring, at, who=None):
        for p in members(at) if who is None else who:
            pl.semaphore_signal(ring, inc=1, device_id=p, device_id_type=MESH)

    tail = ranked(2)[-2:] + ranked(3)
    late = (level == 3) | (level == 2) & (o >= n_outer - 2) & (place_in == wide - 1)
    for at in (2 - high, (1 - high) * 3, across):
        pl.when(~late)(functools.partial(greet, barrier, at))
    pl.when(~late)(functools.partial(greet, barrier, level, own))
    for p in tail:
        pl.when(late & ((p[0] != o) | (p[1] != i)))(functools.partial(greet, barrier, level, [p]))
    for load in loads[2 * SUB :] + rest:
        load.start()

    def meet():
        pl.semaphore_wait(barrier, n_devices - 1 - len(tail) + len(tail) * late.astype(jnp.int32))

    def answer():
        for p in ranked(0) + ranked(1) + ranked(2)[:-2]:
            pl.when(late)(functools.partial(greet, last_sem, level, [p]))

    def meet_last():
        pl.when(~late)(lambda: pl.semaphore_wait(last_sem, len(tail)))

    rows, pitches = pieces_of(n_devices)

    def send(k, peers):
        dst = recvs[k].at[pl.ds(slot * pitches[k], rows[k])]
        for po, pi in peers:
            pltpu.make_async_remote_copy(
                src_ref=sends[k].at[pl.ds((po * n_inner + pi) * rows[k], rows[k])], dst_ref=dst,
                send_sem=send_sem, recv_sem=recv_sem.at[k],
                device_id=(po, pi), device_id_type=MESH).start()

    def own_copy(k):
        return pltpu.make_async_copy(
            sends[k].at[pl.ds(me * rows[k], rows[k])],
            recvs[k].at[pl.ds(slot * pitches[k], rows[k])], own_sem.at[k])

    def wait_rows(ref, count, sem):
        part = ref.at[pl.ds(0, count)]
        pltpu.make_async_copy(part, part, sem).wait()

    def rows_of(g, pair, ct, s):
        return [x_ref[pl.ds(g * SUB * q_rows + (2 * pair + w) * SUB + 2 * ct + s, SUB, stride=q_rows), :] for w in range(2)]

    def keep(chunk, g, pair, values):
        at = pl.ds((g * SUB + pair) * 2 * SUB, 2 * SUB)
        for s, value in enumerate(values):
            high, low = split_bf16(value)
            bh_ref[chunk, at, s * LANES : (s + 1) * LANES] = high
            bl_ref[chunk, at, s * LANES : (s + 1) * LANES] = low

    dims = (((1,), (1,)), ((), ()))

    def transform(k, place, chunk, groups, side=None):
        at = pl.ds(groups[0] * LANES, len(groups) * LANES)
        th, tl, bh, bl = th_ref[chunk], tl_ref[chunk], bh_ref[chunk, at, :], bl_ref[chunk, at, :]
        starts = range(n_devices)
        if side is not None:
            count = half * SUB
            heads = [o2 * n_inner + side * half for o2 in range(n_outer)]
            th, tl = [jnp.concatenate([ref[chunk, pl.ds(pl.multiple_of(e * SUB, count), count), :] for e in heads], 0)
                      for ref in (th_ref, tl_ref)]
            starts = [e + n for e in heads for n in range(half)]
        res = lax.dot_general(th, bh, dims, preferred_element_type=jnp.float32)
        res += lax.dot_general(th, bl, dims, preferred_element_type=jnp.float32)
        res += lax.dot_general(tl, bh, dims, preferred_element_type=jnp.float32)
        for m, e in enumerate(starts):
            for n, g in enumerate(groups):
                sends[k][pl.ds(pl.multiple_of(e * rows[k] + (place * RADIX + g) * SUB, SUB), SUB), :] = (
                    res[m * SUB : (m + 1) * SUB, n * LANES : (n + 1) * LANES])

    for g in range(RADIX):
        wait_rows(x_ref, SUB * span, load_sem.at[g])
        for pair in range(SUB):
            keep(0, g, pair, [
                jnp.concatenate([(a + c) + (b + d) for a, b, c, d in zip(*[rows_of(g, pair, ct, s) for ct in range(RADIX)])], 0)
                for s in range(2)])
        if g == 1:
            wait_rows(th_ref, 1, load_sem.at[RADIX])
            wait_rows(tl_ref, 1, load_sem.at[RADIX])
        if g % 2:
            transform(0, 0, 0, (g - 1, g), 1 - high)
    meet()
    send(0, first)
    answer()
    transform(0, 0, 0, range(RADIX), high)
    send(0, then)
    own_copy(0).start()

    zero = jnp.zeros((SUB, LANES), jnp.float32)
    squares, zr, zi = [zero] * 4, zero, zero
    for g in range(RADIX):
        for pair in range(SUB):
            part = [[rows_of(g, pair, ct, s) for s in range(2)] for ct in range(RADIX)]
            for ct in range(RADIX):
                for s in range(2):
                    for w in range(2):
                        squares[ct] = squares[ct] + part[ct][s][w] * part[ct][s][w]
            for w in range(2):
                angle = 2.0 * math.pi / total_len * n_devices * (rev(2 * pair + w, 4) * SUB * RADIX + rev(g, 2))
                cw, sw = math.cos(angle), math.sin(angle)
                zr = zr + (part[0][0][w] * cw + part[0][1][w] * sw)
                zi = zi + (part[0][1][w] * cw - part[0][0][w] * sw)
            (x0r, x0i), (x1r, x1i), (x2r, x2i), (x3r, x3i) = [
                [jnp.concatenate(part[ct][s], 0) for s in range(2)] for ct in range(RADIX)]
            br, bi, dr, di = x0r - x2r, x0i - x2i, x1r - x3r, x1i - x3i
            keep(1, g, pair, (br - di, bi + dr))
            keep(2, g, pair, ((x0r + x2r) - (x1r + x3r), (x0i + x2i) - (x1i + x3i)))
            keep(3, g, pair, (br + di, bi - dr))

    for ref in (th_ref, tl_ref):
        wait_rows(ref, RADIX - 1, load_sem.at[RADIX + 1])
    rest[-1].wait()
    pc, ps = turn_ref[2 * n_devices : 2 * n_devices + SUB, :], turn_ref[2 * n_devices + SUB :, :]
    oc, os_ = turn_ref[pl.ds(slot, 1), :], turn_ref[pl.ds(n_devices + slot, 1), :]
    total = jnp.sum(jnp.sum((squares[0] + squares[1]) + (squares[2] + squares[3]), 0, keepdims=True), 1, keepdims=True)
    yr = jnp.sum(zr * pc + zi * ps, 0, keepdims=True)
    yi = jnp.sum(zi * pc - zr * ps, 0, keepdims=True)
    wr = jnp.sum(yr * oc + yi * os_, 1, keepdims=True)
    wi = jnp.sum(yi * oc - yr * os_, 1, keepdims=True)
    lane = lax.broadcasted_iota(jnp.int32, (1, LANES), 1)
    stat = jnp.where(lane == 0, total, jnp.where(lane == 1, wr, jnp.where(lane == 2, wi, 0.0)))
    mine = pl.ds(o * half + i % half, 1)
    near_ref[mine, :] = stat

    def send_row(src, dst, sem, to):
        pltpu.make_async_remote_copy(
            src_ref=src, dst_ref=dst, send_sem=send_sem, recv_sem=stat_sem.at[sem],
            device_id=to, device_id_type=MESH).start()

    for k, chunks in list(enumerate(PIECES))[1:]:
        for place, chunk in enumerate(chunks):
            transform(k, place, chunk, range(RADIX))
        if k == 1:
            send(1, first)
            meet_last()
            send(0, second)
            for to in own + members(across):
                send_row(near_ref.at[mine], near_ref.at[mine], 0, to)
        if k == n_pieces - 1:
            wait_rows(near_ref, half * n_outer - 1, stat_sem.at[0])
            half_ref[...] = jnp.sum(near_ref[...], 0, keepdims=True)
            send_row(half_ref, far_ref, 1, peer(0, half))
        send(k, left if k == 1 else order)
        own_copy(k).start()

    for k, chunks in enumerate(PIECES):
        wait_rows(recvs[k], (n_devices - 1) * rows[k], recv_sem.at[k])
        own_copy(k).wait()
        if k == STAT:
            wait_rows(far_ref, 1, stat_sem.at[1])
            sums = half_ref[...] + far_ref[...]
            mean_square = jnp.sum(jnp.where(lane == 0, sums, 0.0), 1, keepdims=True) / total_len
            shifted = mean_square + 1e-06
            factor = lax.rsqrt(shifted)
            factor = factor * (1.5 - 0.5 * shifted * factor * factor)
            checks = jnp.where(lane == 0, mean_square, sums * (factor / math.sqrt(total_len)))
            tot_ref[...] = jnp.broadcast_to(checks, (SUB, LANES))
            factor = jnp.broadcast_to(factor, (SUB, LANES))
            fac_ref[...] = factor
        ready = range(STAT + 1) if k == STAT else [k] if STAT < k < n_pieces - 1 else []
        for kk in ready:
            for place, chunk in enumerate(PIECES[kk]):
                for h in range(SUB):
                    base = ((h // 2) * (RADIX - 1) + chunk) * 2 * LANES + h % 2
                    for m, v in enumerate(turn_tiles(recvs[kk], pitches[kk], place, h, n_devices, factor)):
                        field[pl.ds(base + rev(m, 4) * 2 * SUB, SUB, stride=2), :] = v
    for k in range(n_pieces):
        wait_rows(sends[k], (n_devices - 1) * rows[k], send_sem)
    wait_rows(near_ref, half * n_outer, send_sem)


def finish_kernel(n_devices, pitch, field, last, tot_ref, fac_ref, out_hbm, checks_hbm, turned, checks_ref, sem):
    f_rows = 2 * LANES
    many = (RADIX - 1) * f_rows
    stores = []
    for fq in range(RADIX):
        stores.append(pltpu.make_async_copy(
            field.at[pl.ds(fq * many, many)], out_hbm.at[pl.ds(fq * RADIX * f_rows, many)], sem.at[0]))
        stores[-1].start()
    checks_ref[...] = tot_ref[0:1, 0:3]
    checks_copy = pltpu.make_async_copy(checks_ref, checks_hbm, sem.at[1])
    checks_copy.start()
    factor = fac_ref[...]
    for h in range(SUB):
        base = h // 2 * f_rows + h % 2
        for m, v in enumerate(turn_tiles(last, pitch, 0, h, n_devices, factor)):
            turned[pl.ds(base + rev(m, 4) * 2 * SUB, SUB, stride=2), :] = v
        if h % 2:
            fq = h // 2
            stores.append(pltpu.make_async_copy(
                turned.at[pl.ds(fq * f_rows, f_rows)],
                out_hbm.at[pl.ds((fq * RADIX + RADIX - 1) * f_rows, f_rows)], sem.at[0]))
            stores[-1].start()
    pltpu.make_async_copy(out_hbm, out_hbm, sem.at[0]).wait()
    checks_copy.wait()


def fast(n_outer, n_inner, amplitudes):
    amp_dev = amplitudes.shape[1]
    n_devices = n_outer * n_inner
    rows_count = amp_dev // COLUMNS
    total_len = amp_dev * n_devices
    view = amplitudes.reshape(2, amp_dev // LANES, LANES).transpose(1, 0, 2).reshape(-1, LANES)
    table, turn = tables(n_devices, total_len)
    th = table.astype(jnp.bfloat16)
    tl = (table - th.astype(np.float32)).astype(jnp.bfloat16)
    hbm, vmem = pl.BlockSpec(memory_space=pltpu.HBM), pl.BlockSpec(memory_space=pltpu.VMEM)
    rows, pitches = pieces_of(n_devices)
    small = pltpu.VMEM((SUB, LANES), jnp.float32)
    f_rows = 2 * LANES
    pair = pltpu.VMEM((RADIX, rows_count, 2 * LANES), jnp.bfloat16)
    scratch = [
        pltpu.VMEM((RADIX * SUB * (LANES + 4), LANES), jnp.float32),
        pltpu.VMEM(th.shape, jnp.bfloat16),
        pltpu.VMEM(tl.shape, jnp.bfloat16),
        pltpu.VMEM(turn.shape, jnp.float32),
        pair,
        pair,
        *[pltpu.VMEM((n_devices * r, LANES), jnp.float32) for r in rows],
        *[pltpu.VMEM((n_devices * p, LANES), jnp.float32) for p in pitches[:-1]],
        pltpu.VMEM((n_devices // 2, LANES), jnp.float32),
        pltpu.VMEM((1, LANES), jnp.float32),
        pltpu.VMEM((1, LANES), jnp.float32),
        pltpu.SemaphoreType.DMA,
        pltpu.SemaphoreType.DMA((len(PIECES),)),
        pltpu.SemaphoreType.DMA((len(PIECES),)),
        pltpu.SemaphoreType.DMA((RADIX + 3,)),
        pltpu.SemaphoreType.REGULAR,
        pltpu.SemaphoreType.DMA((2,)),
    ]
    parts = pl.pallas_call(
        functools.partial(kernel, n_outer, n_inner, total_len),
        out_shape=(
            pltpu.VMEM((RADIX * (RADIX - 1) * f_rows, LANES), jnp.float32),
            pltpu.VMEM((n_devices * pitches[-1], LANES), jnp.float32),
            small,
            small,
        ),
        in_specs=[hbm] * 4,
        out_specs=(vmem,) * 4,
        scratch_shapes=scratch,
        compiler_params=pltpu.CompilerParams(collective_id=0, has_side_effects=True, vmem_limit_bytes=32_000_000),
    )(*[pltpu.with_memory_space_constraint(v, pltpu.HBM) for v in (view, jnp.asarray(th), jnp.asarray(tl), jnp.asarray(turn))])
    field, checks = pl.pallas_call(
        functools.partial(finish_kernel, n_devices, pitches[-1]),
        out_shape=(jax.ShapeDtypeStruct(view.shape, jnp.float32), jax.ShapeDtypeStruct((1, 3), jnp.float32)),
        in_specs=[vmem] * 4,
        out_specs=(hbm, hbm),
        scratch_shapes=[
            pltpu.VMEM((RADIX * f_rows, LANES), jnp.float32),
            pltpu.VMEM((1, 3), jnp.float32),
            pltpu.SemaphoreType.DMA((2,)),
        ],
        compiler_params=pltpu.CompilerParams(vmem_limit_bytes=32_000_000),
    )(*parts)
    result = field.reshape(-1, 2, LANES).transpose(1, 0, 2).reshape(2, amp_dev)
    return result, checks.reshape(3)


def reverse_index(values, count):
    result = jnp.zeros_like(values)
    for bit_pos in range(count):
        result = result | (values >> bit_pos & 1) << count - 1 - bit_pos
    return result


def reversal_table(size, count):
    indices = jnp.arange(size, dtype=jnp.int32)
    return (reverse_index(indices, count)[:, None] == indices[None, :]).astype(jnp.float32)


def check_terms(current, positions, angle_scale):
    angles = positions.astype(jnp.float32) * angle_scale
    cosine = jnp.cos(angles)
    sine = jnp.sin(angles)
    squares = jnp.sum(current * current)
    phase_real = jnp.sum(current[0] * cosine + current[1] * sine)
    phase_imag = jnp.sum(current[1] * cosine - current[0] * sine)
    return (squares, phase_real, phase_imag)


def per_device(amplitudes):
    amp_dev = amplitudes.shape[1]
    n_outer = lax.axis_size("outer")
    n_inner = lax.axis_size("inner")
    outer_bits = n_outer.bit_length() - 1
    inner_bits = n_inner.bit_length() - 1
    global_bits = outer_bits + inner_bits
    local_bits = amp_dev.bit_length() - 1
    n_devices = n_outer * n_inner
    high_count = amp_dev // n_devices
    total_len = amp_dev * n_devices
    columns = 2**WINDOW
    rows_count = amp_dev // columns
    column_ids = jnp.arange(columns, dtype=jnp.int32)
    reversed_ids = reverse_index(column_ids, WINDOW)
    products = column_ids[:, None] * reversed_ids[None, :] % columns
    angles = products.astype(jnp.float32) * (2.0 * math.pi / columns)
    real_part = jnp.cos(angles) / math.sqrt(columns)
    imag_part = jnp.sin(angles) / math.sqrt(columns)
    table = jnp.concatenate(
        [jnp.concatenate([real_part, imag_part], 1), jnp.concatenate([-imag_part, real_part], 1)], 0
    )
    stacked = jnp.concatenate(
        [amplitudes[0].reshape(rows_count, columns), amplitudes[1].reshape(rows_count, columns)], 1
    )
    result = jnp.dot(
        stacked, table, precision=lax.Precision.HIGHEST, preferred_element_type=jnp.float32
    )
    windowed = jnp.stack([result[:, :columns].reshape(-1), result[:, columns:].reshape(-1)])
    device_id = lax.axis_index("outer") * n_inner + lax.axis_index("inner")
    angle_scale = 2.0 * math.pi / total_len
    local_ids = jnp.arange(amp_dev, dtype=jnp.int32)
    positions = reverse_index(device_id * amp_dev + local_ids, local_bits + global_bits)
    totals = lax.psum(check_terms(windowed, positions, angle_scale), ("outer", "inner"))
    device_table = reversal_table(n_devices, global_bits)
    high_table = reversal_table(high_count, local_bits - global_bits)
    grid = windowed.reshape(2, high_count, n_devices)
    ordered = jnp.einsum("pm,shm->sph", device_table, grid, precision=lax.Precision.HIGHEST)
    blocks = ordered.reshape(2, n_outer, n_inner, high_count)
    blocks = lax.all_to_all(
        lax.all_to_all(blocks, "outer", split_axis=1, concat_axis=1, tiled=True),
        "inner",
        split_axis=2,
        concat_axis=2,
        tiled=True,
    )
    received = blocks.reshape(2, n_devices, high_count)
    turned_high = jnp.einsum("qh,sdh->sdq", high_table, received, precision=lax.Precision.HIGHEST)
    placed = jnp.einsum("ed,sdq->sqe", device_table, turned_high, precision=lax.Precision.HIGHEST)
    reversed_field = placed.reshape(2, amp_dev)
    mean_square = totals[0] / total_len
    factor = lax.rsqrt(mean_square + 1e-06)
    scaled = factor / math.sqrt(total_len)
    checks = jnp.stack([mean_square, totals[1] * scaled, totals[2] * scaled])
    return (reversed_field * factor, checks)


def solution(mesh):
    n_outer, n_inner = mesh.shape["outer"], mesh.shape["inner"]

    def body(amplitudes):
        rows_count = amplitudes.shape[1] // COLUMNS
        n_devices = n_outer * n_inner
        if rows_count * n_devices == LANES * LANES and n_devices * SUB == 2 * LANES and n_inner % 4 == 0:
            return fast(n_outer, n_inner, amplitudes)
        return per_device(amplitudes)

    return jax.shard_map(
        body,
        mesh=mesh,
        in_specs=(P(None, ("outer", "inner")),),
        out_specs=(P(None, ("outer", "inner")), P()),
        check_vma=False,
    )
```
